128 devices in a mesh: samp: 16 (over z, x), feat: 8 (over y, core).
Axes of the slice: x: 4, y: 4, z: 4, core: 2. Of those that a mesh axis runs over, the one named last changes fastest.
Arguments:
- features: bfloat16 [262144, 2048], P('samp', 'feat'), may hold values from -40 to 40
- labels: int32 [262144], P('samp'), may hold values from 0 to 9
- weights: float32 [10, 2048], P(None, 'feat'), may hold values from -6 to 6
- sketch_basis: float32 [10, 2048, 512], P(None, 'feat'), may hold values from -0.0390625 to 0.0390625
- sketch_values: float32 [512], replicated, may hold values from 0.05 to 2
Outputs:
- newton_step: float32 [10, 2048], P(None, 'feat')
The draws below stay inside these ranges and needn't reach their ends.
All inputs are finite; a program needn't handle non-finite values.
Results may differ from the reference program's by a relative error of at most 0.001.
The reference program's roundings to bfloat16 on the way count: a program that leaves them out, or rounds other values in their place, can miss the bound.
Values may be sent and summed in bfloat16 or wider, within the bound.
A program may use at most 128 MiB of HBM per device.

```python
import math
import jax
import jax.numpy as jnp
from jax import lax

F = 2048
K = 10
R = 512
ITERS = 3
NS = 262144


def class_weights(key):
    drawn = jax.random.normal(jax.random.fold_in(key, 7001), (K, F), jnp.float32)
    return jnp.clip(drawn, -6.0, 6.0)


def draw_weights(key, part):
    return class_weights(key)


def draw_features(key, part):
    keys = jax.random.split(jax.random.fold_in(key, 7002), 4)
    columns = jnp.arange(F, dtype=jnp.float32)
    col_scale = jnp.exp(jax.random.uniform(keys[0], (F,), jnp.float32, math.log(0.5), math.log(5.0)))
    col_scale = col_scale * jnp.exp(0.5 * math.log(3.0) * columns / F)
    values = jax.random.normal(keys[3], (NS, F), jnp.float32) * col_scale[None, :]
    return jnp.clip(values, -40.0, 40.0).astype(jnp.bfloat16)


def set_ends(array, rng, least, top_value):
    longest = array.shape.index(max(array.shape))
    spots = []
    for shift in (0, 1):
        where = [jax.random.randint(jax.random.fold_in(rng, axis), (), 0, length) for axis, length in enumerate(array.shape)]
        where[longest] = (where[longest] + shift) % array.shape[longest]
        spots.append(tuple(where))
    return array.at[spots[0]].set(least).at[spots[1]].set(top_value)


def level_of(rng, dims, shards, least, largest):
    gain, own = 1.0, jax.random.fold_in(rng, 6)
    for axis_at, parts in shards:
        steps = jnp.exp(jax.random.uniform(jax.random.fold_in(own, axis_at), (parts,), jnp.float32, least / len(shards), largest / len(shards)))
        gain = gain * jnp.repeat(steps, dims[axis_at] // parts).reshape([-1 if axis == axis_at else 1 for axis in range(len(dims))])
    return gain


def gaussian(key, shape, spread, bound, shards=(), kind=jnp.bfloat16):
    loudness = level_of(key, shape, shards, -0.22, 0.18) if shards else 1.0
    entries = jax.random.normal(key, shape, jnp.float32) * spread * loudness
    return jnp.minimum(jnp.maximum(entries, -bound), bound).astype(kind)


def setup_inputs(seed: int = 0) -> dict:
    arg_keys = jax.random.split(jax.random.key(seed), 6)
    return {
        "features": draw_features(jax.random.fold_in(arg_keys[5], 71), 0),
        "labels": set_ends(jax.random.randint(arg_keys[1], (NS,), 0, K), jax.random.fold_in(arg_keys[1], 1), 0, K - 1).astype(jnp.int32),
        "weights": draw_weights(jax.random.fold_in(arg_keys[5], 71), 0),
        "sketch_basis": gaussian(arg_keys[3], (K, F, R), (F * K) ** -0.5, 0.0390625, ((1, 8),), jnp.float32),
        "sketch_values": jnp.clip(jnp.exp(jax.random.uniform(arg_keys[4], (R,), jnp.float32, math.log(0.05), math.log(2.0))), 0.05, 2.0),
    }


ridge = 0.05
contract_last = (((1,), (1,)), ((), ()))

def column_softmax(scores):
    column_max = lax.optimization_barrier(jnp.max(scores, axis=0, keepdims=True))
    shifted_exp = jnp.exp(scores - column_max)
    return shifted_exp / lax.optimization_barrier(jnp.sum(shifted_exp, axis=0, keepdims=True))

def reference(features, labels, weights, sketch_basis, sketch_values):
    total_rows = features.shape[0]

    def project(vector):
        return lax.dot_general(vector.astype(jnp.bfloat16).astype(jnp.float32), features.astype(jnp.float32), contract_last, preferred_element_type=jnp.float32)

    def collect(coeffs):
        return jnp.dot(coeffs.astype(jnp.bfloat16).astype(jnp.float32), features.astype(jnp.float32), preferred_element_type=jnp.float32)
    probabilities = column_softmax(project(weights) / math.sqrt(F))
    onehot = (labels[None, :] == jnp.arange(K, dtype=jnp.int32)[:, None]).astype(jnp.float32)
    gradient = collect(probabilities - onehot) * (math.sqrt(F) / total_rows) + ridge * weights

    def hessian(direction):
        image_vals = project(direction)
        weighted = probabilities * image_vals
        curvature = weighted - probabilities * lax.optimization_barrier(jnp.sum(weighted, axis=0, keepdims=True))
        return collect(curvature) / total_rows + ridge * direction
    flat_basis = sketch_basis.reshape(K * F, R)
    gram_matrix = jnp.dot(flat_basis.T, flat_basis, precision=lax.Precision.HIGHEST)
    factor = jnp.linalg.cholesky(gram_matrix)
    coefficients = (jnp.min(sketch_values) + ridge) / (sketch_values + ridge) - 1.0

    def precondition(residue):
        projection = jnp.dot(residue.reshape(-1), flat_basis, precision=lax.Precision.HIGHEST)
        inner_coords = jax.scipy.linalg.solve_triangular(factor, projection, lower=True)
        outer_coords = jax.scipy.linalg.solve_triangular(factor, coefficients * inner_coords, lower=True, trans=1)
        return residue + jnp.dot(flat_basis, outer_coords, precision=lax.Precision.HIGHEST).reshape(residue.shape)
    residue = -gradient
    newton_step = jnp.zeros_like(residue)
    scaled_res = precondition(residue)
    direction = scaled_res
    res_dot = jnp.sum(residue * scaled_res)
    for iteration in range(ITERS):
        hess_image = hessian(direction)
        step_size = res_dot / jnp.sum(direction * hess_image)
        newton_step = newton_step + step_size * direction
        if iteration + 1 < ITERS:
            residue = residue - step_size * hess_image
            scaled_res = precondition(residue)
            new_dot = jnp.sum(residue * scaled_res)
            direction = scaled_res + new_dot / res_dot * direction
            res_dot = new_dot
    return newton_step
```

```python
import functools
import math

import jax
import jax.numpy as jnp
from jax import lax
from jax.experimental import pallas as pl
from jax.experimental.pallas import tpu as pltpu
from jax.sharding import PartitionSpec as P

F = 2048
ITERS = 3
RIDGE = 0.05
SAMP, YS, CORES = 16, 4, 2
FEAT = YS * CORES
ROWS = 16384
HALF = ROWS // CORES
CHUNKS = 4
CROWS = HALF // CHUNKS
PIECE = CROWS // YS
COLS = 256
K = 10
RANK = 512
LT = K * COLS // 128
f32, bf16 = jnp.float32, jnp.bfloat16
HI = lax.Precision.HIGHEST
NT = (((1,), (1,)), ((), ()))
TN = (((0,), (0,)), ((), ()))


def rcopy(src, dst, send, recv, dev):
    return pltpu.make_async_remote_copy(
        src_ref=src, dst_ref=dst, send_sem=send, recv_sem=recv,
        device_id=dev, device_id_type=pl.DeviceIdType.MESH,
    )


def rows_of(n):
    return lax.broadcasted_iota(jnp.int32, (n, 128), 0)


def pack(wide):
    low = wide[8:16]
    third = low[:, :128] + pltpu.roll(low[:, 128:], 2, 0)
    return jnp.concatenate([wide[:8], third], axis=1)


def unpack(packed):
    third = packed[:, 256:]
    row = rows_of(8)
    left = jnp.where(row < 2, third, 0.0)
    right = jnp.where(row < 2, pltpu.roll(third, 6, 0), 0.0)
    return jnp.concatenate([packed[:, :256], jnp.concatenate([left, right], axis=1)], axis=0)


def lane_row(packed, k, h):
    if k < 8:
        return packed[k : k + 1, h * 128 : (h + 1) * 128]
    r = 2 * h + (k - 8)
    return packed[r : r + 1, 256:384]


def column(row):
    return jnp.broadcast_to(row, (128, 128)).T


def factor_block(A, N):
    for p in range(16):
        lo = 8 * p
        n = 128 - lo
        ap = A[lo:128, :]
        cols = [jnp.broadcast_to(ap[:, lo + j : lo + j + 1], (n, 128)) for j in range(8)]
        arow, nrow = A[lo : lo + 8, :], N[lo : lo + 8, :]
        cs, us, ns = [], [], []
        for j in range(8):
            r = lax.rsqrt(cols[j][j : j + 1, :])
            c = cols[j] * r
            u = arow[j : j + 1, :] * r
            v = nrow[j : j + 1, :] * r
            for k in range(j + 1, 8):
                cols[k] = cols[k] - c * c[k : k + 1, :]
            arow = arow - c[:8] * u
            nrow = nrow - c[:8] * v
            cs.append(c)
            us.append(u)
            ns.append(v)
        if n > 8:
            at, nt = A[lo + 8 : 128, :], N[lo + 8 : 128, :]
            for j in range(8):
                at = at - cs[j][8:] * us[j]
                nt = nt - cs[j][8:] * ns[j]
            A[lo + 8 : 128, :] = at
            N[lo + 8 : 128, :] = nt
        N[lo : lo + 8, :] = jnp.concatenate(ns, axis=0)


def kernel(
    feat, labels, w16, basis, svals, out,
    X, bst, BT, dB, imgf, imgb, recvg, recvh, prob, E, Q, Qr, ar, fe,
    gparts, gall, V, AK, FA, FN, ccol, tmp, vec, prow, scal,
    sx_own, sx_s, sx_r, s_b, rs_s, rs_r, ag_s, ag_r, q_s, q_r, d_s, d_r,
    ar_s, ar_r, fe_s, fe_r, gf_s, gf_r, gs_s, gs_r,
):
    s = lax.axis_index("samp")
    f = lax.axis_index("feat")
    y = lax.div(f, CORES)
    c = lax.rem(f, CORES)
    sib = (s, f + 1 - 2 * c)

    def samp_dev(i):
        return lax.rem(s + i, SAMP)

    def feat_dev(i):
        return lax.rem(f + i, FEAT)

    def y_dev(i):
        return lax.rem(y + i, YS)

    for k in range(K):
        pltpu.make_async_copy(basis.at[pl.ds(k * COLS, COLS)], bst.at[pl.ds(k * COLS, COLS)], s_b.at[k]).start()

    def own_rows(t):
        return pl.ds(pl.multiple_of(c * HALF + t * CROWS, CROWS), CROWS)

    def sib_rows(t):
        return pl.ds(pl.multiple_of((1 - c) * HALF + t * CROWS, CROWS), CROWS)

    def x_own(t):
        return pltpu.make_async_copy(feat.at[own_rows(t)], X.at[c, pl.ds(t * CROWS, CROWS)], sx_own.at[t])

    def x_send(t):
        return rcopy(feat.at[sib_rows(t)], X.at[c, pl.ds(t * CROWS, CROWS)], sx_s.at[t], sx_r.at[t], sib)

    def x_recv(t):
        dst = X.at[1 - c, pl.ds(t * CROWS, CROWS)]
        return rcopy(dst, dst, sx_s.at[t], sx_r.at[t], sib)

    for t in range(CHUNKS):
        x_own(t).start()

    def d_copy(ph):
        return rcopy(dB.at[ph, c], dB.at[ph, c], d_s.at[ph], d_r.at[ph], sib)

    def d_recv(ph):
        return rcopy(dB.at[ph, 1 - c], dB.at[ph, 1 - c], d_s.at[ph], d_r.at[ph], sib)

    barrier = pltpu.get_barrier_semaphore()
    for i in range(1, FEAT):
        pl.semaphore_signal(barrier, inc=1, device_id=(s, feat_dev(i)), device_id_type=pl.DeviceIdType.MESH)
    for i in range(1, SAMP):
        pl.semaphore_signal(barrier, inc=1, device_id=(samp_dev(i), f), device_id_type=pl.DeviceIdType.MESH)

    w = w16[...]
    dB[0, c] = w.astype(bf16)
    pl.semaphore_wait(barrier, FEAT - 1 + SAMP - 1)
    d_copy(0).start()
    for t in range(CHUNKS):
        x_send(t).start()

    @pl.loop(0, K)
    def _(k):
        pltpu.make_async_copy(
            basis.at[pl.ds(k * COLS, COLS)], bst.at[pl.ds(k * COLS, COLS)], s_b.at[k]
        ).wait()
        for h in range(2):
            for jt in range(4):
                blk = bst[pl.ds(pl.multiple_of(k * COLS + h * 128, 128), 128), jt * 128 : (jt + 1) * 128]
                BT[jt * 128 : (jt + 1) * 128, pl.ds(pl.multiple_of(k * COLS + h * 128, 128), 128)] = blk.T

    blk_id = lax.min(s, 9)
    ba = sum((blk_id >= e).astype(jnp.int32) for e in (4, 7, 9))
    bb = blk_id - lax.div(ba * (9 - ba), 2) + ba

    def gram_step(kk, acc):
        cols = pl.ds(pl.multiple_of(kk * 256, 256), 256)
        return acc + lax.dot_general(
            BT[pl.ds(pl.multiple_of(ba * 128, 128), 128), cols],
            BT[pl.ds(pl.multiple_of(bb * 128, 128), 128), cols],
            NT, precision=HI, preferred_element_type=f32,
        )

    gparts[f] = lax.fori_loop(0, K, gram_step, jnp.zeros((128, 128), f32))

    def gf_copy(i):
        return rcopy(gparts.at[f], gparts.at[f], gf_s.at[i], gf_r.at[f], (s, feat_dev(i)))

    def gf_recv(i):
        src = feat_dev(i)
        return rcopy(gparts.at[src], gparts.at[src], gf_s.at[i], gf_r.at[src], (s, src))

    def gs_copy(i):
        return rcopy(gall.at[s], gall.at[s], gs_s.at[i], gs_r.at[s], (samp_dev(i), f))

    @pl.when(s < 10)
    def _():
        for i in range(1, FEAT):
            gf_copy(i).start()

    def rs_copy(ph, t, i, grad):
        o = y_dev(i)
        src = imgf.at[t, o] if grad else imgb.at[t, o]
        dst = recvg.at[t, y] if grad else recvh.at[ph - 1, t, y]
        return rcopy(src, dst, rs_s.at[ph, t, i], rs_r.at[ph, t, y], (s, CORES * o + c))

    def rs_recv(ph, t, i, grad):
        o = y_dev(i)
        dst = recvg.at[t, o] if grad else recvh.at[ph - 1, t, o]
        return rcopy(dst, dst, rs_s.at[ph, t, i], rs_r.at[ph, t, o], (s, CORES * o + c))

    def ag_copy(ph, t, i):
        return rcopy(E.at[ph, t, y], E.at[ph, t, y], ag_s.at[ph, t, i], ag_r.at[ph, t, y], (s, CORES * y_dev(i) + c))

    def ag_recv(ph, t, i):
        o = y_dev(i)
        return rcopy(E.at[ph, t, o], E.at[ph, t, o], ag_s.at[ph, t, i], ag_r.at[ph, t, o], (s, CORES * o + c))

    def images(ph, grad):
        @pl.loop(0, CHUNKS)
        def _(t):
            if grad:
                x_own(t).wait()
                x_recv(t).wait_recv()
            at = pl.ds(pl.multiple_of(t * CROWS, CROWS), CROWS)
            img = lax.dot_general(dB[ph, 0], X[0, at], NT, preferred_element_type=f32)
            img = img + lax.dot_general(dB[ph, 1], X[1, at], NT, preferred_element_type=f32)
            for o in range(YS):
                piece = img[:, o * PIECE : (o + 1) * PIECE]
                imgf[t, o] = piece
                if not grad:
                    imgb[t, o] = piece.astype(bf16)
            for i in range(1, YS):
                rs_copy(ph, t, i, grad).start()

    def pieces(ph, grad):
        @pl.loop(0, CHUNKS)
        def _(t):
            total = imgf[t, y]
            for i in range(1, YS):
                rs_recv(ph, t, i, grad).wait_recv()
            for i in range(1, YS):
                o = y_dev(i)
                total = total + (recvg[t, o] if grad else recvh[ph - 1, t, o].astype(f32))
            if grad:
                logits = total / math.sqrt(F)
                row = lax.broadcasted_iota(jnp.int32, (16, PIECE), 0)
                logits = jnp.where(row < K, logits, -jnp.inf)
                top = jnp.max(logits, axis=0, keepdims=True)
                ex = jnp.exp(logits - top)
                pr = ex / jnp.sum(ex, axis=0, keepdims=True)
                prob[t] = pr
                own = labels[pl.ds(c * (CHUNKS * YS) + t * YS + y, 1), :]
                coeffs = pr - jnp.where(row == own, 1.0, 0.0)
            else:
                pr = prob[t]
                weighted = pr * total
                coeffs = weighted - pr * jnp.sum(weighted, axis=0, keepdims=True)
            E[ph, t, y] = coeffs.astype(bf16)
            for i in range(1, YS):
                ag_copy(ph, t, i).start()

    def collect(ph):
        Q[...] = jnp.zeros_like(Q)

        @pl.loop(0, CHUNKS)
        def _(t):
            for i in range(1, YS):
                ag_recv(ph, t, i).wait_recv()
            e = jnp.concatenate([E[ph, t, o] for o in range(YS)], axis=1)
            at = pl.ds(pl.multiple_of(t * CROWS, CROWS), CROWS)
            for h in range(2):
                Q[h] = Q[h] + jnp.dot(e, X[h, at], preferred_element_type=f32)

    def q_copy(ph):
        return rcopy(Q.at[1 - c], Qr.at[ph], q_s.at[ph], q_r.at[ph], sib)

    def ar_copy(ph, i):
        return rcopy(ar.at[ph, s], ar.at[ph, s], ar_s.at[ph, i], ar_r.at[ph, s], (samp_dev(i), f))

    def ar_recv(ph, i):
        o = samp_dev(i)
        return rcopy(ar.at[ph, o], ar.at[ph, o], ar_s.at[ph, i], ar_r.at[ph, o], (o, f))

    def fe_copy(ph, i):
        return rcopy(fe.at[ph, f], fe.at[ph, f], fe_s.at[ph, i], fe_r.at[ph, f], (s, feat_dev(i)))

    def fe_recv(ph, i):
        o = feat_dev(i)
        return rcopy(fe.at[ph, o], fe.at[ph, o], fe_s.at[ph, i], fe_r.at[ph, o], (s, o))

    def start_sums(ph):
        q_copy(ph).start()
        q_copy(ph).wait_recv()
        ar[ph, s] = pack(Q[c] + Qr[ph])
        for i in range(1, SAMP):
            ar_copy(ph, i).start()

    def finish_sums(ph):
        for i in range(1, SAMP):
            ar_recv(ph, i).wait_recv()
        total = ar[ph, 0]
        for o in range(1, SAMP):
            total = total + ar[ph, o]
        return total

    def drain(ph, grad):
        d_copy(ph).wait_send()
        q_copy(ph).wait_send()

        @pl.loop(0, CHUNKS)
        def _(t):
            for i in range(1, YS):
                rs_copy(ph, t, i, grad).wait_send()
                ag_copy(ph, t, i).wait_send()

    def exchange(ph, message):
        fe[ph, f] = message
        for i in range(1, FEAT):
            fe_copy(ph, i).start()
        for i in range(1, FEAT):
            fe_recv(ph, i).wait_recv()
        total = fe[ph, 0]
        for o in range(1, FEAT):
            total = total + fe[ph, o]
        return total

    d_recv(0).wait_recv()
    images(0, True)

    @pl.when(s < 10)
    def _():
        for i in range(1, FEAT):
            gf_recv(i).wait_recv()
        total = gparts[0]
        for o in range(1, FEAT):
            total = total + gparts[o]
        gall[s] = total
        for i in range(1, SAMP):
            gs_copy(i).start()

    pieces(0, True)
    collect(0)
    start_sums(0)

    sv = svals[...]
    low = jnp.min(jnp.min(sv, axis=1, keepdims=True), axis=0, keepdims=True)
    coef = (low + RIDGE) / (sv + RIDGE) - 1.0
    for jt in range(4):
        ccol[jt * 128 : (jt + 1) * 128, :] = column(coef[jt : jt + 1, :])
    V[...] = jnp.zeros_like(V)
    eye = jnp.where(rows_of(128) == lax.broadcasted_iota(jnp.int32, (128, 128), 1), 1.0, 0.0).astype(f32)

    @pl.loop(0, 4)
    def _(kb):
        off = lax.div(kb * (9 - kb), 2) - kb
        for l in range(4):
            src = lax.max(off + l, 0)

            @pl.when((l >= kb) & (src != s))
            def _():
                rcopy(gall.at[src], gall.at[src], gs_s.at[0], gs_r.at[src], (src, f)).wait_recv()

            @pl.when(l >= kb)
            def _():
                AK[:, l * 128 : (l + 1) * 128] = gall[src]

            @pl.when(l < kb)
            def _():
                AK[:, l * 128 : (l + 1) * 128] = jnp.zeros((128, 128), f32)

            AK[:, RANK + l * 128 : RANK + (l + 1) * 128] = jnp.where(kb == l, eye, 0.0)
        kcols = pl.ds(pl.multiple_of(kb * 128, 128), 128)

        @pl.when(kb > 0)
        def _():
            for l in range(4):
                lanes = slice(l * 256, (l + 1) * 256)
                AK[:, lanes] = AK[:, lanes] - lax.dot_general(
                    V[:, kcols], V[:, lanes], TN, precision=HI, preferred_element_type=f32
                )

        FA[...] = AK[:, kcols]
        FN[...] = eye
        factor_block(FA, FN)
        inv = FN[...]
        for l in range(8):
            lanes = slice(l * 128, (l + 1) * 128)
            blk = jnp.dot(inv, AK[:, lanes], precision=HI, preferred_element_type=f32)
            if l < 4:
                blk = jnp.where(l < kb, 0.0, blk)
            V[kcols, lanes] = blk

    def basis_dots(packed):
        rows = [lane_row(packed, lt // 2, lt % 2) for lt in range(LT)]

        @pl.loop(0, 8)
        def _(g):
            at = pl.ds(pl.multiple_of(g * 64, 64), 64)
            acc = BT[at, 0:128] * rows[0]
            for lt in range(1, LT):
                acc = acc + BT[at, lt * 128 : (lt + 1) * 128] * rows[lt]
            tmp[at, :] = acc

        return [jnp.sum(tmp[jt * 128 : (jt + 1) * 128, :].T, axis=0, keepdims=True) for jt in range(4)]

    def lanes_of(a, b):
        t = a * b
        t = jnp.sum(t[:, :128] + t[:, 128:256] + t[:, 256:], axis=0, keepdims=True)
        return t + pltpu.roll(t, 64, 1)

    lane = lax.broadcasted_iota(jnp.int32, (1, 128), 1)

    def both(x, z):
        return jnp.where(lane < 64, x, z)

    def halves(total):
        wide = lax.broadcasted_iota(jnp.int32, (8, 128), 1)
        lo = jnp.sum(jnp.where(wide < 64, total, 0.0), axis=1, keepdims=True)
        hi = jnp.sum(jnp.where(wide < 64, 0.0, total), axis=1, keepdims=True)
        return lo, hi

    def inner_part(p):
        y_rows = [jnp.zeros((8, 128), f32) for _ in range(4)]
        dot = jnp.zeros((8, 128), f32)
        for g in range(8):
            at = slice(g * 64, (g + 1) * 64)
            m = V[at, RANK : RANK + 128] * p[0]
            for l in range(1, 4):
                m = m + V[at, RANK + l * 128 : RANK + (l + 1) * 128] * p[l]
            inner = jnp.sum(m, axis=1, keepdims=True)
            ci = ccol[at, :] * inner
            d = ci * inner
            for b in range(8):
                dot = dot + d[b * 8 : (b + 1) * 8]
            for l in range(4):
                t = V[at, RANK + l * 128 : RANK + (l + 1) * 128] * ci
                for b in range(8):
                    y_rows[l] = y_rows[l] + t[b * 8 : (b + 1) * 8]
        return (
            [jnp.sum(t, axis=0, keepdims=True) for t in y_rows],
            jnp.sum(dot, axis=0, keepdims=True)[:, :1],
        )

    def basis_apply(y_rows):
        for jt in range(4):
            tmp[jt * 128 : (jt + 1) * 128, :] = column(y_rows[jt])

        def body(g, accs):
            out = list(accs)
            for b in range(4):
                at = pl.ds(pl.multiple_of(g * 32 + b * 8, 8), 8)
                col = tmp[at, :]
                for lt in range(LT):
                    out[lt] = out[lt] + BT[at, lt * 128 : (lt + 1) * 128] * col
            return tuple(out)

        accs = lax.fori_loop(0, 16, body, tuple(jnp.zeros((8, 128), f32) for _ in range(LT)))
        rows = [jnp.sum(t, axis=0, keepdims=True) for t in accs]
        tiles = [jnp.concatenate([rows[2 * k + h] for k in range(8)], axis=0) for h in range(2)]
        zero = jnp.zeros((1, 128), f32)
        last = jnp.concatenate([rows[16], rows[18], rows[17], rows[19]] + [zero] * 4, axis=0)
        return jnp.concatenate(tiles + [last], axis=1)

    def set_direction(ph, d):
        vec[1] = d
        dB[ph, c] = unpack(d).astype(bf16)
        d_copy(ph).start()

    NS = float(SAMP * ROWS)
    zrow = jnp.zeros((1, 128), f32)
    res = -(finish_sums(0) * (math.sqrt(F) / NS) + RIDGE * pack(w))
    drain(0, True)
    p0 = basis_dots(res)
    tot = exchange(0, jnp.concatenate(p0 + [zrow, zrow, both(lanes_of(res, res), zrow), zrow], axis=0))
    lo, hi = halves(tot)
    y_rows, py = inner_part([tot[i : i + 1] for i in range(4)])
    rr = lo[6:7]
    prow[...] = tot
    vec[0] = res
    vec[2] = jnp.zeros((8, 384), f32)
    scal[0:1, :] = jnp.broadcast_to(rr, (1, 128))
    scal[1:2, :] = jnp.broadcast_to(rr + py, (1, 128))
    set_direction(1, res + basis_apply(y_rows))

    @pl.loop(0, ITERS)
    def _(it):
        ph = it + 1
        d_recv(ph).wait_recv()
        images(ph, False)
        pieces(ph, False)
        collect(ph)
        start_sums(ph)
        drain(ph, False)
        d, r = vec[1], vec[0]
        q = finish_sums(ph) / NS + RIDGE * d
        bq = basis_dots(q)
        tot = exchange(ph, jnp.concatenate(bq + [
            both(lanes_of(d, q), lanes_of(r, d)),
            both(lanes_of(r, q), lanes_of(q, q)),
            both(lanes_of(r, r), zrow),
            zrow,
        ], axis=0))
        lo, hi = halves(tot)
        step = hi[4:5] / lo[4:5]
        x = vec[2] + step * d
        vec[2] = x

        @pl.when(it == ITERS - 1)
        def _():
            out[...] = unpack(x)

        @pl.when(it < ITERS - 1)
        def _():
            rn = r - step * q
            vec[0] = rn
            pn = prow[...] - step * tot
            prow[...] = pn
            y_rows, py = inner_part([pn[i : i + 1] for i in range(4)])
            rr = lo[6:7] - 2.0 * step * lo[5:6] + step * step * hi[5:6]
            new = rr + py
            beta = new / scal[1:2, 0:1]
            scal[1:2, :] = jnp.broadcast_to(new, (1, 128))
            set_direction(ph + 1, rn + basis_apply(y_rows) + beta * d)

    for t in range(CHUNKS):
        x_send(t).wait_send()

    @pl.when(s < 10)
    def _():
        for i in range(1, FEAT):
            gf_copy(i).wait_send()
        for i in range(1, SAMP):
            gs_copy(i).wait_send()

    @pl.loop(0, ITERS + 1)
    def _(ph):
        for i in range(1, SAMP):
            ar_copy(ph, i).wait_send()
        for i in range(1, FEAT):
            fe_copy(ph, i).wait_send()


def on_device(features, labels, weights, sketch_basis, sketch_values):
    vmem = pl.BlockSpec(memory_space=pltpu.VMEM)
    hbm = pl.BlockSpec(memory_space=pl.ANY)
    V = pltpu.VMEM
    dma = pltpu.SemaphoreType.DMA
    PH = ITERS + 1
    scratch = [
        V((2, HALF, COLS), bf16),
        V((K * COLS, RANK), f32),
        V((RANK, K * COLS), f32),
        V((PH, 2, 16, COLS), bf16),
        V((CHUNKS, YS, 16, PIECE), f32),
        V((CHUNKS, YS, 16, PIECE), bf16),
        V((CHUNKS, YS, 16, PIECE), f32),
        V((ITERS, CHUNKS, YS, 16, PIECE), bf16),
        V((CHUNKS, 16, PIECE), f32),
        V((PH, CHUNKS, YS, 16, PIECE), bf16),
        V((2, 16, COLS), f32),
        V((PH, 16, COLS), f32),
        V((PH, SAMP, 8, 384), f32),
        V((PH, FEAT, 8, 128), f32),
        V((FEAT, 128, 128), f32),
        V((SAMP, 128, 128), f32),
        V((RANK, 2 * RANK), f32),
        V((128, 2 * RANK), f32),
        V((128, 128), f32),
        V((128, 128), f32),
        V((RANK, 128), f32),
        V((RANK, 128), f32),
        V((3, 8, 384), f32),
        V((8, 128), f32),
        V((8, 128), f32),
        dma((CHUNKS,)), dma((CHUNKS,)), dma((CHUNKS,)), dma((K,)),
        dma((PH, CHUNKS, YS)), dma((PH, CHUNKS, YS)), dma((PH, CHUNKS, YS)), dma((PH, CHUNKS, YS)),
        dma((PH,)), dma((PH,)), dma((PH,)), dma((PH,)),
        dma((PH, SAMP)), dma((PH, SAMP)), dma((PH, FEAT)), dma((PH, FEAT)),
        dma((FEAT,)), dma((FEAT,)), dma((SAMP,)), dma((SAMP,)),
    ]
    step = pl.pallas_call(
        kernel,
        out_shape=jax.ShapeDtypeStruct((16, COLS), f32),
        in_specs=[hbm, vmem, vmem, hbm, vmem],
        out_specs=vmem,
        scratch_shapes=scratch,
        compiler_params=pltpu.CompilerParams(
            collective_id=0, has_side_effects=True, vmem_limit_bytes=60 * 1024 * 1024
        ),
        name="newton_step",
    )(
        features,
        labels.reshape(CORES * CHUNKS * YS, PIECE),
        jnp.pad(weights, ((0, 6), (0, 0))),
        sketch_basis.reshape(K * COLS, RANK),
        sketch_values.reshape(4, 128),
    )
    return step[:K]


def solution(mesh):
    in_specs = (P("samp", "feat"), P("samp"), P(None, "feat"), P(None, "feat", None), P())
    return jax.shard_map(
        on_device, mesh=mesh, in_specs=in_specs, out_specs=P(None, "feat"), check_vma=False
    )
```

```python
import functools
import math

import jax
import jax.numpy as jnp
from jax import lax
from jax.experimental import pallas as pl
from jax.experimental.pallas import tpu as pltpu
from jax.sharding import PartitionSpec as P

F = 2048
ITERS = 3
RIDGE = 0.05
SAMP, YS, CORES = 16, 4, 2
FEAT = YS * CORES
ROWS = 16384
HALF = ROWS // CORES
CHUNKS = 4
CROWS = HALF // CHUNKS
PIECE = CROWS // YS
COLS = 256
K = 10
RANK = 512
LT = K * COLS // 128
f32, bf16 = jnp.float32, jnp.bfloat16
HI = lax.Precision.HIGHEST
NT = (((1,), (1,)), ((), ()))
TN = (((0,), (0,)), ((), ()))
OFFS = (0, 4, 7, 9)
FAR_SAMP = sorted(range(1, SAMP), key=lambda i: -(min(i // 4, 4 - i // 4) + min(i % 4, 4 - i % 4)))
FAR_FEAT = (4, 5, 3, 2, 6, 7, 1)


def scoped(name):
    def wrap(fn):
        @functools.wraps(fn)
        def run(*args):
            with jax.named_scope(name):
                return fn(*args)
        return run
    return wrap


def rcopy(src, dst, send, recv, dev):
    return pltpu.make_async_remote_copy(
        src_ref=src, dst_ref=dst, send_sem=send, recv_sem=recv,
        device_id=dev, device_id_type=pl.DeviceIdType.MESH,
    )


def rows_of(n):
    return lax.broadcasted_iota(jnp.int32, (n, 128), 0)


def pack(wide):
    low = wide[8:16]
    third = low[:, :128] + pltpu.roll(low[:, 128:], 2, 0)
    return jnp.concatenate([wide[:8], third], axis=1)


def unpack(packed):
    third = packed[:, 256:]
    row = rows_of(8)
    left = jnp.where(row < 2, third, 0.0)
    right = jnp.where(row < 2, pltpu.roll(third, 6, 0), 0.0)
    return jnp.concatenate([packed[:, :256], jnp.concatenate([left, right], axis=1)], axis=0)


def lane_row(packed, k, h):
    if k < 8:
        return packed[k : k + 1, h * 128 : (h + 1) * 128]
    r = 2 * h + (k - 8)
    return packed[r : r + 1, 256:384]


def column(row):
    return jnp.broadcast_to(row, (128, 128)).T


def lane_bcast(x, j):
    return jnp.broadcast_to(x[:, j : j + 1], (x.shape[0], 128))


@scoped('factor')
def factor_block(A, N):
    diag = [lane_bcast(A[0:8, :], j) for j in range(8)]
    for p in range(16):
        lo = 8 * p
        more = lo + 8 < 128
        if more:
            below = [lane_bcast(A[lo + 8 : 128, :], lo + j) for j in range(8)]
            ahead = [lane_bcast(A[lo + 8 : lo + 16, :], lo + 8 + j) for j in range(8)]
        rs, cs = [], []
        for j in range(8):
            r = lax.rsqrt(diag[j][j : j + 1, :])
            c = diag[j] * r
            for k in range(j + 1, 8):
                diag[k] = diag[k] - c * c[k : k + 1, :]
            rs.append(r)
            cs.append(c)
        arow, nrow = A[lo : lo + 8, :], N[lo : lo + 8, :]
        us, ns = [], []
        for j in range(8):
            us.append(arow[j : j + 1, :] * rs[j])
            ns.append(nrow[j : j + 1, :] * rs[j])
            if j < 7:
                arow = arow - cs[j] * us[j]
                nrow = nrow - cs[j] * ns[j]
        N[lo : lo + 8, :] = jnp.concatenate(ns, axis=0)
        if not more:
            continue
        bs = []
        for j in range(8):
            t = below[j]
            for i in range(j):
                t = t - bs[i] * cs[i][j : j + 1, :]
            bs.append(t * rs[j])
        for k in range(8):
            for j in range(8):
                ahead[k] = ahead[k] - bs[j][:8] * bs[j][k : k + 1, :]
        diag = ahead
        at, nt = A[lo + 8 : 128, :], N[lo + 8 : 128, :]
        for j in range(8):
            at = at - bs[j] * us[j]
            nt = nt - bs[j] * ns[j]
        A[lo + 8 : 128, :] = at
        N[lo + 8 : 128, :] = nt


def kernel(
    feat, labels, weights, basis, svals, out,
    X, bst, BT, dB, imgf, imgb, recvg, recvh, prob, E, Q, Qr, ar, fe,
    lab, gpart, grecv, gall, V, acc, FA, FN, ccol, tmp, vec, prow, scal,
    sx_own, sx_s, sx_r, s_b, rs_s, rs_r, ag_s, ag_r, q_s, q_r, d_s, d_r,
    ar_s, ar_r, fe_s, fe_r, gf_s, gf_r, gs_s, gs_r, gy_s, gy_r, l_s,
):
    s = lax.axis_index("samp")
    f = lax.axis_index("feat")
    y = lax.div(f, CORES)
    c = lax.rem(f, CORES)
    sib = (s, f + 1 - 2 * c)

    def samp_dev(i):
        return lax.rem(s + i, SAMP)

    def feat_dev(i):
        return lax.rem(f + i, FEAT)

    def y_dev(i):
        return lax.rem(y + i, YS)

    for k in range(K):
        pltpu.make_async_copy(basis.at[pl.ds(k * COLS, COLS)], bst.at[pl.ds(k * COLS, COLS)], s_b.at[k]).start()

    def own_rows(t):
        return pl.ds(pl.multiple_of(c * HALF + t * CROWS, CROWS), CROWS)

    def sib_rows(t):
        return pl.ds(pl.multiple_of((1 - c) * HALF + t * CROWS, CROWS), CROWS)

    def x_own(t):
        return pltpu.make_async_copy(feat.at[own_rows(t)], X.at[c, pl.ds(t * CROWS, CROWS)], sx_own.at[t])

    def x_send(t):
        return rcopy(feat.at[sib_rows(t)], X.at[c, pl.ds(t * CROWS, CROWS)], sx_s.at[t], sx_r.at[t], sib)

    def x_recv(t):
        dst = X.at[1 - c, pl.ds(t * CROWS, CROWS)]
        return rcopy(dst, dst, sx_s.at[t], sx_r.at[t], sib)

    def lab_copy(t):
        start = pl.multiple_of(c * HALF + t * CROWS + y * PIECE, PIECE)
        return pltpu.make_async_copy(labels.at[pl.ds(start, PIECE)], lab.at[t, 0], l_s.at[t])

    for t in range(CHUNKS):
        x_own(t).start()
        lab_copy(t).start()

    def d_copy(ph):
        return rcopy(dB.at[ph, c], dB.at[ph, c], d_s.at[ph], d_r.at[ph], sib)

    def d_recv(ph):
        return rcopy(dB.at[ph, 1 - c], dB.at[ph, 1 - c], d_s.at[ph], d_r.at[ph], sib)

    barrier = pltpu.get_barrier_semaphore()
    for i in range(1, FEAT):
        pl.semaphore_signal(barrier, inc=1, device_id=(s, feat_dev(i)), device_id_type=pl.DeviceIdType.MESH)
    for i in range(1, SAMP):
        pl.semaphore_signal(barrier, inc=1, device_id=(samp_dev(i), f), device_id_type=pl.DeviceIdType.MESH)

    w = jnp.concatenate([weights[...], jnp.zeros((16 - K, COLS), f32)], axis=0)
    dB[0, c] = w.astype(bf16)

    @pl.loop(0, K)
    @scoped('transpose')
    def _(k):
        pltpu.make_async_copy(
            basis.at[pl.ds(k * COLS, COLS)], bst.at[pl.ds(k * COLS, COLS)], s_b.at[k]
        ).wait()
        for h in range(2):
            for jt in range(4):
                blk = bst[pl.ds(pl.multiple_of(k * COLS + h * 128, 128), 128), jt * 128 : (jt + 1) * 128]
                BT[jt * 128 : (jt + 1) * 128, pl.ds(pl.multiple_of(k * COLS + h * 128, 128), 128)] = blk.T

    blk_id = lax.min(s, 9)
    ba = sum((blk_id >= e).astype(jnp.int32) for e in (4, 7, 9))
    bb = blk_id - lax.div(ba * (9 - ba), 2) + ba

    with jax.named_scope('gram'):
        block = lax.dot_general(
            BT[pl.ds(pl.multiple_of(ba * 128, 128), 128), :],
            BT[pl.ds(pl.multiple_of(bb * 128, 128), 128), :],
            NT, precision=HI, preferred_element_type=f32,
        )
        for g in range(FEAT):
            gpart[g] = block[g * 16 : (g + 1) * 16]

    def gf_copy(i):
        o = feat_dev(i)
        return rcopy(gpart.at[o], grecv.at[f], gf_s.at[i], gf_r.at[f], (s, o))

    def gf_recv(i):
        o = feat_dev(i)
        return rcopy(grecv.at[o], grecv.at[o], gf_s.at[i], gf_r.at[o], (s, o))

    def gs_copy(i):
        return rcopy(gall.at[f, s], gall.at[f, s], gs_s.at[i], gs_r.at[s], (samp_dev(i), f))

    def gs_recv(o):
        return rcopy(gall.at[f, o], gall.at[f, o], gs_s.at[0], gs_r.at[o], (o, f))

    def gy_copy(kb, i):
        at = pl.ds(OFFS[kb], 4 - kb)
        return rcopy(gall.at[f, at], gall.at[f, at], gy_s.at[kb, i], gy_r.at[kb, f], (s, feat_dev(i)))

    def gy_recv(kb, i):
        at, o = pl.ds(OFFS[kb], 4 - kb), feat_dev(i)
        return rcopy(gall.at[o, at], gall.at[o, at], gy_s.at[kb, i], gy_r.at[kb, o], (s, o))

    with jax.named_scope('barrier'):
        pl.semaphore_wait(barrier, FEAT - 1 + SAMP - 1)

    @pl.when(s < 10)
    def _():
        for i in FAR_FEAT:
            gf_copy(i).start()

    d_copy(0).start()
    for t in range(CHUNKS):
        x_send(t).start()

    @pl.when(s < 10)
    @scoped('gram_sum')
    def _():
        for i in range(1, FEAT):
            gf_recv(i).wait_recv()
        grecv[f] = gpart[f]
        total = grecv[0]
        for o in range(1, FEAT):
            total = total + grecv[o]
        gall[f, s] = total
        for i in FAR_SAMP:
            gs_copy(i).start()

    def rs_copy(ph, t, i, grad):
        o = y_dev(i)
        src = imgf.at[t, o] if grad else imgb.at[t, o]
        dst = recvg.at[t, y] if grad else recvh.at[ph - 1, t, y]
        return rcopy(src, dst, rs_s.at[ph, t, i], rs_r.at[ph, t, y], (s, CORES * o + c))

    def rs_recv(ph, t, i, grad):
        o = y_dev(i)
        dst = recvg.at[t, o] if grad else recvh.at[ph - 1, t, o]
        return rcopy(dst, dst, rs_s.at[ph, t, i], rs_r.at[ph, t, o], (s, CORES * o + c))

    def ag_copy(ph, t, i):
        return rcopy(E.at[ph, t, y], E.at[ph, t, y], ag_s.at[ph, t, i], ag_r.at[ph, t, y], (s, CORES * y_dev(i) + c))

    def ag_recv(ph, t, i):
        o = y_dev(i)
        return rcopy(E.at[ph, t, o], E.at[ph, t, o], ag_s.at[ph, t, i], ag_r.at[ph, t, o], (s, CORES * o + c))

    @scoped('images')
    def images(ph, grad):
        @pl.loop(0, CHUNKS)
        def _(t):
            if grad:
                x_own(t).wait()
                x_recv(t).wait_recv()
            at = pl.ds(pl.multiple_of(t * CROWS, CROWS), CROWS)
            img = lax.dot_general(dB[ph, 0], X[0, at], NT, preferred_element_type=f32)
            img = img + lax.dot_general(dB[ph, 1], X[1, at], NT, preferred_element_type=f32)
            for o in range(YS):
                piece = img[:, o * PIECE : (o + 1) * PIECE]
                imgf[t, o] = piece
                if not grad:
                    imgb[t, o] = piece.astype(bf16)
            for i in range(1, YS):
                rs_copy(ph, t, i, grad).start()

    @scoped('pieces')
    def pieces(ph, grad):
        @pl.loop(0, CHUNKS)
        def _(t):
            total = imgf[t, y]
            for i in range(1, YS):
                rs_recv(ph, t, i, grad).wait_recv()
            for i in range(1, YS):
                o = y_dev(i)
                total = total + (recvg[t, o] if grad else recvh[ph - 1, t, o].astype(f32))
            if grad:
                logits = total / math.sqrt(F)
                row = lax.broadcasted_iota(jnp.int32, (16, PIECE), 0)
                logits = jnp.where(row < K, logits, -jnp.inf)
                top = jnp.max(logits, axis=0, keepdims=True)
                ex = jnp.exp(logits - top)
                pr = ex / jnp.sum(ex, axis=0, keepdims=True)
                prob[t] = pr
                lab_copy(t).wait()
                own = lab[t]
                coeffs = pr - jnp.where(row == own, 1.0, 0.0)
            else:
                pr = prob[t]
                weighted = pr * total
                coeffs = weighted - pr * jnp.sum(weighted, axis=0, keepdims=True)
            E[ph, t, y] = coeffs.astype(bf16)
            for i in range(1, YS):
                ag_copy(ph, t, i).start()

    @scoped('collect')
    def collect(ph):
        Q[...] = jnp.zeros_like(Q)

        @pl.loop(0, CHUNKS)
        def _(t):
            for i in range(1, YS):
                ag_recv(ph, t, i).wait_recv()
            e = jnp.concatenate([E[ph, t, o] for o in range(YS)], axis=1)
            at = pl.ds(pl.multiple_of(t * CROWS, CROWS), CROWS)
            for h in range(2):
                Q[h] = Q[h] + jnp.dot(e, X[h, at], preferred_element_type=f32)

    def q_copy(ph):
        return rcopy(Q.at[1 - c], Qr.at[ph], q_s.at[ph], q_r.at[ph], sib)

    def ar_copy(ph, i):
        return rcopy(ar.at[ph, s], ar.at[ph, s], ar_s.at[ph, i], ar_r.at[ph, s], (samp_dev(i), f))

    def ar_recv(ph, i):
        o = samp_dev(i)
        return rcopy(ar.at[ph, o], ar.at[ph, o], ar_s.at[ph, i], ar_r.at[ph, o], (o, f))

    def fe_copy(ph, i):
        return rcopy(fe.at[ph, f], fe.at[ph, f], fe_s.at[ph, i], fe_r.at[ph, f], (s, feat_dev(i)))

    def fe_recv(ph, i):
        o = feat_dev(i)
        return rcopy(fe.at[ph, o], fe.at[ph, o], fe_s.at[ph, i], fe_r.at[ph, o], (s, o))

    @scoped('sums_start')
    def start_sums(ph):
        q_copy(ph).start()
        q_copy(ph).wait_recv()
        ar[ph, s] = pack(Q[c] + Qr[ph])
        for i in FAR_SAMP:
            ar_copy(ph, i).start()

    @scoped('sums_finish')
    def finish_sums(ph):
        for i in range(1, SAMP):
            ar_recv(ph, i).wait_recv()
        total = ar[ph, 0]
        for o in range(1, SAMP):
            total = total + ar[ph, o]
        return total

    @scoped('drain')
    def drain(ph, grad):
        d_copy(ph).wait_send()
        q_copy(ph).wait_send()

        @pl.loop(0, CHUNKS)
        def _(t):
            for i in range(1, YS):
                rs_copy(ph, t, i, grad).wait_send()
                ag_copy(ph, t, i).wait_send()

    @scoped('exchange')
    def exchange(ph, message):
        fe[ph, f] = message
        for i in FAR_FEAT:
            fe_copy(ph, i).start()
        for i in range(1, FEAT):
            fe_recv(ph, i).wait_recv()
        total = fe[ph, 0]
        for o in range(1, FEAT):
            total = total + fe[ph, o]
        return total

    with jax.named_scope('dwait'):
        d_recv(0).wait_recv()
    images(0, True)

    @scoped('gram_gather')
    def gram_gather():
        for kb in range(4):
            for o in range(OFFS[kb], OFFS[kb] + 4 - kb):
                @pl.when(s != o)
                def _():
                    gs_recv(o).wait_recv()
            for i in FAR_FEAT:
                gy_copy(kb, i).start()

    gram_gather()
    pieces(0, True)

    sv = svals[...]
    low = jnp.min(jnp.min(sv, axis=1, keepdims=True), axis=0, keepdims=True)
    coef = (low + RIDGE) / (sv + RIDGE) - 1.0
    for jt in range(4):
        ccol[jt * 128 : (jt + 1) * 128, :] = column(coef[jt : jt + 1, :])
    eye = jnp.where(rows_of(128) == lax.broadcasted_iota(jnp.int32, (128, 128), 1), 1.0, 0.0).astype(f32)

    def lanes(a, b):
        return slice(a * 128, b * 128)

    def dot_hi(a, b, dims=(((1,), (0,)), ((), ()))):
        return lax.dot_general(a, b, dims, precision=HI, preferred_element_type=f32)

    def gram_block(k, l):
        blk = jnp.concatenate([gall[o, OFFS[k] + l - k] for o in range(FEAT)], axis=0)
        return blk if k == 0 else blk - acc[k, :, lanes(l, l + 1)]

    def add_to(k, i, a, b):
        term = dot_hi(V[k, :, lanes(i, i + 1)], V[k, :, lanes(a, b)], TN)
        first = k == 0 if b <= 4 else k == a - 4
        acc[i, :, lanes(a, b)] = term if first else acc[i, :, lanes(a, b)] + term

    def rest_of(k):
        inv = V[k, :, lanes(4 + k, 5 + k)]
        if k < 2:
            V[k, :, lanes(k + 2, 4)] = dot_hi(inv, jnp.concatenate([gram_block(k, l) for l in range(k + 2, 4)], axis=1))
        if k > 0:
            V[k, :, lanes(4, 4 + k)] = -dot_hi(inv, acc[k, :, lanes(4, 4 + k)])
        for i in range(k + 1, 4):
            if i > k + 1:
                add_to(k, i, i, 4)
            elif i < 3:
                add_to(k, i, i + 1, 4)
            if k > 0:
                add_to(k, i, 4, 4 + k)
            add_to(k, i, 4 + k, 5 + k)

    for kb in range(4):
        with jax.named_scope('chol_wait'):
            for i in range(1, FEAT):
                gy_recv(kb, i).wait_recv()
        with jax.named_scope('chol'):
            FA[...] = gram_block(kb, kb)
            FN[...] = eye
            if kb > 0:
                rest_of(kb - 1)
            factor_block(FA, FN)
            V[kb, :, lanes(4 + kb, 5 + kb)] = FN[...]
            if kb < 3:
                V[kb, :, lanes(kb + 1, kb + 2)] = dot_hi(FN[...], gram_block(kb, kb + 1))
                add_to(kb, kb + 1, kb + 1, kb + 2)
        if kb == 1:
            collect(0)
            start_sums(0)
    rest_of(3)

    @scoped('basis_dots')
    def basis_dots(packed):
        rows = [lane_row(packed, lt // 2, lt % 2) for lt in range(LT)]

        @pl.loop(0, 8)
        def _(g):
            at = pl.ds(pl.multiple_of(g * 64, 64), 64)
            acc = BT[at, 0:128] * rows[0]
            for lt in range(1, LT):
                acc = acc + BT[at, lt * 128 : (lt + 1) * 128] * rows[lt]
            tmp[at, :] = acc

        return [jnp.sum(tmp[jt * 128 : (jt + 1) * 128, :].T, axis=0, keepdims=True) for jt in range(4)]

    def lanes_of(a, b):
        t = a * b
        t = jnp.sum(t[:, :128] + t[:, 128:256] + t[:, 256:], axis=0, keepdims=True)
        return t + pltpu.roll(t, 64, 1)

    lane = lax.broadcasted_iota(jnp.int32, (1, 128), 1)

    def both(x, z):
        return jnp.where(lane < 64, x, z)

    def halves(total):
        wide = lax.broadcasted_iota(jnp.int32, (8, 128), 1)
        lo = jnp.sum(jnp.where(wide < 64, total, 0.0), axis=1, keepdims=True)
        hi = jnp.sum(jnp.where(wide < 64, 0.0, total), axis=1, keepdims=True)
        return lo, hi

    @scoped('inner')
    def inner_part(p):
        y_rows = [jnp.zeros((8, 128), f32) for _ in range(4)]
        dot = jnp.zeros((8, 128), f32)
        for g in range(8):
            kb, at, crow = g // 2, slice((g % 2) * 64, (g % 2) * 64 + 64), slice(g * 64, (g + 1) * 64)
            m = V[kb, at, lanes(4, 5)] * p[0]
            for l in range(1, kb + 1):
                m = m + V[kb, at, lanes(4 + l, 5 + l)] * p[l]
            inner = jnp.sum(m, axis=1, keepdims=True)
            ci = ccol[crow, :] * inner
            d = ci * inner
            for b in range(8):
                dot = dot + d[b * 8 : (b + 1) * 8]
            for l in range(kb + 1):
                t = V[kb, at, lanes(4 + l, 5 + l)] * ci
                for b in range(8):
                    y_rows[l] = y_rows[l] + t[b * 8 : (b + 1) * 8]
        return (
            [jnp.sum(t, axis=0, keepdims=True) for t in y_rows],
            jnp.sum(dot, axis=0, keepdims=True)[:, :1],
        )

    @scoped('basis_apply')
    def basis_apply(y_rows):
        for jt in range(4):
            tmp[jt * 128 : (jt + 1) * 128, :] = column(y_rows[jt])

        def body(g, accs):
            out = list(accs)
            for b in range(4):
                at = pl.ds(pl.multiple_of(g * 32 + b * 8, 8), 8)
                col = tmp[at, :]
                for lt in range(LT):
                    out[lt] = out[lt] + BT[at, lt * 128 : (lt + 1) * 128] * col
            return tuple(out)

        accs = lax.fori_loop(0, 16, body, tuple(jnp.zeros((8, 128), f32) for _ in range(LT)))
        rows = [jnp.sum(t, axis=0, keepdims=True) for t in accs]
        tiles = [jnp.concatenate([rows[2 * k + h] for k in range(8)], axis=0) for h in range(2)]
        zero = jnp.zeros((1, 128), f32)
        last = jnp.concatenate([rows[16], rows[18], rows[17], rows[19]] + [zero] * 4, axis=0)
        return jnp.concatenate(tiles + [last], axis=1)

    def set_direction(ph, d):
        vec[1] = d
        dB[ph, c] = unpack(d).astype(bf16)
        d_copy(ph).start()

    NS = float(SAMP * ROWS)
    zrow = jnp.zeros((1, 128), f32)
    res = -(finish_sums(0) * (math.sqrt(F) / NS) + RIDGE * pack(w))
    drain(0, True)
    p0 = basis_dots(res)
    tot = exchange(0, jnp.concatenate(p0 + [zrow, zrow, both(lanes_of(res, res), zrow), zrow], axis=0))
    lo, hi = halves(tot)
    y_rows, py = inner_part([tot[i : i + 1] for i in range(4)])
    rr = lo[6:7]
    prow[...] = tot
    vec[0] = res
    vec[2] = jnp.zeros((8, 384), f32)
    scal[0:1, :] = jnp.broadcast_to(rr, (1, 128))
    scal[1:2, :] = jnp.broadcast_to(rr + py, (1, 128))
    set_direction(1, res + basis_apply(y_rows))

    @pl.loop(0, ITERS)
    def _(it):
        ph = it + 1
        with jax.named_scope('dwait'):
            d_recv(ph).wait_recv()
        images(ph, False)
        pieces(ph, False)
        collect(ph)
        start_sums(ph)
        drain(ph, False)
        d, r = vec[1], vec[0]
        q = finish_sums(ph) / NS + RIDGE * d
        bq = basis_dots(q)
        tot = exchange(ph, jnp.concatenate(bq + [
            both(lanes_of(d, q), lanes_of(r, d)),
            both(lanes_of(r, q), lanes_of(q, q)),
            both(lanes_of(r, r), zrow),
            zrow,
        ], axis=0))
        lo, hi = halves(tot)
        step = hi[4:5] / lo[4:5]
        x = vec[2] + step * d
        vec[2] = x

        @pl.when(it == ITERS - 1)
        def _():
            out[...] = unpack(x)[:K]

        @pl.when(it < ITERS - 1)
        def _():
            rn = r - step * q
            vec[0] = rn
            pn = prow[...] - step * tot
            prow[...] = pn
            y_rows, py = inner_part([pn[i : i + 1] for i in range(4)])
            rr = lo[6:7] - 2.0 * step * lo[5:6] + step * step * hi[5:6]
            new = rr + py
            beta = new / scal[1:2, 0:1]
            scal[1:2, :] = jnp.broadcast_to(new, (1, 128))
            set_direction(ph + 1, rn + basis_apply(y_rows) + beta * d)

    for t in range(CHUNKS):
        x_send(t).wait_send()

    @pl.when(s < 10)
    def _():
        for i in range(1, FEAT):
            gf_copy(i).wait_send()
        for i in range(1, SAMP):
            gs_copy(i).wait_send()

    for kb in range(4):
        for i in range(1, FEAT):
            gy_copy(kb, i).wait_send()

    @pl.loop(0, ITERS + 1)
    def _(ph):
        for i in range(1, SAMP):
            ar_copy(ph, i).wait_send()
        for i in range(1, FEAT):
            fe_copy(ph, i).wait_send()


def on_device(features, labels, weights, sketch_basis, sketch_values):
    vmem = pl.BlockSpec(memory_space=pltpu.VMEM)
    hbm = pl.BlockSpec(memory_space=pl.ANY)
    V = pltpu.VMEM
    dma = pltpu.SemaphoreType.DMA
    PH = ITERS + 1
    scratch = [
        V((2, HALF, COLS), bf16),
        V((K * COLS, RANK), f32),
        V((RANK, K * COLS), f32),
        V((PH, 2, 16, COLS), bf16),
        V((CHUNKS, YS, 16, PIECE), f32),
        V((CHUNKS, YS, 16, PIECE), bf16),
        V((CHUNKS, YS, 16, PIECE), f32),
        V((ITERS, CHUNKS, YS, 16, PIECE), bf16),
        V((CHUNKS, 16, PIECE), f32),
        V((PH, CHUNKS, YS, 16, PIECE), bf16),
        V((2, 16, COLS), f32),
        V((PH, 16, COLS), f32),
        V((PH, SAMP, 8, 384), f32),
        V((PH, FEAT, 8, 128), f32),
        V((CHUNKS, 1, PIECE), jnp.int32),
        V((FEAT, 16, 128), f32),
        V((FEAT, 16, 128), f32),
        V((FEAT, SAMP, 16, 128), f32),
        V((4, 128, 2 * RANK), f32),
        V((4, 128, 2 * RANK), f32),
        V((128, 128), f32),
        V((128, 128), f32),
        V((RANK, 128), f32),
        V((RANK, 128), f32),
        V((3, 8, 384), f32),
        V((8, 128), f32),
        V((8, 128), f32),
        dma((CHUNKS,)), dma((CHUNKS,)), dma((CHUNKS,)), dma((K,)),
        dma((PH, CHUNKS, YS)), dma((PH, CHUNKS, YS)), dma((PH, CHUNKS, YS)), dma((PH, CHUNKS, YS)),
        dma((PH,)), dma((PH,)), dma((PH,)), dma((PH,)),
        dma((PH, SAMP)), dma((PH, SAMP)), dma((PH, FEAT)), dma((PH, FEAT)),
        dma((FEAT,)), dma((FEAT,)), dma((SAMP,)), dma((SAMP,)),
        dma((4, FEAT)), dma((4, FEAT)), dma((CHUNKS,)),
    ]
    step = pl.pallas_call(
        kernel,
        out_shape=jax.ShapeDtypeStruct((K, COLS), f32),
        in_specs=[hbm, hbm, vmem, hbm, vmem],
        out_specs=vmem,
        scratch_shapes=scratch,
        compiler_params=pltpu.CompilerParams(
            collective_id=0, has_side_effects=True, vmem_limit_bytes=60 * 1024 * 1024
        ),
        name="newton_step",
    )(
        features,
        labels,
        weights,
        sketch_basis.reshape(K * COLS, RANK),
        sketch_values.reshape(4, 128),
    )
    return step


def solution(mesh):
    in_specs = (P("samp", "feat"), P("samp"), P(None, "feat"), P(None, "feat", None), P())
    return jax.shard_map(
        on_device, mesh=mesh, in_specs=in_specs, out_specs=P(None, "feat"), check_vma=False
    )
```

```python
import functools
import math

import jax
import jax.numpy as jnp
from jax import lax
from jax.experimental import pallas as pl
from jax.experimental.pallas import tpu as pltpu
from jax.sharding import PartitionSpec as P

F = 2048
ITERS = 3
RIDGE = 0.05
SAMP, YS, CORES = 16, 4, 2
FEAT = YS * CORES
ROWS = 16384
HALF = ROWS // CORES
CHUNKS = 4
CROWS = HALF // CHUNKS
PIECE = CROWS // YS
PWIDE = PIECE + 128
COLS = 256
K = 10
RANK = 512
LT = K * COLS // 128
f32, bf16 = jnp.float32, jnp.bfloat16
HI = lax.Precision.HIGHEST
NT = (((1,), (1,)), ((), ()))
TN = (((0,), (0,)), ((), ()))
OFFS = (0, 4, 7, 9)
MSGS = ((0, 1), (1, 3), (4, 3), (7, 2), (9, 1))
FAR_SAMP = sorted(range(1, SAMP), key=lambda i: -(min(i // 4, 4 - i // 4) + min(i % 4, 4 - i % 4)))
FAR_FEAT = (4, 5, 3, 2, 6, 7, 1)


def scoped(name):
    def wrap(fn):
        @functools.wraps(fn)
        def run(*args):
            with jax.named_scope(name):
                return fn(*args)
        return run
    return wrap


def rcopy(src, dst, send, recv, dev):
    return pltpu.make_async_remote_copy(
        src_ref=src, dst_ref=dst, send_sem=send, recv_sem=recv,
        device_id=dev, device_id_type=pl.DeviceIdType.MESH,
    )


def rows_of(n):
    return lax.broadcasted_iota(jnp.int32, (n, 128), 0)


def pack(wide):
    low = wide[8:16]
    third = low[:, :128] + pltpu.roll(low[:, 128:], 2, 0)
    return jnp.concatenate([wide[:8], third], axis=1)


def unpack(packed):
    third = packed[:, 256:]
    row = rows_of(8)
    left = jnp.where(row < 2, third, 0.0)
    right = jnp.where(row < 2, pltpu.roll(third, 6, 0), 0.0)
    return jnp.concatenate([packed[:, :256], jnp.concatenate([left, right], axis=1)], axis=0)


def pack_piece(wide):
    low = wide[8:16]
    last = low[:, :128]
    for q in range(1, PIECE // 128):
        last = last + pltpu.roll(low[:, q * 128 : (q + 1) * 128], 2 * q, 0)
    return jnp.concatenate([wide[:8], last], axis=1)


def unpack_piece(packed):
    last = packed[:, PIECE:]
    row = rows_of(8)
    low = [
        jnp.where(row < 2, pltpu.roll(last, (8 - 2 * q) % 8, 0) if q else last, 0.0) for q in range(PIECE // 128)
    ]
    return jnp.concatenate([packed[:, :PIECE], jnp.concatenate(low, axis=1)], axis=0)


def spread_piece(packed):
    last = packed[:, PIECE:]
    row = rows_of(8)
    low = [jnp.where((row >= 2 * q) & (row < 2 * q + 2), last, 0.0) for q in range(PIECE // 128)]
    return jnp.concatenate([packed[:, :PIECE], jnp.concatenate(low, axis=1)], axis=0)


def fold_rows(wide):
    low = wide[8:16]
    low = low + pltpu.roll(low, 4, 0)
    low = low + pltpu.roll(low, 2, 0)
    row = lax.broadcasted_iota(jnp.int32, low.shape, 0)
    return jnp.concatenate([wide[:8], jnp.where(row < 2, low, 0.0)], axis=0)


def lane_row(packed, k, h):
    if k < 8:
        return packed[k : k + 1, h * 128 : (h + 1) * 128]
    r = 2 * h + (k - 8)
    return packed[r : r + 1, 256:384]


def column(row):
    return jnp.broadcast_to(row, (128, 128)).T


def lane_bcast(x, j):
    return jnp.broadcast_to(x[:, j : j + 1], (x.shape[0], 128))


@scoped('factor')
def factor_block(A, N):
    diag = [lane_bcast(A[0:8, :], j) for j in range(8)]
    for p in range(16):
        lo = 8 * p
        more = lo + 8 < 128
        if more:
            below = [lane_bcast(A[lo + 8 : 128, :], lo + j) for j in range(8)]
            ahead = [lane_bcast(A[lo + 8 : lo + 16, :], lo + 8 + j) for j in range(8)]
        rs, cs = [], []
        for j in range(8):
            r = lax.rsqrt(diag[j][j : j + 1, :])
            c = diag[j] * r
            for k in range(j + 1, 8):
                diag[k] = diag[k] - c * c[k : k + 1, :]
            rs.append(r)
            cs.append(c)
        arow, nrow = A[lo : lo + 8, :], N[lo : lo + 8, :]
        us, ns = [], []
        for j in range(8):
            us.append(arow[j : j + 1, :] * rs[j])
            ns.append(nrow[j : j + 1, :] * rs[j])
            if j < 7:
                arow = arow - cs[j] * us[j]
                nrow = nrow - cs[j] * ns[j]
        N[lo : lo + 8, :] = jnp.concatenate(ns, axis=0)
        if not more:
            continue
        bs = []
        for j in range(8):
            t = below[j]
            for i in range(j):
                t = t - bs[i] * cs[i][j : j + 1, :]
            bs.append(t * rs[j])
        for k in range(8):
            for j in range(8):
                ahead[k] = ahead[k] - bs[j][:8] * bs[j][k : k + 1, :]
        diag = ahead
        at, nt = A[lo + 8 : 128, :], N[lo + 8 : 128, :]
        for j in range(8):
            at = at - bs[j] * us[j]
            nt = nt - bs[j] * ns[j]
        A[lo + 8 : 128, :] = at
        N[lo + 8 : 128, :] = nt


def kernel(
    feat, labels, weights, basis, svals, out,
    X, bst, BT, dB, imgf, imgb, recvg, recvh, prob, E, Q, Qr, ar, dots, fe,
    lab, gpart, grecv, gall, V, acc, FA, FN, ccol, tmp, vec, prow, scal,
    sx_own, sx_s, sx_r, s_b, rs_s, rs_r, ag_s, ag_r, q_s, q_r, d_s, d_r,
    ar_s, ar_r, fe_s, fe_r, gf_s, gf_r, gs_s, gs_r, gy_s, gy_r, l_s,
):
    s = lax.axis_index("samp")
    f = lax.axis_index("feat")
    y = lax.div(f, CORES)
    c = lax.rem(f, CORES)
    sib = (s, f + 1 - 2 * c)

    def samp_dev(i):
        return lax.rem(s + i, SAMP)

    def feat_dev(i):
        return lax.rem(f + i, FEAT)

    def y_dev(i):
        return lax.rem(y + i, YS)

    for k in range(K):
        pltpu.make_async_copy(basis.at[pl.ds(k * COLS, COLS)], bst.at[pl.ds(k * COLS, COLS)], s_b.at[k]).start()

    def own_rows(t):
        return pl.ds(pl.multiple_of(c * HALF + t * CROWS, CROWS), CROWS)

    def sib_rows(t):
        return pl.ds(pl.multiple_of((1 - c) * HALF + t * CROWS, CROWS), CROWS)

    def x_own(t):
        return pltpu.make_async_copy(feat.at[own_rows(t)], X.at[c, pl.ds(t * CROWS, CROWS)], sx_own.at[t])

    def x_send(t):
        return rcopy(feat.at[sib_rows(t)], X.at[c, pl.ds(t * CROWS, CROWS)], sx_s.at[t], sx_r.at[t], sib)

    def x_recv(t):
        dst = X.at[1 - c, pl.ds(t * CROWS, CROWS)]
        return rcopy(dst, dst, sx_s.at[t], sx_r.at[t], sib)

    def lab_copy(t):
        start = pl.multiple_of(c * HALF + t * CROWS + y * PIECE, PIECE)
        return pltpu.make_async_copy(labels.at[pl.ds(start, PIECE)], lab.at[t, 0], l_s.at[t])


    def d_copy(ph):
        return rcopy(dB.at[ph, c], dB.at[ph, c], d_s.at[ph], d_r.at[ph], sib)

    def d_recv(ph):
        return rcopy(dB.at[ph, 1 - c], dB.at[ph, 1 - c], d_s.at[ph], d_r.at[ph], sib)

    barrier = pltpu.get_barrier_semaphore()
    for i in range(1, FEAT):
        pl.semaphore_signal(barrier, inc=1, device_id=(s, feat_dev(i)), device_id_type=pl.DeviceIdType.MESH)
    for i in range(1, SAMP):
        pl.semaphore_signal(barrier, inc=1, device_id=(samp_dev(i), f), device_id_type=pl.DeviceIdType.MESH)

    w = jnp.concatenate([weights[...], jnp.zeros((16 - K, COLS), f32)], axis=0)
    dB[0, c] = w.astype(bf16)

    @pl.loop(0, K)
    @scoped('transpose')
    def _(k):
        pltpu.make_async_copy(
            basis.at[pl.ds(k * COLS, COLS)], bst.at[pl.ds(k * COLS, COLS)], s_b.at[k]
        ).wait()
        for h in range(2):
            for jt in range(4):
                blk = bst[pl.ds(pl.multiple_of(k * COLS + h * 128, 128), 128), jt * 128 : (jt + 1) * 128]
                BT[jt * 128 : (jt + 1) * 128, pl.ds(pl.multiple_of(k * COLS + h * 128, 128), 128)] = blk.T

    for t in range(CHUNKS):
        x_own(t).start()
        lab_copy(t).start()

    blk_id = lax.min(s, 9)
    ba = sum((blk_id >= e).astype(jnp.int32) for e in (4, 7, 9))
    bb = blk_id - lax.div(ba * (9 - ba), 2) + ba

    with jax.named_scope('gram'):
        block = lax.dot_general(
            BT[pl.ds(pl.multiple_of(ba * 128, 128), 128), :],
            BT[pl.ds(pl.multiple_of(bb * 128, 128), 128), :],
            NT, precision=HI, preferred_element_type=f32,
        )
        for g in range(FEAT):
            gpart[g] = block[g * 16 : (g + 1) * 16]

    def gf_copy(i):
        o = feat_dev(i)
        return rcopy(gpart.at[o], grecv.at[f], gf_s.at[i], gf_r.at[f], (s, o))

    def gf_recv(i):
        o = feat_dev(i)
        return rcopy(grecv.at[o], grecv.at[o], gf_s.at[i], gf_r.at[o], (s, o))

    def gs_copy(i):
        return rcopy(gall.at[f, s], gall.at[f, s], gs_s.at[i], gs_r.at[s], (samp_dev(i), f))

    def gs_recv(o):
        return rcopy(gall.at[f, o], gall.at[f, o], gs_s.at[0], gs_r.at[o], (o, f))

    def gy_copy(m, i):
        at = pl.ds(*MSGS[m])
        return rcopy(gall.at[f, at], gall.at[f, at], gy_s.at[m, i], gy_r.at[m, f], (s, feat_dev(i)))

    def gy_recv(m, i):
        at, o = pl.ds(*MSGS[m]), feat_dev(i)
        return rcopy(gall.at[o, at], gall.at[o, at], gy_s.at[m, i], gy_r.at[m, o], (s, o))

    with jax.named_scope('barrier'):
        pl.semaphore_wait(barrier, FEAT - 1 + SAMP - 1)

    @pl.when(s < 10)
    def _():
        for i in FAR_FEAT:
            gf_copy(i).start()

    d_copy(0).start()
    for t in range(CHUNKS):
        x_send(t).start()

    @pl.when(s < 10)
    @scoped('gram_sum')
    def _():
        for i in range(1, FEAT):
            gf_recv(i).wait_recv()
        grecv[f] = gpart[f]
        total = grecv[0]
        for o in range(1, FEAT):
            total = total + grecv[o]
        gall[f, s] = total
        for i in FAR_SAMP:
            gs_copy(i).start()

    def rs_copy(ph, t, i, grad):
        o = y_dev(i)
        src = imgf.at[t, o] if grad else imgb.at[t, o]
        dst = recvg.at[t, y] if grad else recvh.at[ph - 1, t, y]
        return rcopy(src, dst, rs_s.at[ph, t, i], rs_r.at[ph, t, y], (s, CORES * o + c))

    def rs_recv(ph, t, i, grad):
        o = y_dev(i)
        dst = recvg.at[t, o] if grad else recvh.at[ph - 1, t, o]
        return rcopy(dst, dst, rs_s.at[ph, t, i], rs_r.at[ph, t, o], (s, CORES * o + c))

    def ag_copy(ph, t, i):
        return rcopy(E.at[ph, t, y], E.at[ph, t, y], ag_s.at[ph, t, i], ag_r.at[ph, t, y], (s, CORES * y_dev(i) + c))

    def ag_recv(ph, t, i):
        o = y_dev(i)
        return rcopy(E.at[ph, t, o], E.at[ph, t, o], ag_s.at[ph, t, i], ag_r.at[ph, t, o], (s, CORES * o + c))

    @scoped('images')
    def images(ph, grad):
        @pl.loop(0, CHUNKS)
        def _(t):
            at = pl.ds(pl.multiple_of(t * CROWS, CROWS), CROWS)
            if grad:
                x_own(t).wait()
            img = lax.dot_general(dB[ph, c], X[c, at], NT, preferred_element_type=f32)

            @pl.when(t == 0)
            def _():
                d_recv(ph).wait_recv()

            if grad:
                x_recv(t).wait_recv()
            img = img + lax.dot_general(dB[ph, 1 - c], X[1 - c, at], NT, preferred_element_type=f32)
            for o in range(YS):
                piece = pack_piece(img[:, o * PIECE : (o + 1) * PIECE])
                imgf[t, o] = piece
                if not grad:
                    imgb[t, o] = piece.astype(bf16)
            for i in range(1, YS):
                rs_copy(ph, t, i, grad).start()

    @scoped('pieces')
    def pieces(ph, grad):
        @pl.loop(0, CHUNKS)
        def _(t):
            total = imgf[t, y]
            for i in range(1, YS):
                rs_recv(ph, t, i, grad).wait_recv()
            for i in range(1, YS):
                o = y_dev(i)
                total = total + (recvg[t, o] if grad else recvh[ph - 1, t, o].astype(f32))
            total = unpack_piece(total)
            if grad:
                logits = total / math.sqrt(F)
                row = lax.broadcasted_iota(jnp.int32, (16, PIECE), 0)
                logits = jnp.where(row < K, logits, -jnp.inf)
                top = jnp.max(logits, axis=0, keepdims=True)
                ex = jnp.exp(logits - top)
                pr = ex / jnp.sum(ex, axis=0, keepdims=True)
                prob[t] = pr
                lab_copy(t).wait()
                own = lab[t]
                coeffs = pr - jnp.where(row == own, 1.0, 0.0)
            else:
                pr = prob[t]
                weighted = pr * total
                coeffs = weighted - pr * jnp.sum(weighted, axis=0, keepdims=True)
            E[ph, t, y] = pack_piece(coeffs).astype(bf16)
            for i in range(1, YS):
                ag_copy(ph, t, i).start()

    @scoped('collect')
    def collect(ph):
        Q[...] = jnp.zeros_like(Q)

        @pl.loop(0, CHUNKS)
        def _(t):
            for i in range(1, YS):
                ag_recv(ph, t, i).wait_recv()
            e = jnp.concatenate([spread_piece(E[ph, t, o].astype(f32)) for o in range(YS)], axis=1).astype(bf16)
            at = pl.ds(pl.multiple_of(t * CROWS, CROWS), CROWS)
            for h in range(2):
                Q[h] = Q[h] + jnp.dot(e, X[h, at], preferred_element_type=f32)

        for h in range(2):
            Q[h] = fold_rows(Q[h])

    def q_copy(ph):
        return rcopy(Q.at[1 - c], Qr.at[ph], q_s.at[ph], q_r.at[ph], sib)

    def ar_copy(ph, i):
        return rcopy(ar.at[ph, s], ar.at[ph, s], ar_s.at[ph, i], ar_r.at[ph, s], (samp_dev(i), f))

    def ar_recv(ph, i):
        o = samp_dev(i)
        return rcopy(ar.at[ph, o], ar.at[ph, o], ar_s.at[ph, i], ar_r.at[ph, o], (o, f))

    def fe_copy(ph, i):
        return rcopy(fe.at[ph, f], fe.at[ph, f], fe_s.at[ph, i], fe_r.at[ph, f], (s, feat_dev(i)))

    def fe_recv(ph, i):
        o = feat_dev(i)
        return rcopy(fe.at[ph, o], fe.at[ph, o], fe_s.at[ph, i], fe_r.at[ph, o], (s, o))

    def chip_sum(ph):
        q_copy(ph).start()
        q_copy(ph).wait_recv()
        return pack(Q[c] + Qr[ph])

    @scoped('sums_start')
    def start_sums(ph):
        ar[ph, s] = chip_sum(ph)
        for i in range(1, SAMP):
            ar_copy(ph, i).start()

    @scoped('sums_finish')
    def finish_sums(ph):
        for i in range(1, SAMP):
            ar_recv(ph, i).wait_recv()
        total = ar[ph, 0]
        for o in range(1, SAMP):
            total = total + ar[ph, o]
        return total

    def last_copy(i):
        return rcopy(dots.at[s], dots.at[s], ar_s.at[ITERS, i], ar_r.at[ITERS, s], (samp_dev(i), f))

    def last_recv(i):
        o = samp_dev(i)
        return rcopy(dots.at[o], dots.at[o], ar_s.at[ITERS, i], ar_r.at[ITERS, o], (o, f))

    @scoped('sums_last')
    def sums_last(message):
        dots[s] = message
        for i in range(1, SAMP):
            last_copy(i).start()
        drain(ITERS, False)
        for i in range(1, SAMP):
            last_recv(i).wait_recv()
        total = dots[0]
        for o in range(1, SAMP):
            total = total + dots[o]
        return total

    @scoped('drain')
    def drain(ph, grad):
        d_copy(ph).wait_send()
        q_copy(ph).wait_send()

        @pl.loop(0, CHUNKS)
        def _(t):
            for i in range(1, YS):
                rs_copy(ph, t, i, grad).wait_send()
                ag_copy(ph, t, i).wait_send()

    @scoped('exchange')
    def exchange(ph, message):
        fe[ph, f] = message
        for i in FAR_FEAT:
            fe_copy(ph, i).start()
        for i in range(1, FEAT):
            fe_recv(ph, i).wait_recv()
        total = fe[ph, 0]
        for o in range(1, FEAT):
            total = total + fe[ph, o]
        return total

    images(0, True)

    @scoped('gram_gather')
    def gram_gather():
        for m, (start, count) in enumerate(MSGS):
            for o in range(start, start + count):
                @pl.when(s != o)
                def _():
                    gs_recv(o).wait_recv()
            for i in FAR_FEAT:
                gy_copy(m, i).start()

    gram_gather()
    pieces(0, True)

    sv = svals[...]
    low = jnp.min(jnp.min(sv, axis=1, keepdims=True), axis=0, keepdims=True)
    coef = (low + RIDGE) / (sv + RIDGE) - 1.0
    for jt in range(4):
        ccol[jt * 128 : (jt + 1) * 128, :] = column(coef[jt : jt + 1, :])
    eye = jnp.where(rows_of(128) == lax.broadcasted_iota(jnp.int32, (128, 128), 1), 1.0, 0.0).astype(f32)

    def lanes(a, b):
        return slice(a * 128, b * 128)

    def dot_hi(a, b, dims=(((1,), (0,)), ((), ()))):
        return lax.dot_general(a, b, dims, precision=HI, preferred_element_type=f32)

    def gram_block(k, l):
        blk = jnp.concatenate([gall[o, OFFS[k] + l - k] for o in range(FEAT)], axis=0)
        return blk if k == 0 else blk - acc[k, :, lanes(l, l + 1)]

    def add_to(k, i, a, b):
        term = dot_hi(V[k, :, lanes(i, i + 1)], V[k, :, lanes(a, b)], TN)
        first = k == 0 if b <= 4 else k == a - 4
        acc[i, :, lanes(a, b)] = term if first else acc[i, :, lanes(a, b)] + term

    def rest_of(k):
        inv = V[k, :, lanes(4 + k, 5 + k)]
        if k < 2:
            V[k, :, lanes(k + 2, 4)] = dot_hi(inv, jnp.concatenate([gram_block(k, l) for l in range(k + 2, 4)], axis=1))
        if k > 0:
            V[k, :, lanes(4, 4 + k)] = -dot_hi(inv, acc[k, :, lanes(4, 4 + k)])
        for i in range(k + 1, 4):
            if i > k + 1:
                add_to(k, i, i, 4)
            elif i < 3:
                add_to(k, i, i + 1, 4)
            if k > 0:
                add_to(k, i, 4, 4 + k)
            add_to(k, i, 4 + k, 5 + k)

    for kb in range(4):
        with jax.named_scope('chol_wait'):
            for i in range(1, FEAT):
                gy_recv(kb + 1 if kb else 0, i).wait_recv()
        with jax.named_scope('chol'):
            FA[...] = gram_block(kb, kb)
            FN[...] = eye
            if kb > 0:
                rest_of(kb - 1)
            factor_block(FA, FN)
            V[kb, :, lanes(4 + kb, 5 + kb)] = FN[...]
            if kb == 0:
                for i in range(1, FEAT):
                    gy_recv(1, i).wait_recv()
            if kb < 3:
                V[kb, :, lanes(kb + 1, kb + 2)] = dot_hi(FN[...], gram_block(kb, kb + 1))
                add_to(kb, kb + 1, kb + 1, kb + 2)
        if kb == 1:
            collect(0)
            start_sums(0)
    rest_of(3)

    @scoped('basis_dots')
    def basis_dots(packed):
        rows = [lane_row(packed, lt // 2, lt % 2) for lt in range(LT)]

        @pl.loop(0, 8)
        def _(g):
            at = pl.ds(pl.multiple_of(g * 64, 64), 64)
            acc = BT[at, 0:128] * rows[0]
            for lt in range(1, LT):
                acc = acc + BT[at, lt * 128 : (lt + 1) * 128] * rows[lt]
            tmp[at, :] = acc

        return [jnp.sum(tmp[jt * 128 : (jt + 1) * 128, :].T, axis=0, keepdims=True) for jt in range(4)]

    def lanes_of(a, b):
        t = a * b
        t = jnp.sum(t[:, :128] + t[:, 128:256] + t[:, 256:], axis=0, keepdims=True)
        return t + pltpu.roll(t, 64, 1)

    lane = lax.broadcasted_iota(jnp.int32, (1, 128), 1)

    def both(x, z):
        return jnp.where(lane < 64, x, z)

    def halves(total):
        wide = lax.broadcasted_iota(jnp.int32, (8, 128), 1)
        lo = jnp.sum(jnp.where(wide < 64, total, 0.0), axis=1, keepdims=True)
        hi = jnp.sum(jnp.where(wide < 64, 0.0, total), axis=1, keepdims=True)
        return lo, hi

    @scoped('inner')
    def inner_part(p):
        y_rows = [jnp.zeros((8, 128), f32) for _ in range(4)]
        dot = jnp.zeros((8, 128), f32)
        for g in range(8):
            kb, at, crow = g // 2, slice((g % 2) * 64, (g % 2) * 64 + 64), slice(g * 64, (g + 1) * 64)
            m = V[kb, at, lanes(4, 5)] * p[0]
            for l in range(1, kb + 1):
                m = m + V[kb, at, lanes(4 + l, 5 + l)] * p[l]
            inner = jnp.sum(m, axis=1, keepdims=True)
            ci = ccol[crow, :] * inner
            d = ci * inner
            for b in range(8):
                dot = dot + d[b * 8 : (b + 1) * 8]
            for l in range(kb + 1):
                t = V[kb, at, lanes(4 + l, 5 + l)] * ci
                for b in range(8):
                    y_rows[l] = y_rows[l] + t[b * 8 : (b + 1) * 8]
        return (
            [jnp.sum(t, axis=0, keepdims=True) for t in y_rows],
            jnp.sum(dot, axis=0, keepdims=True)[:, :1],
        )

    @scoped('basis_apply')
    def basis_apply(y_rows):
        for jt in range(4):
            tmp[jt * 128 : (jt + 1) * 128, :] = column(y_rows[jt])

        def body(g, accs):
            out = list(accs)
            for b in range(4):
                at = pl.ds(pl.multiple_of(g * 32 + b * 8, 8), 8)
                col = tmp[at, :]
                for lt in range(LT):
                    out[lt] = out[lt] + BT[at, lt * 128 : (lt + 1) * 128] * col
            return tuple(out)

        accs = lax.fori_loop(0, 16, body, tuple(jnp.zeros((8, 128), f32) for _ in range(LT)))
        rows = [jnp.sum(t, axis=0, keepdims=True) for t in accs]
        tiles = [jnp.concatenate([rows[2 * k + h] for k in range(8)], axis=0) for h in range(2)]
        zero = jnp.zeros((1, 128), f32)
        last = jnp.concatenate([rows[16], rows[18], rows[17], rows[19]] + [zero] * 4, axis=0)
        return jnp.concatenate(tiles + [last], axis=1)

    def set_direction(ph, d):
        vec[1] = d
        dB[ph, c] = unpack(d).astype(bf16)
        d_copy(ph).start()

    NS = float(SAMP * ROWS)
    zrow = jnp.zeros((1, 128), f32)
    res = -(finish_sums(0) * (math.sqrt(F) / NS) + RIDGE * pack(w))
    drain(0, True)
    p0 = basis_dots(res)
    tot = exchange(0, jnp.concatenate(p0 + [zrow, zrow, both(lanes_of(res, res), zrow), zrow], axis=0))
    lo, hi = halves(tot)
    y_rows, py = inner_part([tot[i : i + 1] for i in range(4)])
    rr = lo[6:7]
    prow[...] = tot
    vec[0] = res
    vec[2] = jnp.zeros((8, 384), f32)
    scal[0:1, :] = jnp.broadcast_to(rr, (1, 128))
    scal[1:2, :] = jnp.broadcast_to(rr + py, (1, 128))
    set_direction(1, res + basis_apply(y_rows))

    @pl.loop(0, ITERS)
    def _(it):
        ph = it + 1
        images(ph, False)
        pieces(ph, False)
        collect(ph)

        @pl.when(it == ITERS - 1)
        def _():
            d, r = vec[1], vec[0]
            dq = sums_last(jnp.broadcast_to(lanes_of(d, chip_sum(ITERS)), (8, 128)))[0:1]
            dq = dq / NS + RIDGE * lanes_of(d, d)
            lo, hi = halves(exchange(ITERS, jnp.broadcast_to(both(dq, lanes_of(r, d)), (8, 128))))
            out[...] = unpack(vec[2] + hi[0:1] / lo[0:1] * d)[:K]

        @pl.when(it < ITERS - 1)
        def _():
            start_sums(ph)
            drain(ph, False)
            d, r = vec[1], vec[0]
            q = finish_sums(ph) / NS + RIDGE * d
            bq = basis_dots(q)
            tot = exchange(ph, jnp.concatenate(bq + [
                both(lanes_of(d, q), lanes_of(r, d)),
                both(lanes_of(r, q), lanes_of(q, q)),
                both(lanes_of(r, r), zrow),
                zrow,
            ], axis=0))
            lo, hi = halves(tot)
            step = hi[4:5] / lo[4:5]
            vec[2] = vec[2] + step * d
            rn = r - step * q
            vec[0] = rn
            pn = prow[...] - step * tot
            prow[...] = pn
            y_rows, py = inner_part([pn[i : i + 1] for i in range(4)])
            rr = lo[6:7] - 2.0 * step * lo[5:6] + step * step * hi[5:6]
            new = rr + py
            beta = new / scal[1:2, 0:1]
            scal[1:2, :] = jnp.broadcast_to(new, (1, 128))
            set_direction(ph + 1, rn + basis_apply(y_rows) + beta * d)

    for t in range(CHUNKS):
        x_send(t).wait_send()

    @pl.when(s < 10)
    def _():
        for i in range(1, FEAT):
            gf_copy(i).wait_send()
        for i in range(1, SAMP):
            gs_copy(i).wait_send()

    for m in range(len(MSGS)):
        for i in range(1, FEAT):
            gy_copy(m, i).wait_send()

    for i in range(1, SAMP):
        last_copy(i).wait_send()

    @pl.loop(0, ITERS + 1)
    def _(ph):
        @pl.when(ph < ITERS)
        def _():
            for i in range(1, SAMP):
                ar_copy(ph, i).wait_send()
        for i in range(1, FEAT):
            fe_copy(ph, i).wait_send()


def on_device(features, labels, weights, sketch_basis, sketch_values):
    vmem = pl.BlockSpec(memory_space=pltpu.VMEM)
    hbm = pl.BlockSpec(memory_space=pl.ANY)
    V = pltpu.VMEM
    dma = pltpu.SemaphoreType.DMA
    PH = ITERS + 1
    scratch = [
        V((2, HALF, COLS), bf16),
        V((K * COLS, RANK), f32),
        V((RANK, K * COLS), f32),
        V((PH, 2, 16, COLS), bf16),
        V((CHUNKS, YS, 8, PWIDE), f32),
        V((CHUNKS, YS, 8, PWIDE), bf16),
        V((CHUNKS, YS, 8, PWIDE), f32),
        V((ITERS, CHUNKS, YS, 8, PWIDE), bf16),
        V((CHUNKS, 16, PIECE), f32),
        V((PH, CHUNKS, YS, 8, PWIDE), bf16),
        V((2, 16, COLS), f32),
        V((PH, 16, COLS), f32),
        V((ITERS, SAMP, 8, 384), f32),
        V((SAMP, 8, 128), f32),
        V((PH, FEAT, 8, 128), f32),
        V((CHUNKS, 1, PIECE), jnp.int32),
        V((FEAT, 16, 128), f32),
        V((FEAT, 16, 128), f32),
        V((FEAT, SAMP, 16, 128), f32),
        V((4, 128, 2 * RANK), f32),
        V((4, 128, 2 * RANK), f32),
        V((128, 128), f32),
        V((128, 128), f32),
        V((RANK, 128), f32),
        V((RANK, 128), f32),
        V((3, 8, 384), f32),
        V((8, 128), f32),
        V((8, 128), f32),
        dma((CHUNKS,)), dma((CHUNKS,)), dma((CHUNKS,)), dma((K,)),
        dma((PH, CHUNKS, YS)), dma((PH, CHUNKS, YS)), dma((PH, CHUNKS, YS)), dma((PH, CHUNKS, YS)),
        dma((PH,)), dma((PH,)), dma((PH,)), dma((PH,)),
        dma((PH, SAMP)), dma((PH, SAMP)), dma((PH, FEAT)), dma((PH, FEAT)),
        dma((FEAT,)), dma((FEAT,)), dma((SAMP,)), dma((SAMP,)),
        dma((5, FEAT)), dma((5, FEAT)), dma((CHUNKS,)),
    ]
    step = pl.pallas_call(
        kernel,
        out_shape=jax.ShapeDtypeStruct((K, COLS), f32),
        in_specs=[hbm, hbm, vmem, hbm, vmem],
        out_specs=vmem,
        scratch_shapes=scratch,
        compiler_params=pltpu.CompilerParams(
            collective_id=0, has_side_effects=True, vmem_limit_bytes=60 * 1024 * 1024
        ),
        name="newton_step",
    )(
        features,
        labels,
        weights,
        sketch_basis.reshape(K * COLS, RANK),
        sketch_values.reshape(4, 128),
    )
    return step


def solution(mesh):
    in_specs = (P("samp", "feat"), P("samp"), P(None, "feat"), P(None, "feat", None), P())
    return jax.shard_map(
        on_device, mesh=mesh, in_specs=in_specs, out_specs=P(None, "feat"), check_vma=False
    )
```

```python
import functools
import math

import jax
import jax.numpy as jnp
from jax import lax
from jax.experimental import pallas as pl
from jax.experimental.pallas import tpu as pltpu
from jax.sharding import PartitionSpec as P

F = 2048
ITERS = 3
RIDGE = 0.05
SAMP, YS, CORES = 16, 4, 2
FEAT = YS * CORES
ROWS = 16384
HALF = ROWS // CORES
CHUNKS = 4
CROWS = HALF // CHUNKS
PIECE = CROWS // YS
PTILES = PIECE // 128
PWIDE = PIECE + (PTILES + 3) // 4 * 128
COLS = 256
K = 10
RANK = 512
LT = K * COLS // 128
f32, bf16 = jnp.float32, jnp.bfloat16
HI = lax.Precision.HIGHEST
NT = (((1,), (1,)), ((), ()))
TN = (((0,), (0,)), ((), ()))
OFFS = (0, 4, 7, 9)
MSGS = ((0, 1), (1, 3), (4, 3), (7, 2), (9, 1))
FAR_SAMP = sorted(range(1, SAMP), key=lambda i: -(min(i // 4, 4 - i // 4) + min(i % 4, 4 - i % 4)))
FAR_FEAT = (4, 5, 3, 2, 6, 7, 1)


def scoped(name):
    def wrap(fn):
        @functools.wraps(fn)
        def run(*args):
            with jax.named_scope(name):
                return fn(*args)
        return run
    return wrap


def rcopy(src, dst, send, recv, dev):
    return pltpu.make_async_remote_copy(
        src_ref=src, dst_ref=dst, send_sem=send, recv_sem=recv,
        device_id=dev, device_id_type=pl.DeviceIdType.MESH,
    )


def rows_of(n):
    return lax.broadcasted_iota(jnp.int32, (n, 128), 0)


def pack(wide):
    low = wide[8:16]
    third = low[:, :128] + pltpu.roll(low[:, 128:], 2, 0)
    return jnp.concatenate([wide[:8], third], axis=1)


def unpack(packed):
    third = packed[:, 256:]
    row = rows_of(8)
    left = jnp.where(row < 2, third, 0.0)
    right = jnp.where(row < 2, pltpu.roll(third, 6, 0), 0.0)
    return jnp.concatenate([packed[:, :256], jnp.concatenate([left, right], axis=1)], axis=0)


def pack_piece(wide):
    low = wide[8:16]
    tiles = [wide[:8]]
    for e in range(0, PTILES, 4):
        last = low[:, e * 128 : (e + 1) * 128]
        for q in range(e + 1, min(e + 4, PTILES)):
            last = last + pltpu.roll(low[:, q * 128 : (q + 1) * 128], 2 * (q - e), 0)
        tiles.append(last)
    return jnp.concatenate(tiles, axis=1)


def shared_tile(packed, q):
    at = PIECE + q // 4 * 128
    return packed[:, at : at + 128]


def unpack_piece(packed):
    row = rows_of(8)
    low = []
    for q in range(PTILES):
        tile = shared_tile(packed, q)
        low.append(jnp.where(row < 2, pltpu.roll(tile, 8 - 2 * (q % 4), 0) if q % 4 else tile, 0.0))
    return jnp.concatenate([packed[:, :PIECE], jnp.concatenate(low, axis=1)], axis=0)


def spread_piece(packed):
    row = rows_of(8)
    low = [
        jnp.where((row >= 2 * (q % 4)) & (row < 2 * (q % 4) + 2), shared_tile(packed, q), 0.0) for q in range(PTILES)
    ]
    return jnp.concatenate([packed[:, :PIECE], jnp.concatenate(low, axis=1)], axis=0)


def fold_rows(wide):
    low = wide[8:16]
    low = low + pltpu.roll(low, 4, 0)
    low = low + pltpu.roll(low, 2, 0)
    row = lax.broadcasted_iota(jnp.int32, low.shape, 0)
    return jnp.concatenate([wide[:8], jnp.where(row < 2, low, 0.0)], axis=0)


def lane_row(packed, k, h):
    if k < 8:
        return packed[k : k + 1, h * 128 : (h + 1) * 128]
    r = 2 * h + (k - 8)
    return packed[r : r + 1, 256:384]


def column(row):
    return jnp.broadcast_to(row, (128, 128)).T


def lane_bcast(x, j):
    return jnp.broadcast_to(x[:, j : j + 1], (x.shape[0], 128))


@scoped('factor')
def factor_block(A, N):
    diag = [lane_bcast(A[0:8, :], j) for j in range(8)]
    for p in range(16):
        lo = 8 * p
        more = lo + 8 < 128
        if more:
            below = [lane_bcast(A[lo + 8 : 128, :], lo + j) for j in range(8)]
            ahead = [lane_bcast(A[lo + 8 : lo + 16, :], lo + 8 + j) for j in range(8)]
        rs, cs = [], []
        for j in range(8):
            r = lax.rsqrt(diag[j][j : j + 1, :])
            c = diag[j] * r
            for k in range(j + 1, 8):
                diag[k] = diag[k] - c * c[k : k + 1, :]
            rs.append(r)
            cs.append(c)
        arow, nrow = A[lo : lo + 8, :], N[lo : lo + 8, :]
        us, ns = [], []
        for j in range(8):
            us.append(arow[j : j + 1, :] * rs[j])
            ns.append(nrow[j : j + 1, :] * rs[j])
            if j < 7:
                arow = arow - cs[j] * us[j]
                nrow = nrow - cs[j] * ns[j]
        N[lo : lo + 8, :] = jnp.concatenate(ns, axis=0)
        if not more:
            continue
        bs = []
        for j in range(8):
            t = below[j]
            for i in range(j):
                t = t - bs[i] * cs[i][j : j + 1, :]
            bs.append(t * rs[j])
        for k in range(8):
            for j in range(8):
                ahead[k] = ahead[k] - bs[j][:8] * bs[j][k : k + 1, :]
        diag = ahead
        at, nt = A[lo + 8 : 128, :], N[lo + 8 : 128, :]
        for j in range(8):
            at = at - bs[j] * us[j]
            nt = nt - bs[j] * ns[j]
        A[lo + 8 : 128, :] = at
        N[lo + 8 : 128, :] = nt


def kernel(
    feat, labels, weights, basis, svals, out,
    X, own, bst, BT, dB, imgf, imgb, recvg, recvh, prob, E, Q, Qr, ar, dots, fe,
    lab, gpart, grecv, gall, V, acc, FA, FN, ccol, tmp, vec, prow, scal,
    sx_own, sx_s, sx_r, s_b, rs_s, rs_r, ag_s, ag_r, q_s, q_r, d_s, d_r,
    ar_s, ar_r, fe_s, fe_r, gf_s, gf_r, gs_s, gs_r, gy_s, gy_r, l_s,
):
    s = lax.axis_index("samp")
    f = lax.axis_index("feat")
    y = lax.div(f, CORES)
    c = lax.rem(f, CORES)
    sib = (s, f + 1 - 2 * c)

    def samp_dev(i):
        return lax.rem(s + i, SAMP)

    def feat_dev(i):
        return lax.rem(f + i, FEAT)

    def y_dev(i):
        return lax.rem(y + i, YS)

    for k in range(K):
        pltpu.make_async_copy(basis.at[pl.ds(k * COLS, COLS)], bst.at[pl.ds(k * COLS, COLS)], s_b.at[k]).start()

    def own_rows(t):
        return pl.ds(pl.multiple_of(c * HALF + t * CROWS, CROWS), CROWS)

    def sib_rows(t):
        return pl.ds(pl.multiple_of((1 - c) * HALF + t * CROWS, CROWS), CROWS)

    def x_own(t):
        return pltpu.make_async_copy(feat.at[own_rows(t)], X.at[c, pl.ds(t * CROWS, CROWS)], sx_own.at[t])

    def x_send(t):
        return rcopy(feat.at[sib_rows(t)], X.at[c, pl.ds(t * CROWS, CROWS)], sx_s.at[t], sx_r.at[t], sib)

    def x_recv(t):
        dst = X.at[1 - c, pl.ds(t * CROWS, CROWS)]
        return rcopy(dst, dst, sx_s.at[t], sx_r.at[t], sib)

    def lab_copy(t):
        start = pl.multiple_of(c * HALF + t * CROWS + y * PIECE, PIECE)
        return pltpu.make_async_copy(labels.at[pl.ds(start, PIECE)], lab.at[t, 0], l_s.at[t])


    def d_copy(ph):
        return rcopy(dB.at[ph, c], dB.at[ph, c], d_s.at[ph], d_r.at[ph], sib)

    def d_recv(ph):
        return rcopy(dB.at[ph, 1 - c], dB.at[ph, 1 - c], d_s.at[ph], d_r.at[ph], sib)

    barrier = pltpu.get_barrier_semaphore()
    for i in range(1, FEAT):
        pl.semaphore_signal(barrier, inc=1, device_id=(s, feat_dev(i)), device_id_type=pl.DeviceIdType.MESH)
    for i in range(1, SAMP):
        pl.semaphore_signal(barrier, inc=1, device_id=(samp_dev(i), f), device_id_type=pl.DeviceIdType.MESH)

    w = jnp.concatenate([weights[...], jnp.zeros((16 - K, COLS), f32)], axis=0)
    dB[0, c] = w.astype(bf16)

    @pl.loop(0, K)
    @scoped('transpose')
    def _(k):
        pltpu.make_async_copy(
            basis.at[pl.ds(k * COLS, COLS)], bst.at[pl.ds(k * COLS, COLS)], s_b.at[k]
        ).wait()
        for h in range(2):
            for jt in range(4):
                blk = bst[pl.ds(pl.multiple_of(k * COLS + h * 128, 128), 128), jt * 128 : (jt + 1) * 128]
                BT[jt * 128 : (jt + 1) * 128, pl.ds(pl.multiple_of(k * COLS + h * 128, 128), 128)] = blk.T

    for t in range(CHUNKS):
        x_own(t).start()
        lab_copy(t).start()

    blk_id = lax.min(s, 9)
    ba = sum((blk_id >= e).astype(jnp.int32) for e in (4, 7, 9))
    bb = blk_id - lax.div(ba * (9 - ba), 2) + ba

    with jax.named_scope('gram'):
        block = lax.dot_general(
            BT[pl.ds(pl.multiple_of(ba * 128, 128), 128), :],
            BT[pl.ds(pl.multiple_of(bb * 128, 128), 128), :],
            NT, precision=HI, preferred_element_type=f32,
        )
        for g in range(FEAT):
            gpart[g] = block[g * 16 : (g + 1) * 16]

    def gf_copy(i):
        o = feat_dev(i)
        return rcopy(gpart.at[o], grecv.at[f], gf_s.at[i], gf_r.at[f], (s, o))

    def gf_recv(i):
        o = feat_dev(i)
        return rcopy(grecv.at[o], grecv.at[o], gf_s.at[i], gf_r.at[o], (s, o))

    def gs_copy(i):
        return rcopy(gall.at[f, s], gall.at[f, s], gs_s.at[i], gs_r.at[s], (samp_dev(i), f))

    def gs_recv(o):
        return rcopy(gall.at[f, o], gall.at[f, o], gs_s.at[0], gs_r.at[o], (o, f))

    def gy_copy(m, i):
        at = pl.ds(*MSGS[m])
        return rcopy(gall.at[f, at], gall.at[f, at], gy_s.at[m, i], gy_r.at[m, f], (s, feat_dev(i)))

    def gy_recv(m, i):
        at, o = pl.ds(*MSGS[m]), feat_dev(i)
        return rcopy(gall.at[o, at], gall.at[o, at], gy_s.at[m, i], gy_r.at[m, o], (s, o))

    with jax.named_scope('barrier'):
        pl.semaphore_wait(barrier, FEAT - 1 + SAMP - 1)

    @pl.when(s < 10)
    def _():
        for i in FAR_FEAT:
            gf_copy(i).start()

    d_copy(0).start()
    for t in range(CHUNKS):
        x_send(t).start()

    @pl.when(s < 10)
    @scoped('gram_sum')
    def _():
        for i in range(1, FEAT):
            gf_recv(i).wait_recv()
        grecv[f] = gpart[f]
        total = grecv[0]
        for o in range(1, FEAT):
            total = total + grecv[o]
        gall[f, s] = total
        for i in FAR_SAMP:
            gs_copy(i).start()

    def rs_copy(ph, t, i, grad):
        o = y_dev(i)
        src = imgf.at[t, o] if grad else imgb.at[t, o]
        dst = recvg.at[t, y] if grad else recvh.at[ph - 1, t, y]
        return rcopy(src, dst, rs_s.at[ph, t, i], rs_r.at[ph, t, y], (s, CORES * o + c))

    def rs_recv(ph, t, i, grad):
        o = y_dev(i)
        dst = recvg.at[t, o] if grad else recvh.at[ph - 1, t, o]
        return rcopy(dst, dst, rs_s.at[ph, t, i], rs_r.at[ph, t, o], (s, CORES * o + c))

    def ag_copy(ph, t, i):
        return rcopy(E.at[ph, t, y], E.at[ph, t, y], ag_s.at[ph, t, i], ag_r.at[ph, t, y], (s, CORES * y_dev(i) + c))

    def ag_recv(ph, t, i):
        o = y_dev(i)
        return rcopy(E.at[ph, t, o], E.at[ph, t, o], ag_s.at[ph, t, i], ag_r.at[ph, t, o], (s, CORES * o + c))

    @scoped('images')
    def images(ph, grad):
        for t in range(CHUNKS):
            at = slice(t * CROWS, (t + 1) * CROWS)
            if grad:
                x_own(t).wait()
            own[t] = lax.dot_general(dB[ph, c], X[c, at], NT, preferred_element_type=f32)
        d_recv(ph).wait_recv()
        for t in range(CHUNKS):
            at = slice(t * CROWS, (t + 1) * CROWS)
            if grad:
                x_recv(t).wait_recv()
            img = own[t] + lax.dot_general(dB[ph, 1 - c], X[1 - c, at], NT, preferred_element_type=f32)
            for o in range(YS):
                piece = pack_piece(img[:, o * PIECE : (o + 1) * PIECE])
                imgf[t, o] = piece
                if not grad:
                    imgb[t, o] = piece.astype(bf16)
            for i in range(1, YS):
                rs_copy(ph, t, i, grad).start()

    @scoped('pieces')
    def pieces(ph, grad):
        @pl.loop(0, CHUNKS)
        def _(t):
            total = imgf[t, y]
            for i in range(1, YS):
                rs_recv(ph, t, i, grad).wait_recv()
            for i in range(1, YS):
                o = y_dev(i)
                total = total + (recvg[t, o] if grad else recvh[ph - 1, t, o].astype(f32))
            total = unpack_piece(total)
            if grad:
                logits = total / math.sqrt(F)
                row = lax.broadcasted_iota(jnp.int32, (16, PIECE), 0)
                logits = jnp.where(row < K, logits, -jnp.inf)
                top = jnp.max(logits, axis=0, keepdims=True)
                ex = jnp.exp(logits - top)
                pr = ex / jnp.sum(ex, axis=0, keepdims=True)
                prob[t] = pr
                lab_copy(t).wait()
                mine = lab[t]
                coeffs = pr - jnp.where(row == mine, 1.0, 0.0)
            else:
                pr = prob[t]
                weighted = pr * total
                coeffs = weighted - pr * jnp.sum(weighted, axis=0, keepdims=True)
            E[ph, t, y] = pack_piece(coeffs).astype(bf16)
            for i in range(1, YS):
                ag_copy(ph, t, i).start()

    @scoped('collect')
    def collect(ph):
        Q[...] = jnp.zeros_like(Q)

        @pl.loop(0, CHUNKS)
        def _(t):
            for i in range(1, YS):
                ag_recv(ph, t, i).wait_recv()
            e = jnp.concatenate([spread_piece(E[ph, t, o].astype(f32)) for o in range(YS)], axis=1).astype(bf16)
            at = pl.ds(pl.multiple_of(t * CROWS, CROWS), CROWS)
            for h in range(2):
                Q[h] = Q[h] + jnp.dot(e, X[h, at], preferred_element_type=f32)

        for h in range(2):
            Q[h] = fold_rows(Q[h])

    def q_copy(ph):
        return rcopy(Q.at[1 - c], Qr.at[ph], q_s.at[ph], q_r.at[ph], sib)

    def ar_copy(ph, i):
        return rcopy(ar.at[ph, s], ar.at[ph, s], ar_s.at[ph, i], ar_r.at[ph, s], (samp_dev(i), f))

    def ar_recv(ph, i):
        o = samp_dev(i)
        return rcopy(ar.at[ph, o], ar.at[ph, o], ar_s.at[ph, i], ar_r.at[ph, o], (o, f))

    def fe_copy(ph, i):
        return rcopy(fe.at[ph, f], fe.at[ph, f], fe_s.at[ph, i], fe_r.at[ph, f], (s, feat_dev(i)))

    def fe_recv(ph, i):
        o = feat_dev(i)
        return rcopy(fe.at[ph, o], fe.at[ph, o], fe_s.at[ph, i], fe_r.at[ph, o], (s, o))

    def chip_sum(ph):
        q_copy(ph).start()
        q_copy(ph).wait_recv()
        return pack(Q[c] + Qr[ph])

    @scoped('sums_start')
    def start_sums(ph):
        ar[ph, s] = chip_sum(ph)
        for i in range(1, SAMP):
            ar_copy(ph, i).start()

    @scoped('sums_finish')
    def finish_sums(ph):
        for i in range(1, SAMP):
            ar_recv(ph, i).wait_recv()
        total = ar[ph, 0]
        for o in range(1, SAMP):
            total = total + ar[ph, o]
        return total

    def last_copy(i):
        return rcopy(dots.at[s], dots.at[s], ar_s.at[ITERS, i], ar_r.at[ITERS, s], (samp_dev(i), f))

    def last_recv(i):
        o = samp_dev(i)
        return rcopy(dots.at[o], dots.at[o], ar_s.at[ITERS, i], ar_r.at[ITERS, o], (o, f))

    @scoped('sums_last')
    def sums_last(message):
        dots[s] = message
        for i in range(1, SAMP):
            last_copy(i).start()
        drain(ITERS, False)
        for i in range(1, SAMP):
            last_recv(i).wait_recv()
        total = dots[0]
        for o in range(1, SAMP):
            total = total + dots[o]
        return total

    @scoped('drain')
    def drain(ph, grad):
        d_copy(ph).wait_send()
        q_copy(ph).wait_send()

        @pl.loop(0, CHUNKS)
        def _(t):
            for i in range(1, YS):
                rs_copy(ph, t, i, grad).wait_send()
                ag_copy(ph, t, i).wait_send()

    def send_sums(ph, message):
        fe[ph, f] = message
        for i in FAR_FEAT:
            fe_copy(ph, i).start()

    @scoped('exchange')
    def take_sums(ph):
        for i in range(1, FEAT):
            fe_recv(ph, i).wait_recv()
        total = fe[ph, 0]
        for o in range(1, FEAT):
            total = total + fe[ph, o]
        return total

    def exchange(ph, message):
        send_sums(ph, message)
        return take_sums(ph)

    images(0, True)

    @scoped('gram_gather')
    def gram_gather(first, last):
        for m in range(first, last):
            start, count = MSGS[m]
            for o in range(start, start + count):
                @pl.when(s != o)
                def _():
                    gs_recv(o).wait_recv()
            for i in FAR_FEAT:
                gy_copy(m, i).start()

    gram_gather(0, 2)
    pieces(0, True)
    gram_gather(2, 5)

    sv = svals[...]
    low = jnp.min(jnp.min(sv, axis=1, keepdims=True), axis=0, keepdims=True)
    coef = (low + RIDGE) / (sv + RIDGE) - 1.0
    for jt in range(4):
        ccol[jt * 128 : (jt + 1) * 128, :] = column(coef[jt : jt + 1, :])
    eye = jnp.where(rows_of(128) == lax.broadcasted_iota(jnp.int32, (128, 128), 1), 1.0, 0.0).astype(f32)

    def lanes(a, b):
        return slice(a * 128, b * 128)

    def dot_hi(a, b, dims=(((1,), (0,)), ((), ()))):
        return lax.dot_general(a, b, dims, precision=HI, preferred_element_type=f32)

    def gram_block(k, l):
        blk = jnp.concatenate([gall[o, OFFS[k] + l - k] for o in range(FEAT)], axis=0)
        return blk if k == 0 else blk - acc[k, :, lanes(l, l + 1)]

    def add_to(k, i, a, b):
        term = dot_hi(V[k, :, lanes(i, i + 1)], V[k, :, lanes(a, b)], TN)
        first = k == 0 if b <= 4 else k == a - 4
        acc[i, :, lanes(a, b)] = term if first else acc[i, :, lanes(a, b)] + term

    def rest_of(k):
        inv = V[k, :, lanes(4 + k, 5 + k)]
        if k < 2:
            V[k, :, lanes(k + 2, 4)] = dot_hi(inv, jnp.concatenate([gram_block(k, l) for l in range(k + 2, 4)], axis=1))
        if k > 0:
            V[k, :, lanes(4, 4 + k)] = -dot_hi(inv, acc[k, :, lanes(4, 4 + k)])
        for i in range(k + 1, 4):
            if i > k + 1:
                add_to(k, i, i, 4)
            elif i < 3:
                add_to(k, i, i + 1, 4)
            if k > 0:
                add_to(k, i, 4, 4 + k)
            add_to(k, i, 4 + k, 5 + k)

    @scoped('basis_dots')
    def basis_dots(packed):
        rows = [lane_row(packed, lt // 2, lt % 2) for lt in range(LT)]

        @pl.loop(0, 8)
        def _(g):
            at = pl.ds(pl.multiple_of(g * 64, 64), 64)
            acc = BT[at, 0:128] * rows[0]
            for lt in range(1, LT):
                acc = acc + BT[at, lt * 128 : (lt + 1) * 128] * rows[lt]
            tmp[at, :] = acc

        return [jnp.sum(tmp[jt * 128 : (jt + 1) * 128, :].T, axis=0, keepdims=True) for jt in range(4)]

    def lanes_of(a, b):
        t = a * b
        t = jnp.sum(t[:, :128] + t[:, 128:256] + t[:, 256:], axis=0, keepdims=True)
        return t + pltpu.roll(t, 64, 1)

    lane = lax.broadcasted_iota(jnp.int32, (1, 128), 1)

    def both(x, z):
        return jnp.where(lane < 64, x, z)

    def halves(total):
        wide = lax.broadcasted_iota(jnp.int32, (8, 128), 1)
        lo = jnp.sum(jnp.where(wide < 64, total, 0.0), axis=1, keepdims=True)
        hi = jnp.sum(jnp.where(wide < 64, 0.0, total), axis=1, keepdims=True)
        return lo, hi

    @scoped('inner')
    def inner_part(p):
        y_rows = [jnp.zeros((8, 128), f32) for _ in range(4)]
        dot = jnp.zeros((8, 128), f32)
        for g in range(8):
            kb, at, crow = g // 2, slice((g % 2) * 64, (g % 2) * 64 + 64), slice(g * 64, (g + 1) * 64)
            m = V[kb, at, lanes(4, 5)] * p[0]
            for l in range(1, kb + 1):
                m = m + V[kb, at, lanes(4 + l, 5 + l)] * p[l]
            inner = jnp.sum(m, axis=1, keepdims=True)
            ci = ccol[crow, :] * inner
            d = ci * inner
            for b in range(8):
                dot = dot + d[b * 8 : (b + 1) * 8]
            for l in range(kb + 1):
                t = V[kb, at, lanes(4 + l, 5 + l)] * ci
                for b in range(8):
                    y_rows[l] = y_rows[l] + t[b * 8 : (b + 1) * 8]
        return (
            [jnp.sum(t, axis=0, keepdims=True) for t in y_rows],
            jnp.sum(dot, axis=0, keepdims=True)[:, :1],
        )

    @scoped('basis_apply')
    def basis_apply(y_rows):
        for jt in range(4):
            tmp[jt * 128 : (jt + 1) * 128, :] = column(y_rows[jt])

        def body(g, accs):
            out = list(accs)
            for b in range(4):
                at = pl.ds(pl.multiple_of(g * 32 + b * 8, 8), 8)
                col = tmp[at, :]
                for lt in range(LT):
                    out[lt] = out[lt] + BT[at, lt * 128 : (lt + 1) * 128] * col
            return tuple(out)

        accs = lax.fori_loop(0, 16, body, tuple(jnp.zeros((8, 128), f32) for _ in range(LT)))
        rows = [jnp.sum(t, axis=0, keepdims=True) for t in accs]
        tiles = [jnp.concatenate([rows[2 * k + h] for k in range(8)], axis=0) for h in range(2)]
        zero = jnp.zeros((1, 128), f32)
        last = jnp.concatenate([rows[16], rows[18], rows[17], rows[19]] + [zero] * 4, axis=0)
        return jnp.concatenate(tiles + [last], axis=1)

    def set_direction(ph, d):
        vec[1] = d
        dB[ph, c] = unpack(d).astype(bf16)
        d_copy(ph).start()

    NS = float(SAMP * ROWS)
    zrow = jnp.zeros((1, 128), f32)
    for kb in range(4):
        with jax.named_scope('chol_wait'):
            for i in range(1, FEAT):
                gy_recv(kb + 1 if kb else 0, i).wait_recv()
        with jax.named_scope('chol'):
            FA[...] = gram_block(kb, kb)
            FN[...] = eye
            if kb > 0:
                rest_of(kb - 1)
            factor_block(FA, FN)
            V[kb, :, lanes(4 + kb, 5 + kb)] = FN[...]
            if kb == 0:
                for i in range(1, FEAT):
                    gy_recv(1, i).wait_recv()
            if kb < 3:
                V[kb, :, lanes(kb + 1, kb + 2)] = dot_hi(FN[...], gram_block(kb, kb + 1))
                add_to(kb, kb + 1, kb + 1, kb + 2)
        if kb == 0:
            collect(0)
            start_sums(0)
        if kb == 2:
            res = -(finish_sums(0) * (math.sqrt(F) / NS) + RIDGE * pack(w))
            vec[0] = res
            send_sums(0, jnp.concatenate(
                basis_dots(res) + [zrow, zrow, both(lanes_of(res, res), zrow), zrow], axis=0
            ))
    rest_of(3)

    drain(0, True)
    tot = take_sums(0)
    lo, hi = halves(tot)
    y_rows, py = inner_part([tot[i : i + 1] for i in range(4)])
    rr = lo[6:7]
    prow[...] = tot
    vec[2] = jnp.zeros((8, 384), f32)
    scal[0:1, :] = jnp.broadcast_to(rr, (1, 128))
    scal[1:2, :] = jnp.broadcast_to(rr + py, (1, 128))
    set_direction(1, vec[0] + basis_apply(y_rows))

    @pl.loop(0, ITERS)
    def _(it):
        ph = it + 1
        images(ph, False)
        pieces(ph, False)
        collect(ph)

        @pl.when(it == ITERS - 1)
        def _():
            d, r = vec[1], vec[0]
            dq = sums_last(jnp.broadcast_to(lanes_of(d, chip_sum(ITERS)), (8, 128)))[0:1]
            dq = dq / NS + RIDGE * lanes_of(d, d)
            lo, hi = halves(exchange(ITERS, jnp.broadcast_to(both(dq, lanes_of(r, d)), (8, 128))))
            out[...] = unpack(vec[2] + hi[0:1] / lo[0:1] * d)[:K]

        @pl.when(it < ITERS - 1)
        def _():
            start_sums(ph)
            drain(ph, False)
            d, r = vec[1], vec[0]
            q = finish_sums(ph) / NS + RIDGE * d
            bq = basis_dots(q)
            tot = exchange(ph, jnp.concatenate(bq + [
                both(lanes_of(d, q), lanes_of(r, d)),
                both(lanes_of(r, q), lanes_of(q, q)),
                both(lanes_of(r, r), zrow),
                zrow,
            ], axis=0))
            lo, hi = halves(tot)
            step = hi[4:5] / lo[4:5]
            vec[2] = vec[2] + step * d
            rn = r - step * q
            vec[0] = rn
            pn = prow[...] - step * tot
            prow[...] = pn
            y_rows, py = inner_part([pn[i : i + 1] for i in range(4)])
            rr = lo[6:7] - 2.0 * step * lo[5:6] + step * step * hi[5:6]
            new = rr + py
            beta = new / scal[1:2, 0:1]
            scal[1:2, :] = jnp.broadcast_to(new, (1, 128))
            set_direction(ph + 1, rn + basis_apply(y_rows) + beta * d)

    for t in range(CHUNKS):
        x_send(t).wait_send()

    @pl.when(s < 10)
    def _():
        for i in range(1, FEAT):
            gf_copy(i).wait_send()
        for i in range(1, SAMP):
            gs_copy(i).wait_send()

    for m in range(len(MSGS)):
        for i in range(1, FEAT):
            gy_copy(m, i).wait_send()

    for i in range(1, SAMP):
        last_copy(i).wait_send()

    @pl.loop(0, ITERS + 1)
    def _(ph):
        @pl.when(ph < ITERS)
        def _():
            for i in range(1, SAMP):
                ar_copy(ph, i).wait_send()
        for i in range(1, FEAT):
            fe_copy(ph, i).wait_send()


def on_device(features, labels, weights, sketch_basis, sketch_values):
    vmem = pl.BlockSpec(memory_space=pltpu.VMEM)
    hbm = pl.BlockSpec(memory_space=pl.ANY)
    V = pltpu.VMEM
    dma = pltpu.SemaphoreType.DMA
    PH = ITERS + 1
    scratch = [
        V((2, HALF, COLS), bf16),
        V((CHUNKS, 16, CROWS), f32),
        V((K * COLS, RANK), f32),
        V((RANK, K * COLS), f32),
        V((PH, 2, 16, COLS), bf16),
        V((CHUNKS, YS, 8, PWIDE), f32),
        V((CHUNKS, YS, 8, PWIDE), bf16),
        V((CHUNKS, YS, 8, PWIDE), f32),
        V((ITERS, CHUNKS, YS, 8, PWIDE), bf16),
        V((CHUNKS, 16, PIECE), f32),
        V((PH, CHUNKS, YS, 8, PWIDE), bf16),
        V((2, 16, COLS), f32),
        V((PH, 16, COLS), f32),
        V((ITERS, SAMP, 8, 384), f32),
        V((SAMP, 8, 128), f32),
        V((PH, FEAT, 8, 128), f32),
        V((CHUNKS, 1, PIECE), jnp.int32),
        V((FEAT, 16, 128), f32),
        V((FEAT, 16, 128), f32),
        V((FEAT, SAMP, 16, 128), f32),
        V((4, 128, 2 * RANK), f32),
        V((4, 128, 2 * RANK), f32),
        V((128, 128), f32),
        V((128, 128), f32),
        V((RANK, 128), f32),
        V((RANK, 128), f32),
        V((3, 8, 384), f32),
        V((8, 128), f32),
        V((8, 128), f32),
        dma((CHUNKS,)), dma((CHUNKS,)), dma((CHUNKS,)), dma((K,)),
        dma((PH, CHUNKS, YS)), dma((PH, CHUNKS, YS)), dma((PH, CHUNKS, YS)), dma((PH, CHUNKS, YS)),
        dma((PH,)), dma((PH,)), dma((PH,)), dma((PH,)),
        dma((PH, SAMP)), dma((PH, SAMP)), dma((PH, FEAT)), dma((PH, FEAT)),
        dma((FEAT,)), dma((FEAT,)), dma((SAMP,)), dma((SAMP,)),
        dma((5, FEAT)), dma((5, FEAT)), dma((CHUNKS,)),
    ]
    step = pl.pallas_call(
        kernel,
        out_shape=jax.ShapeDtypeStruct((K, COLS), f32),
        in_specs=[hbm, hbm, vmem, hbm, vmem],
        out_specs=vmem,
        scratch_shapes=scratch,
        compiler_params=pltpu.CompilerParams(
            collective_id=0, has_side_effects=True, vmem_limit_bytes=60 * 1024 * 1024
        ),
        name="newton_step",
    )(
        features,
        labels,
        weights,
        sketch_basis.reshape(K * COLS, RANK),
        sketch_values.reshape(4, 128),
    )
    return step


def solution(mesh):
    in_specs = (P("samp", "feat"), P("samp"), P(None, "feat"), P(None, "feat", None), P())
    return jax.shard_map(
        on_device, mesh=mesh, in_specs=in_specs, out_specs=P(None, "feat"), check_vma=False
    )
```

```python
import functools
import math

import jax
import jax.numpy as jnp
from jax import lax
from jax.experimental import pallas as pl
from jax.experimental.pallas import tpu as pltpu
from jax.sharding import PartitionSpec as P

F = 2048
ITERS = 3
RIDGE = 0.05
SAMP, YS, CORES = 16, 4, 2
FEAT = YS * CORES
ROWS = 16384
HALF = ROWS // CORES
CHUNKS = 4
CROWS = HALF // CHUNKS
PIECE = CROWS // YS
PTILES = PIECE // 128
PWIDE = PIECE + (PTILES + 3) // 4 * 128
COLS = 256
K = 10
RANK = 512
LT = K * COLS // 128
f32, bf16 = jnp.float32, jnp.bfloat16
HI = lax.Precision.HIGHEST
NT = (((1,), (1,)), ((), ()))
TN = (((0,), (0,)), ((), ()))
OFFS = (0, 4, 7, 9)
MSGS = ((0, 1), (1, 3), (4, 3), (7, 2), (9, 1))
FAR_SAMP = sorted(range(1, SAMP), key=lambda i: -(min(i // 4, 4 - i // 4) + min(i % 4, 4 - i % 4)))
FAR_FEAT = (4, 5, 3, 2, 6, 7, 1)


def scoped(name):
    def wrap(fn):
        @functools.wraps(fn)
        def run(*args):
            with jax.named_scope(name):
                return fn(*args)
        return run
    return wrap


def rcopy(src, dst, send, recv, dev):
    return pltpu.make_async_remote_copy(
        src_ref=src, dst_ref=dst, send_sem=send, recv_sem=recv,
        device_id=dev, device_id_type=pl.DeviceIdType.MESH,
    )


def rows_of(n):
    return lax.broadcasted_iota(jnp.int32, (n, 128), 0)


def pack(wide):
    low = wide[8:16]
    third = low[:, :128] + pltpu.roll(low[:, 128:], 2, 0)
    return jnp.concatenate([wide[:8], third], axis=1)


def unpack(packed):
    third = packed[:, 256:]
    row = rows_of(8)
    left = jnp.where(row < 2, third, 0.0)
    right = jnp.where(row < 2, pltpu.roll(third, 6, 0), 0.0)
    return jnp.concatenate([packed[:, :256], jnp.concatenate([left, right], axis=1)], axis=0)


def pack_piece(wide):
    low = wide[8:16]
    tiles = [wide[:8]]
    for e in range(0, PTILES, 4):
        last = low[:, e * 128 : (e + 1) * 128]
        for q in range(e + 1, min(e + 4, PTILES)):
            last = last + pltpu.roll(low[:, q * 128 : (q + 1) * 128], 2 * (q - e), 0)
        tiles.append(last)
    return jnp.concatenate(tiles, axis=1)


def shared_tile(packed, q):
    at = PIECE + q // 4 * 128
    return packed[:, at : at + 128]


def unpack_piece(packed):
    row = rows_of(8)
    low = []
    for q in range(PTILES):
        tile = shared_tile(packed, q)
        low.append(jnp.where(row < 2, pltpu.roll(tile, 8 - 2 * (q % 4), 0) if q % 4 else tile, 0.0))
    return jnp.concatenate([packed[:, :PIECE], jnp.concatenate(low, axis=1)], axis=0)


def spread_piece(packed):
    row = rows_of(8)
    low = [
        jnp.where((row >= 2 * (q % 4)) & (row < 2 * (q % 4) + 2), shared_tile(packed, q), 0.0) for q in range(PTILES)
    ]
    return jnp.concatenate([packed[:, :PIECE], jnp.concatenate(low, axis=1)], axis=0)


def fold_rows(wide):
    low = wide[8:16]
    low = low + pltpu.roll(low, 4, 0)
    low = low + pltpu.roll(low, 2, 0)
    row = lax.broadcasted_iota(jnp.int32, low.shape, 0)
    return jnp.concatenate([wide[:8], jnp.where(row < 2, low, 0.0)], axis=0)


def lane_row(packed, k, h):
    if k < 8:
        return packed[k : k + 1, h * 128 : (h + 1) * 128]
    r = 2 * h + (k - 8)
    return packed[r : r + 1, 256:384]


def column(row):
    return jnp.broadcast_to(row, (128, 128)).T


def lane_bcast(x, j):
    return jnp.broadcast_to(x[:, j : j + 1], (x.shape[0], 128))


@scoped('factor')
def factor_block(A, N):
    diag = [lane_bcast(A[0:8, :], j) for j in range(8)]
    for p in range(16):
        lo = 8 * p
        more = lo + 8 < 128
        if more:
            below = [lane_bcast(A[lo + 8 : 128, :], lo + j) for j in range(8)]
            ahead = [lane_bcast(A[lo + 8 : lo + 16, :], lo + 8 + j) for j in range(8)]
        rs, cs = [], []
        for j in range(8):
            r = lax.rsqrt(diag[j][j : j + 1, :])
            c = diag[j] * r
            for k in range(j + 1, 8):
                diag[k] = diag[k] - c * c[k : k + 1, :]
            rs.append(r)
            cs.append(c)
        arow, nrow = A[lo : lo + 8, :], N[lo : lo + 8, :]
        us, ns = [], []
        for j in range(8):
            us.append(arow[j : j + 1, :] * rs[j])
            ns.append(nrow[j : j + 1, :] * rs[j])
            if j < 7:
                arow = arow - cs[j] * us[j]
                nrow = nrow - cs[j] * ns[j]
        N[lo : lo + 8, :] = jnp.concatenate(ns, axis=0)
        if not more:
            continue
        bs = []
        for j in range(8):
            t = below[j]
            for i in range(j):
                t = t - bs[i] * cs[i][j : j + 1, :]
            bs.append(t * rs[j])
        for k in range(8):
            for j in range(8):
                ahead[k] = ahead[k] - bs[j][:8] * bs[j][k : k + 1, :]
        diag = ahead
        at, nt = A[lo + 8 : 128, :], N[lo + 8 : 128, :]
        for j in range(8):
            at = at - bs[j] * us[j]
            nt = nt - bs[j] * ns[j]
        A[lo + 8 : 128, :] = at
        N[lo + 8 : 128, :] = nt


def kernel(
    feat, labels, weights, basis, svals, out,
    X, own, bst, BT, dB, imgf, imgb, recvg, recvh, prob, E, Q, Qr, ar, dots, fe,
    lab, gpart, grecv, gall, V, acc, FA, FN, ccol, tmp, vec, prow, scal,
    sx_own, sx_s, sx_r, s_b, rs_s, rs_r, ag_s, ag_r, q_s, q_r, d_s, d_r,
    ar_s, ar_r, fe_s, fe_r, gf_s, gf_r, gs_s, gs_r, gy_s, gy_r, l_s,
):
    s = lax.axis_index("samp")
    f = lax.axis_index("feat")
    y = lax.div(f, CORES)
    c = lax.rem(f, CORES)
    sib = (s, f + 1 - 2 * c)

    def samp_dev(i):
        return lax.rem(s + i, SAMP)

    def feat_dev(i):
        return lax.rem(f + i, FEAT)

    def y_dev(i):
        return lax.rem(y + i, YS)

    def slot(o, me, n):
        return lax.rem(o - me + n, n)

    def in_order(ref, me, n):
        total = ref[slot(0, me, n)]
        for o in range(1, n):
            total = total + ref[slot(o, me, n)]
        return total

    for k in range(K):
        pltpu.make_async_copy(basis.at[pl.ds(k * COLS, COLS)], bst.at[pl.ds(k * COLS, COLS)], s_b.at[k]).start()

    def own_rows(t):
        return pl.ds(pl.multiple_of(c * HALF + t * CROWS, CROWS), CROWS)

    def sib_rows(t):
        return pl.ds(pl.multiple_of((1 - c) * HALF + t * CROWS, CROWS), CROWS)

    def x_own(t):
        return pltpu.make_async_copy(feat.at[own_rows(t)], X.at[c, pl.ds(t * CROWS, CROWS)], sx_own.at[t])

    def x_send(t):
        return rcopy(feat.at[sib_rows(t)], X.at[c, pl.ds(t * CROWS, CROWS)], sx_s.at[0], sx_r.at[t], sib)

    def x_recv(t):
        dst = X.at[1 - c, pl.ds(t * CROWS, CROWS)]
        return rcopy(dst, dst, sx_s.at[0], sx_r.at[t], sib)

    def x_sent():
        return rcopy(X.at[c], X.at[c], sx_s.at[0], sx_r.at[0], sib)

    def lab_copy(t):
        start = pl.multiple_of(c * HALF + t * CROWS + y * PIECE, PIECE)
        return pltpu.make_async_copy(labels.at[pl.ds(start, PIECE)], lab.at[t, 0], l_s.at[t])


    def d_copy(ph):
        return rcopy(dB.at[ph, c], dB.at[ph, c], d_s.at[0], d_r.at[0], sib)

    def d_recv(ph):
        return rcopy(dB.at[ph, 1 - c], dB.at[ph, 1 - c], d_s.at[0], d_r.at[0], sib)

    barrier = pltpu.get_barrier_semaphore()
    for i in range(1, FEAT):
        pl.semaphore_signal(barrier, inc=1, device_id=(s, feat_dev(i)), device_id_type=pl.DeviceIdType.MESH)
    for i in range(1, SAMP):
        pl.semaphore_signal(barrier, inc=1, device_id=(samp_dev(i), f), device_id_type=pl.DeviceIdType.MESH)

    w = jnp.concatenate([weights[...], jnp.zeros((16 - K, COLS), f32)], axis=0)
    dB[0, c] = w.astype(bf16)

    @pl.loop(0, K)
    @scoped('transpose')
    def _(k):
        pltpu.make_async_copy(
            basis.at[pl.ds(k * COLS, COLS)], bst.at[pl.ds(k * COLS, COLS)], s_b.at[k]
        ).wait()
        for h in range(2):
            for jt in range(4):
                blk = bst[pl.ds(pl.multiple_of(k * COLS + h * 128, 128), 128), jt * 128 : (jt + 1) * 128]
                BT[jt * 128 : (jt + 1) * 128, pl.ds(pl.multiple_of(k * COLS + h * 128, 128), 128)] = blk.T

    for t in range(CHUNKS):
        x_own(t).start()
        lab_copy(t).start()

    blk_id = lax.min(s, 9)
    ba = sum((blk_id >= e).astype(jnp.int32) for e in (4, 7, 9))
    bb = blk_id - lax.div(ba * (9 - ba), 2) + ba

    with jax.named_scope('gram'):
        block = lax.dot_general(
            BT[pl.ds(pl.multiple_of(ba * 128, 128), 128), :],
            BT[pl.ds(pl.multiple_of(bb * 128, 128), 128), :],
            NT, precision=HI, preferred_element_type=f32,
        )
        for g in range(FEAT):
            gpart[g] = block[g * 16 : (g + 1) * 16]

    def gf_copy(i):
        o = feat_dev(i)
        return rcopy(gpart.at[o], grecv.at[FEAT - i], gf_s.at[0], gf_r.at[0], (s, o))

    def gf_all():
        every = grecv.at[pl.ds(1, FEAT - 1)]
        return rcopy(every, every, gf_s.at[0], gf_r.at[0], sib)

    def gs_copy(i):
        return rcopy(gall.at[0, s], gall.at[0, s], gs_s.at[0], gs_r.at[s], (samp_dev(i), f))

    def gs_sent():
        every = gall.at[0, pl.ds(0, SAMP - 1)]
        return rcopy(every, every, gs_s.at[0], gs_r.at[0], sib)

    def gs_recv(o):
        return rcopy(gall.at[0, o], gall.at[0, o], gs_s.at[0], gs_r.at[o], (o, f))

    def gy_copy(m, i):
        at = pl.ds(*MSGS[m])
        return rcopy(gall.at[0, at], gall.at[FEAT - i, at], gy_s.at[m], gy_r.at[m], (s, feat_dev(i)))

    def gy_all(m):
        every = gall.at[pl.ds(1, FEAT - 1), pl.ds(*MSGS[m])]
        return rcopy(every, every, gy_s.at[m], gy_r.at[m], sib)

    with jax.named_scope('barrier'):
        pl.semaphore_wait(barrier, FEAT - 1 + SAMP - 1)

    @pl.when(s < 10)
    def _():
        for i in FAR_FEAT:
            gf_copy(i).start()

    d_copy(0).start()
    for t in range(CHUNKS):
        x_send(t).start()

    def rs_copy(ph, t, i, grad):
        o = y_dev(i)
        src = imgf.at[t, o] if grad else imgb.at[t, o]
        dst = recvg.at[t, YS - i] if grad else recvh.at[ph - 1, t, YS - i]
        return rcopy(src, dst, rs_s.at[0], rs_r.at[t], (s, CORES * o + c))

    def rs_all(ph, t, grad):
        every = recvg.at[t, pl.ds(1, YS - 1)] if grad else recvh.at[ph - 1, t, pl.ds(1, YS - 1)]
        return rcopy(every, every, rs_s.at[0], rs_r.at[t], sib)

    def rs_sent(grad):
        every = imgf.at[pl.ds(0, YS - 1)] if grad else imgb.at[pl.ds(0, YS - 1)]
        return rcopy(every, every, rs_s.at[0], rs_r.at[0], sib)

    def ag_copy(ph, t, i):
        return rcopy(E.at[ph, t, 0], E.at[ph, t, YS - i], ag_s.at[0], ag_r.at[t], (s, CORES * y_dev(i) + c))

    def ag_all(ph, t):
        every = E.at[ph, t, pl.ds(1, YS - 1)]
        return rcopy(every, every, ag_s.at[0], ag_r.at[t], sib)

    def ag_sent(ph):
        every = E.at[ph, pl.ds(0, YS - 1)]
        return rcopy(every, every, ag_s.at[0], ag_r.at[0], sib)

    @scoped('own_images')
    def own_images(ph, grad):
        for t in range(CHUNKS):
            at = slice(t * CROWS, (t + 1) * CROWS)
            if grad:
                x_own(t).wait()
            own[t] = lax.dot_general(dB[ph, c], X[c, at], NT, preferred_element_type=f32)

    @scoped('images')
    def images(ph, grad):
        if not grad:
            own_images(ph, False)
        d_recv(ph).wait_recv()
        for t in range(CHUNKS):
            at = slice(t * CROWS, (t + 1) * CROWS)
            if grad:
                x_recv(t).wait_recv()
            img = own[t] + lax.dot_general(dB[ph, 1 - c], X[1 - c, at], NT, preferred_element_type=f32)
            for o in range(YS):
                piece = pack_piece(img[:, o * PIECE : (o + 1) * PIECE])
                imgf[t, o] = piece
                if not grad:
                    imgb[t, o] = piece.astype(bf16)
            for i in range(1, YS):
                rs_copy(ph, t, i, grad).start()

    @scoped('pieces')
    def pieces(ph, grad):
        @pl.loop(0, CHUNKS)
        def _(t):
            total = imgf[t, y]
            rs_all(ph, t, grad).wait_recv()
            for i in range(1, YS):
                total = total + (recvg[t, i] if grad else recvh[ph - 1, t, i].astype(f32))
            total = unpack_piece(total)
            if grad:
                logits = total / math.sqrt(F)
                row = lax.broadcasted_iota(jnp.int32, (16, PIECE), 0)
                logits = jnp.where(row < K, logits, -jnp.inf)
                top = jnp.max(logits, axis=0, keepdims=True)
                ex = jnp.exp(logits - top)
                pr = ex / jnp.sum(ex, axis=0, keepdims=True)
                prob[t] = pr
                lab_copy(t).wait()
                mine = lab[t]
                coeffs = pr - jnp.where(row == mine, 1.0, 0.0)
            else:
                pr = prob[t]
                weighted = pr * total
                coeffs = weighted - pr * jnp.sum(weighted, axis=0, keepdims=True)
            E[ph, t, 0] = pack_piece(coeffs).astype(bf16)
            for i in range(1, YS):
                ag_copy(ph, t, i).start()

    @scoped('collect')
    def collect(ph):
        Q[...] = jnp.zeros_like(Q)

        @pl.loop(0, CHUNKS)
        def _(t):
            ag_all(ph, t).wait_recv()
            e = jnp.concatenate([spread_piece(E[ph, t, slot(o, y, YS)].astype(f32)) for o in range(YS)], axis=1).astype(bf16)
            at = pl.ds(pl.multiple_of(t * CROWS, CROWS), CROWS)
            for h in range(2):
                Q[h] = Q[h] + jnp.dot(e, X[h, at], preferred_element_type=f32)

        for h in range(2):
            Q[h] = fold_rows(Q[h])

    def q_copy(ph):
        return rcopy(Q.at[1 - c], Qr.at[ph], q_s.at[0], q_r.at[0], sib)

    def ar_copy(ph, i):
        return rcopy(ar.at[ph, 0], ar.at[ph, SAMP - i], ar_s.at[ph], ar_r.at[ph], (samp_dev(i), f))

    def ar_all(ph):
        every = ar.at[ph, pl.ds(1, SAMP - 1)]
        return rcopy(every, every, ar_s.at[ph], ar_r.at[ph], sib)

    def fe_copy(ph, i):
        return rcopy(fe.at[ph, 0], fe.at[ph, FEAT - i], fe_s.at[ph], fe_r.at[ph], (s, feat_dev(i)))

    def fe_all(ph):
        every = fe.at[ph, pl.ds(1, FEAT - 1)]
        return rcopy(every, every, fe_s.at[ph], fe_r.at[ph], sib)

    def chip_sum(ph):
        q_copy(ph).start()
        q_copy(ph).wait_recv()
        return pack(Q[c] + Qr[ph])

    @scoped('sums_start')
    def start_sums(ph):
        ar[ph, 0] = chip_sum(ph)
        for i in range(1, SAMP):
            ar_copy(ph, i).start()

    @scoped('sums_finish')
    def finish_sums(ph):
        ar_all(ph).wait_recv()
        return in_order(ar.at[ph], s, SAMP)

    def last_copy(i):
        return rcopy(dots.at[0], dots.at[SAMP - i], ar_s.at[ITERS], ar_r.at[ITERS], (samp_dev(i), f))

    def last_all():
        every = dots.at[pl.ds(1, SAMP - 1)]
        return rcopy(every, every, ar_s.at[ITERS], ar_r.at[ITERS], sib)

    @scoped('sums_last')
    def sums_last(message):
        dots[0] = message
        for i in range(1, SAMP):
            last_copy(i).start()
        drain(ITERS, False)
        drain_sums(ITERS - 2)
        last_all().wait_recv()
        return in_order(dots, s, SAMP)

    @scoped('drain')
    def drain(ph, grad):
        d_copy(ph).wait_send()
        q_copy(ph).wait_send()
        rs_sent(grad).wait_send()
        ag_sent(ph).wait_send()

    def drain_setup():
        x_sent().wait_send()

        @pl.when(s < 10)
        def _():
            gf_all().wait_send()
            gs_sent().wait_send()

        for m in range(len(MSGS)):
            gy_all(m).wait_send()

    def drain_sums(ph):
        ar_all(ph).wait_send()
        fe_all(ph).wait_send()

    def send_sums(ph, message):
        fe[ph, 0] = message
        for i in FAR_FEAT:
            fe_copy(ph, i).start()

    @scoped('exchange')
    def take_sums(ph):
        fe_all(ph).wait_recv()
        return in_order(fe.at[ph], f, FEAT)

    def exchange(ph, message):
        send_sums(ph, message)
        return take_sums(ph)

    own_images(0, True)

    @pl.when(s < 10)
    @scoped('gram_sum')
    def _():
        gf_all().wait_recv()
        grecv[0] = gpart[f]
        gall[0, s] = in_order(grecv, f, FEAT)
        for i in FAR_SAMP:
            gs_copy(i).start()

    images(0, True)

    @scoped('gram_gather')
    def gram_gather(first, last):
        for m in range(first, last):
            start, count = MSGS[m]
            for o in range(start, start + count):
                @pl.when(s != o)
                def _():
                    gs_recv(o).wait_recv()
            for i in FAR_FEAT:
                gy_copy(m, i).start()

    gram_gather(0, 2)
    pieces(0, True)
    gram_gather(2, 5)

    sv = svals[...]
    low = jnp.min(jnp.min(sv, axis=1, keepdims=True), axis=0, keepdims=True)
    coef = (low + RIDGE) / (sv + RIDGE) - 1.0
    for jt in range(4):
        ccol[jt * 128 : (jt + 1) * 128, :] = column(coef[jt : jt + 1, :])
    eye = jnp.where(rows_of(128) == lax.broadcasted_iota(jnp.int32, (128, 128), 1), 1.0, 0.0).astype(f32)

    def lanes(a, b):
        return slice(a * 128, b * 128)

    def dot_hi(a, b, dims=(((1,), (0,)), ((), ()))):
        return lax.dot_general(a, b, dims, precision=HI, preferred_element_type=f32)

    def gram_block(k, l):
        blk = jnp.concatenate([gall[slot(o, f, FEAT), OFFS[k] + l - k] for o in range(FEAT)], axis=0)
        return blk if k == 0 else blk - acc[k, :, lanes(l, l + 1)]

    def add_to(k, i, a, b):
        term = dot_hi(V[k, :, lanes(i, i + 1)], V[k, :, lanes(a, b)], TN)
        first = k == 0 if b <= 4 else k == a - 4
        acc[i, :, lanes(a, b)] = term if first else acc[i, :, lanes(a, b)] + term

    def rest_of(k):
        inv = V[k, :, lanes(4 + k, 5 + k)]
        if k < 2:
            V[k, :, lanes(k + 2, 4)] = dot_hi(inv, jnp.concatenate([gram_block(k, l) for l in range(k + 2, 4)], axis=1))
        if k > 0:
            V[k, :, lanes(4, 4 + k)] = -dot_hi(inv, acc[k, :, lanes(4, 4 + k)])
        for i in range(k + 1, 4):
            if i > k + 1:
                add_to(k, i, i, 4)
            elif i < 3:
                add_to(k, i, i + 1, 4)
            if k > 0:
                add_to(k, i, 4, 4 + k)
            add_to(k, i, 4 + k, 5 + k)

    @scoped('basis_dots')
    def basis_dots(packed):
        rows = [lane_row(packed, lt // 2, lt % 2) for lt in range(LT)]

        @pl.loop(0, 8)
        def _(g):
            at = pl.ds(pl.multiple_of(g * 64, 64), 64)
            acc = BT[at, 0:128] * rows[0]
            for lt in range(1, LT):
                acc = acc + BT[at, lt * 128 : (lt + 1) * 128] * rows[lt]
            tmp[at, :] = acc

        return [jnp.sum(tmp[jt * 128 : (jt + 1) * 128, :].T, axis=0, keepdims=True) for jt in range(4)]

    def lanes_of(a, b):
        t = a * b
        t = jnp.sum(t[:, :128] + t[:, 128:256] + t[:, 256:], axis=0, keepdims=True)
        return t + pltpu.roll(t, 64, 1)

    lane = lax.broadcasted_iota(jnp.int32, (1, 128), 1)

    def both(x, z):
        return jnp.where(lane < 64, x, z)

    def halves(total):
        wide = lax.broadcasted_iota(jnp.int32, (8, 128), 1)
        lo = jnp.sum(jnp.where(wide < 64, total, 0.0), axis=1, keepdims=True)
        hi = jnp.sum(jnp.where(wide < 64, 0.0, total), axis=1, keepdims=True)
        return lo, hi

    @scoped('inner')
    def inner_part(p):
        y_rows = [jnp.zeros((8, 128), f32) for _ in range(4)]
        dot = jnp.zeros((8, 128), f32)
        for g in range(8):
            kb, at, crow = g // 2, slice((g % 2) * 64, (g % 2) * 64 + 64), slice(g * 64, (g + 1) * 64)
            m = V[kb, at, lanes(4, 5)] * p[0]
            for l in range(1, kb + 1):
                m = m + V[kb, at, lanes(4 + l, 5 + l)] * p[l]
            inner = jnp.sum(m, axis=1, keepdims=True)
            ci = ccol[crow, :] * inner
            d = ci * inner
            for b in range(8):
                dot = dot + d[b * 8 : (b + 1) * 8]
            for l in range(kb + 1):
                t = V[kb, at, lanes(4 + l, 5 + l)] * ci
                for b in range(8):
                    y_rows[l] = y_rows[l] + t[b * 8 : (b + 1) * 8]
        return (
            [jnp.sum(t, axis=0, keepdims=True) for t in y_rows],
            jnp.sum(dot, axis=0, keepdims=True)[:, :1],
        )

    @scoped('basis_apply')
    def basis_apply(y_rows):
        for jt in range(4):
            tmp[jt * 128 : (jt + 1) * 128, :] = column(y_rows[jt])

        def body(g, accs):
            out = list(accs)
            for b in range(4):
                at = pl.ds(pl.multiple_of(g * 32 + b * 8, 8), 8)
                col = tmp[at, :]
                for lt in range(LT):
                    out[lt] = out[lt] + BT[at, lt * 128 : (lt + 1) * 128] * col
            return tuple(out)

        accs = lax.fori_loop(0, 16, body, tuple(jnp.zeros((8, 128), f32) for _ in range(LT)))
        rows = [jnp.sum(t, axis=0, keepdims=True) for t in accs]
        tiles = [jnp.concatenate([rows[2 * k + h] for k in range(8)], axis=0) for h in range(2)]
        zero = jnp.zeros((1, 128), f32)
        last = jnp.concatenate([rows[16], rows[18], rows[17], rows[19]] + [zero] * 4, axis=0)
        return jnp.concatenate(tiles + [last], axis=1)

    def set_direction(ph, d):
        vec[1] = d
        dB[ph, c] = unpack(d).astype(bf16)
        d_copy(ph).start()

    NS = float(SAMP * ROWS)
    zrow = jnp.zeros((1, 128), f32)
    for kb in range(4):
        with jax.named_scope('chol_wait'):
            gy_all(kb + 1 if kb else 0).wait_recv()
        with jax.named_scope('chol'):
            FA[...] = gram_block(kb, kb)
            FN[...] = eye
            if kb > 0:
                rest_of(kb - 1)
            factor_block(FA, FN)
            V[kb, :, lanes(4 + kb, 5 + kb)] = FN[...]
            if kb == 0:
                gy_all(1).wait_recv()
            if kb < 3:
                V[kb, :, lanes(kb + 1, kb + 2)] = dot_hi(FN[...], gram_block(kb, kb + 1))
                add_to(kb, kb + 1, kb + 1, kb + 2)
        if kb == 0:
            collect(0)
            start_sums(0)
        if kb == 2:
            res = -(finish_sums(0) * (math.sqrt(F) / NS) + RIDGE * pack(w))
            vec[0] = res
            send_sums(0, jnp.concatenate(
                basis_dots(res) + [zrow, zrow, both(lanes_of(res, res), zrow), zrow], axis=0
            ))
    rest_of(3)

    drain(0, True)
    tot = take_sums(0)
    lo, hi = halves(tot)
    y_rows, py = inner_part([tot[i : i + 1] for i in range(4)])
    rr = lo[6:7]
    prow[...] = tot
    vec[2] = jnp.zeros((8, 384), f32)
    scal[0:1, :] = jnp.broadcast_to(rr, (1, 128))
    scal[1:2, :] = jnp.broadcast_to(rr + py, (1, 128))
    set_direction(1, vec[0] + basis_apply(y_rows))

    @pl.loop(0, ITERS)
    def _(it):
        ph = it + 1
        images(ph, False)
        pieces(ph, False)
        collect(ph)

        @pl.when(it == ITERS - 1)
        def _():
            d, r = vec[1], vec[0]
            dq = sums_last(jnp.broadcast_to(lanes_of(d, chip_sum(ITERS)), (8, 128)))[0:1]
            dq = dq / NS + RIDGE * lanes_of(d, d)
            send_sums(ITERS, jnp.broadcast_to(both(dq, lanes_of(r, d)), (8, 128)))
            drain_sums(ITERS - 1)
            last_all().wait_send()
            lo, hi = halves(take_sums(ITERS))
            with jax.named_scope('out'):
                out[...] = unpack(vec[2] + hi[0:1] / lo[0:1] * d)[:K]

        @pl.when(it < ITERS - 1)
        def _():
            start_sums(ph)
            drain(ph, False)

            @pl.when(it == 0)
            def _():
                drain_setup()

            @pl.when(it > 0)
            def _():
                drain_sums(ph - 2)

            d, r = vec[1], vec[0]
            q = finish_sums(ph) / NS + RIDGE * d
            bq = basis_dots(q)
            tot = exchange(ph, jnp.concatenate(bq + [
                both(lanes_of(d, q), lanes_of(r, d)),
                both(lanes_of(r, q), lanes_of(q, q)),
                both(lanes_of(r, r), zrow),
                zrow,
            ], axis=0))
            lo, hi = halves(tot)
            step = hi[4:5] / lo[4:5]
            vec[2] = vec[2] + step * d
            rn = r - step * q
            vec[0] = rn
            pn = prow[...] - step * tot
            prow[...] = pn
            y_rows, py = inner_part([pn[i : i + 1] for i in range(4)])
            rr = lo[6:7] - 2.0 * step * lo[5:6] + step * step * hi[5:6]
            new = rr + py
            beta = new / scal[1:2, 0:1]
            scal[1:2, :] = jnp.broadcast_to(new, (1, 128))
            set_direction(ph + 1, rn + basis_apply(y_rows) + beta * d)

    with jax.named_scope('last_waits'):
        fe_all(ITERS).wait_send()


def on_device(features, labels, weights, sketch_basis, sketch_values):
    vmem = pl.BlockSpec(memory_space=pltpu.VMEM)
    hbm = pl.BlockSpec(memory_space=pl.ANY)
    V = pltpu.VMEM
    dma = pltpu.SemaphoreType.DMA
    PH = ITERS + 1
    scratch = [
        V((2, HALF, COLS), bf16),
        V((CHUNKS, 16, CROWS), f32),
        V((K * COLS, RANK), f32),
        V((RANK, K * COLS), f32),
        V((PH, 2, 16, COLS), bf16),
        V((CHUNKS, YS, 8, PWIDE), f32),
        V((CHUNKS, YS, 8, PWIDE), bf16),
        V((CHUNKS, YS, 8, PWIDE), f32),
        V((ITERS, CHUNKS, YS, 8, PWIDE), bf16),
        V((CHUNKS, 16, PIECE), f32),
        V((PH, CHUNKS, YS, 8, PWIDE), bf16),
        V((2, 16, COLS), f32),
        V((PH, 16, COLS), f32),
        V((ITERS, SAMP, 8, 384), f32),
        V((SAMP, 8, 128), f32),
        V((PH, FEAT, 8, 128), f32),
        V((CHUNKS, 1, PIECE), jnp.int32),
        V((FEAT, 16, 128), f32),
        V((FEAT, 16, 128), f32),
        V((FEAT, SAMP, 16, 128), f32),
        V((4, 128, 2 * RANK), f32),
        V((4, 128, 2 * RANK), f32),
        V((128, 128), f32),
        V((128, 128), f32),
        V((RANK, 128), f32),
        V((RANK, 128), f32),
        V((3, 8, 384), f32),
        V((8, 128), f32),
        V((8, 128), f32),
        dma((CHUNKS,)), dma((1,)), dma((CHUNKS,)), dma((K,)),
        dma((1,)), dma((CHUNKS,)), dma((1,)), dma((CHUNKS,)),
        dma((1,)), dma((1,)), dma((1,)), dma((1,)),
        dma((PH,)), dma((PH,)), dma((PH,)), dma((PH,)),
        dma((1,)), dma((1,)), dma((1,)), dma((10,)),
        dma((len(MSGS),)), dma((len(MSGS),)), dma((CHUNKS,)),
    ]
    step = pl.pallas_call(
        kernel,
        out_shape=jax.ShapeDtypeStruct((K, COLS), f32),
        in_specs=[hbm, hbm, vmem, hbm, vmem],
        out_specs=vmem,
        scratch_shapes=scratch,
        compiler_params=pltpu.CompilerParams(
            collective_id=0, has_side_effects=True, vmem_limit_bytes=60 * 1024 * 1024
        ),
        name="newton_step",
    )(
        features,
        labels,
        weights,
        sketch_basis.reshape(K * COLS, RANK),
        sketch_values.reshape(4, 128),
    )
    return step


def solution(mesh):
    in_specs = (P("samp", "feat"), P("samp"), P(None, "feat"), P(None, "feat", None), P())
    return jax.shard_map(
        on_device, mesh=mesh, in_specs=in_specs, out_specs=P(None, "feat"), check_vma=False
    )
```

```python
import functools
import math

import jax
import jax.numpy as jnp
from jax import lax
from jax.experimental import pallas as pl
from jax.experimental.pallas import tpu as pltpu
from jax.sharding import PartitionSpec as P

F = 2048
ITERS = 3
RIDGE = 0.05
SAMP, YS, CORES = 16, 4, 2
FEAT = YS * CORES
ROWS = 16384
HALF = ROWS // CORES
CHUNKS = 4
CROWS = HALF // CHUNKS
PIECE = CROWS // YS
PTILES = PIECE // 128
PWIDE = PIECE + (PTILES + 3) // 4 * 128
COLS = 256
K = 10
RANK = 512
LT = K * COLS // 128
f32, bf16 = jnp.float32, jnp.bfloat16
HI = lax.Precision.HIGHEST
NT = (((1,), (1,)), ((), ()))
TN = (((0,), (0,)), ((), ()))
OFFS = (0, 4, 7, 9)
MSGS = ((0, 1), (1, 3), (4, 3), (7, 2), (9, 1))
FAR_SAMP = sorted(range(1, SAMP), key=lambda i: -(min(i // 4, 4 - i // 4) + min(i % 4, 4 - i % 4)))
FAR_FEAT = (4, 5, 3, 2, 6, 7, 1)


def scoped(name):
    def wrap(fn):
        @functools.wraps(fn)
        def run(*args):
            with jax.named_scope(name):
                return fn(*args)
        return run
    return wrap


def rcopy(src, dst, send, recv, dev):
    return pltpu.make_async_remote_copy(
        src_ref=src, dst_ref=dst, send_sem=send, recv_sem=recv,
        device_id=dev, device_id_type=pl.DeviceIdType.MESH,
    )


def rows_of(n):
    return lax.broadcasted_iota(jnp.int32, (n, 128), 0)


def pack(wide):
    low = wide[8:16]
    third = low[:, :128] + pltpu.roll(low[:, 128:], 2, 0)
    return jnp.concatenate([wide[:8], third], axis=1)


def unpack(packed):
    third = packed[:, 256:]
    row = rows_of(8)
    left = jnp.where(row < 2, third, 0.0)
    right = jnp.where(row < 2, pltpu.roll(third, 6, 0), 0.0)
    return jnp.concatenate([packed[:, :256], jnp.concatenate([left, right], axis=1)], axis=0)


def pack_piece(wide):
    low = wide[8:16]
    tiles = [wide[:8]]
    for e in range(0, PTILES, 4):
        last = low[:, e * 128 : (e + 1) * 128]
        for q in range(e + 1, min(e + 4, PTILES)):
            last = last + pltpu.roll(low[:, q * 128 : (q + 1) * 128], 2 * (q - e), 0)
        tiles.append(last)
    return jnp.concatenate(tiles, axis=1)


def shared_tile(packed, q):
    at = PIECE + q // 4 * 128
    return packed[:, at : at + 128]


def unpack_piece(packed):
    row = rows_of(8)
    low = []
    for q in range(PTILES):
        tile = shared_tile(packed, q)
        low.append(jnp.where(row < 2, pltpu.roll(tile, 8 - 2 * (q % 4), 0) if q % 4 else tile, 0.0))
    return jnp.concatenate([packed[:, :PIECE], jnp.concatenate(low, axis=1)], axis=0)


def spread_piece(packed):
    row = rows_of(8)
    low = [
        jnp.where((row >= 2 * (q % 4)) & (row < 2 * (q % 4) + 2), shared_tile(packed, q), 0.0) for q in range(PTILES)
    ]
    return jnp.concatenate([packed[:, :PIECE], jnp.concatenate(low, axis=1)], axis=0)


def fold_rows(wide):
    low = wide[8:16]
    low = low + pltpu.roll(low, 4, 0)
    low = low + pltpu.roll(low, 2, 0)
    row = lax.broadcasted_iota(jnp.int32, low.shape, 0)
    return jnp.concatenate([wide[:8], jnp.where(row < 2, low, 0.0)], axis=0)


def lane_row(packed, k, h):
    if k < 8:
        return packed[k : k + 1, h * 128 : (h + 1) * 128]
    r = 2 * h + (k - 8)
    return packed[r : r + 1, 256:384]


def column(row):
    return jnp.broadcast_to(row, (128, 128)).T


def lane_bcast(x, j):
    return jnp.broadcast_to(x[:, j : j + 1], (x.shape[0], 128))


@scoped('factor')
def factor_block(A, N):
    diag = [lane_bcast(A[0:8, :], j) for j in range(8)]
    for p in range(16):
        lo = 8 * p
        more = lo + 8 < 128
        if more:
            below = [lane_bcast(A[lo + 8 : 128, :], lo + j) for j in range(8)]
            ahead = [lane_bcast(A[lo + 8 : lo + 16, :], lo + 8 + j) for j in range(8)]
        rs, cs = [], []
        for j in range(8):
            r = lax.rsqrt(diag[j][j : j + 1, :])
            c = diag[j] * r
            for k in range(j + 1, 8):
                diag[k] = diag[k] - c * c[k : k + 1, :]
            rs.append(r)
            cs.append(c)
        arow, nrow = A[lo : lo + 8, :], N[lo : lo + 8, :]
        us, ns = [], []
        for j in range(8):
            us.append(arow[j : j + 1, :] * rs[j])
            ns.append(nrow[j : j + 1, :] * rs[j])
            if j < 7:
                arow = arow - cs[j] * us[j]
                nrow = nrow - cs[j] * ns[j]
        N[lo : lo + 8, :] = jnp.concatenate(ns, axis=0)
        if not more:
            continue
        bs = []
        for j in range(8):
            t = below[j]
            for i in range(j):
                t = t - bs[i] * cs[i][j : j + 1, :]
            bs.append(t * rs[j])
        for k in range(8):
            for j in range(8):
                ahead[k] = ahead[k] - bs[j][:8] * bs[j][k : k + 1, :]
        diag = ahead
        at, nt = A[lo + 8 : 128, :], N[lo + 8 : 128, :]
        for j in range(8):
            at = at - bs[j] * us[j]
            nt = nt - bs[j] * ns[j]
        A[lo + 8 : 128, :] = at
        N[lo + 8 : 128, :] = nt


def kernel(
    feat, labels, weights, basis, svals, out,
    X, own, bst, BT, dB, imgf, imgb, recvg, recvh, prob, E, Q, Qr, ar, dots, fe,
    lab, gpart, grecv, gall, V, acc, FA, FN, ccol, tmp, vec, prow, scal,
    sx_own, sx_s, sx_r, s_b, rs_s, rs_r, ag_s, ag_r, q_s, q_r, d_s, d_r,
    ar_s, ar_r, fe_s, fe_r, gf_s, gf_r, gs_s, gs_r, gy_s, gy_r, l_s,
):
    s = lax.axis_index("samp")
    f = lax.axis_index("feat")
    y = lax.div(f, CORES)
    c = lax.rem(f, CORES)
    sib = (s, f + 1 - 2 * c)

    def samp_dev(i):
        return lax.rem(s + i, SAMP)

    def feat_dev(i):
        return lax.rem(f + i, FEAT)

    def y_dev(i):
        return lax.rem(y + i, YS)

    def slot(o, me, n):
        return lax.rem(o - me + n, n)

    def in_order(ref, me, n):
        total = ref[slot(0, me, n)]
        for o in range(1, n):
            total = total + ref[slot(o, me, n)]
        return total

    for k in range(K):
        pltpu.make_async_copy(basis.at[pl.ds(k * COLS, COLS)], bst.at[pl.ds(k * COLS, COLS)], s_b.at[k]).start()

    def own_rows(t):
        return pl.ds(pl.multiple_of(c * HALF + t * CROWS, CROWS), CROWS)

    def sib_rows(t):
        return pl.ds(pl.multiple_of((1 - c) * HALF + t * CROWS, CROWS), CROWS)

    def x_own(t):
        return pltpu.make_async_copy(feat.at[own_rows(t)], X.at[c, pl.ds(t * CROWS, CROWS)], sx_own.at[t])

    def x_send(t):
        return rcopy(feat.at[sib_rows(t)], X.at[c, pl.ds(t * CROWS, CROWS)], sx_s.at[0], sx_r.at[t], sib)

    def x_recv(t):
        dst = X.at[1 - c, pl.ds(t * CROWS, CROWS)]
        return rcopy(dst, dst, sx_s.at[0], sx_r.at[t], sib)

    def x_sent():
        return rcopy(X.at[c], X.at[c], sx_s.at[0], sx_r.at[0], sib)

    def lab_copy(t):
        start = pl.multiple_of(c * HALF + t * CROWS + y * PIECE, PIECE)
        return pltpu.make_async_copy(labels.at[pl.ds(start, PIECE)], lab.at[t, 0], l_s.at[t])


    def d_copy(ph):
        return rcopy(dB.at[ph, c], dB.at[ph, c], d_s.at[0], d_r.at[0], sib)

    def d_recv(ph):
        return rcopy(dB.at[ph, 1 - c], dB.at[ph, 1 - c], d_s.at[0], d_r.at[0], sib)

    barrier = pltpu.get_barrier_semaphore()
    for i in range(1, FEAT):
        pl.semaphore_signal(barrier, inc=1, device_id=(s, feat_dev(i)), device_id_type=pl.DeviceIdType.MESH)
    for i in range(1, SAMP):
        pl.semaphore_signal(barrier, inc=1, device_id=(samp_dev(i), f), device_id_type=pl.DeviceIdType.MESH)

    w = jnp.concatenate([weights[...], jnp.zeros((16 - K, COLS), f32)], axis=0)
    dB[0, c] = w.astype(bf16)

    @pl.loop(0, K)
    @scoped('transpose')
    def _(k):
        pltpu.make_async_copy(
            basis.at[pl.ds(k * COLS, COLS)], bst.at[pl.ds(k * COLS, COLS)], s_b.at[k]
        ).wait()
        for h in range(2):
            for jt in range(4):
                blk = bst[pl.ds(pl.multiple_of(k * COLS + h * 128, 128), 128), jt * 128 : (jt + 1) * 128]
                BT[jt * 128 : (jt + 1) * 128, pl.ds(pl.multiple_of(k * COLS + h * 128, 128), 128)] = blk.T

    for t in range(CHUNKS):
        x_own(t).start()
        lab_copy(t).start()

    blk_id = lax.min(s, 9)
    ba = sum((blk_id >= e).astype(jnp.int32) for e in (4, 7, 9))
    bb = blk_id - lax.div(ba * (9 - ba), 2) + ba

    with jax.named_scope('gram'):
        block = lax.dot_general(
            BT[pl.ds(pl.multiple_of(ba * 128, 128), 128), :],
            BT[pl.ds(pl.multiple_of(bb * 128, 128), 128), :],
            NT, precision=HI, preferred_element_type=f32,
        )
        for g in range(FEAT):
            gpart[g] = block[g * 16 : (g + 1) * 16]

    def gf_copy(i):
        o = feat_dev(i)
        return rcopy(gpart.at[o], grecv.at[FEAT - i], gf_s.at[0], gf_r.at[0], (s, o))

    def gf_all():
        every = grecv.at[pl.ds(1, FEAT - 1)]
        return rcopy(every, every, gf_s.at[0], gf_r.at[0], sib)

    def gs_copy(i):
        return rcopy(gall.at[0, s], gall.at[0, s], gs_s.at[0], gs_r.at[s], (samp_dev(i), f))

    def gs_sent():
        every = gall.at[0, pl.ds(0, SAMP - 1)]
        return rcopy(every, every, gs_s.at[0], gs_r.at[0], sib)

    def gs_recv(o):
        return rcopy(gall.at[0, o], gall.at[0, o], gs_s.at[0], gs_r.at[o], (o, f))

    def gy_copy(m, i):
        at = pl.ds(*MSGS[m])
        return rcopy(gall.at[0, at], gall.at[FEAT - i, at], gy_s.at[m], gy_r.at[m], (s, feat_dev(i)))

    def gy_all(m):
        every = gall.at[pl.ds(1, FEAT - 1), pl.ds(*MSGS[m])]
        return rcopy(every, every, gy_s.at[m], gy_r.at[m], sib)

    with jax.named_scope('barrier'):
        pl.semaphore_wait(barrier, FEAT - 1 + SAMP - 1)

    @pl.when(s < 10)
    def _():
        for i in FAR_FEAT:
            gf_copy(i).start()

    d_copy(0).start()
    for t in range(CHUNKS):
        x_send(t).start()

    def rs_copy(ph, t, i, grad):
        o = y_dev(i)
        src = imgf.at[t, o] if grad else imgb.at[t, o]
        dst = recvg.at[t, YS - i] if grad else recvh.at[ph - 1, t, YS - i]
        return rcopy(src, dst, rs_s.at[0], rs_r.at[t], (s, CORES * o + c))

    def rs_all(ph, t, grad):
        every = recvg.at[t, pl.ds(1, YS - 1)] if grad else recvh.at[ph - 1, t, pl.ds(1, YS - 1)]
        return rcopy(every, every, rs_s.at[0], rs_r.at[t], sib)

    def rs_sent(grad):
        every = imgf.at[pl.ds(0, YS - 1)] if grad else imgb.at[pl.ds(0, YS - 1)]
        return rcopy(every, every, rs_s.at[0], rs_r.at[0], sib)

    def ag_copy(ph, t, i):
        return rcopy(E.at[ph, t, 0], E.at[ph, t, YS - i], ag_s.at[0], ag_r.at[t], (s, CORES * y_dev(i) + c))

    def ag_all(ph, t):
        every = E.at[ph, t, pl.ds(1, YS - 1)]
        return rcopy(every, every, ag_s.at[0], ag_r.at[t], sib)

    def ag_sent(ph):
        every = E.at[ph, pl.ds(0, YS - 1)]
        return rcopy(every, every, ag_s.at[0], ag_r.at[0], sib)

    @scoped('own_images')
    def own_images(ph, grad):
        for t in range(CHUNKS):
            at = slice(t * CROWS, (t + 1) * CROWS)
            if grad:
                x_own(t).wait()
            own[t] = lax.dot_general(dB[ph, c], X[c, at], NT, preferred_element_type=f32)

    @scoped('images')
    def images(ph, grad):
        if not grad:
            own_images(ph, False)
        d_recv(ph).wait_recv()
        for t in range(CHUNKS):
            at = slice(t * CROWS, (t + 1) * CROWS)
            if grad:
                x_recv(t).wait_recv()
            img = own[t] + lax.dot_general(dB[ph, 1 - c], X[1 - c, at], NT, preferred_element_type=f32)
            for o in range(YS):
                piece = pack_piece(img[:, o * PIECE : (o + 1) * PIECE])
                imgf[t, o] = piece
                if not grad:
                    imgb[t, o] = piece.astype(bf16)
            for i in (2, 1, 3):
                rs_copy(ph, t, i, grad).start()

    @scoped('pieces')
    def pieces(ph, grad):
        @pl.loop(0, CHUNKS)
        def _(t):
            total = imgf[t, y]
            rs_all(ph, t, grad).wait_recv()
            for i in range(1, YS):
                total = total + (recvg[t, i] if grad else recvh[ph - 1, t, i].astype(f32))
            total = unpack_piece(total)
            if grad:
                logits = total / math.sqrt(F)
                row = lax.broadcasted_iota(jnp.int32, (16, PIECE), 0)
                logits = jnp.where(row < K, logits, -jnp.inf)
                top = jnp.max(logits, axis=0, keepdims=True)
                ex = jnp.exp(logits - top)
                pr = ex / jnp.sum(ex, axis=0, keepdims=True)
                prob[t] = pr
                lab_copy(t).wait()
                mine = lab[t]
                coeffs = pr - jnp.where(row == mine, 1.0, 0.0)
            else:
                pr = prob[t]
                weighted = pr * total
                coeffs = weighted - pr * jnp.sum(weighted, axis=0, keepdims=True)
            E[ph, t, 0] = pack_piece(coeffs).astype(bf16)
            for i in (2, 1, 3):
                ag_copy(ph, t, i).start()

    @scoped('collect')
    def collect(ph):
        Q[...] = jnp.zeros_like(Q)

        @pl.loop(0, CHUNKS)
        def _(t):
            ag_all(ph, t).wait_recv()
            e = jnp.concatenate([spread_piece(E[ph, t, slot(o, y, YS)].astype(f32)) for o in range(YS)], axis=1).astype(bf16)
            at = pl.ds(pl.multiple_of(t * CROWS, CROWS), CROWS)
            for h in range(2):
                Q[h] = Q[h] + jnp.dot(e, X[h, at], preferred_element_type=f32)

        for h in range(2):
            Q[h] = fold_rows(Q[h])

    def q_copy(ph):
        return rcopy(Q.at[1 - c], Qr.at[ph], q_s.at[0], q_r.at[0], sib)

    def ar_copy(ph, i):
        return rcopy(ar.at[ph, 0], ar.at[ph, SAMP - i], ar_s.at[ph], ar_r.at[ph], (samp_dev(i), f))

    def ar_all(ph):
        every = ar.at[ph, pl.ds(1, SAMP - 1)]
        return rcopy(every, every, ar_s.at[ph], ar_r.at[ph], sib)

    def fe_copy(ph, i):
        return rcopy(fe.at[ph, 0], fe.at[ph, FEAT - i], fe_s.at[ph], fe_r.at[ph], (s, feat_dev(i)))

    def fe_all(ph):
        every = fe.at[ph, pl.ds(1, FEAT - 1)]
        return rcopy(every, every, fe_s.at[ph], fe_r.at[ph], sib)

    def chip_sum(ph):
        q_copy(ph).start()
        q_copy(ph).wait_recv()
        return pack(Q[c] + Qr[ph])

    @scoped('sums_start')
    def start_sums(ph):
        ar[ph, 0] = chip_sum(ph)
        for i in range(1, SAMP):
            ar_copy(ph, i).start()

    @scoped('sums_finish')
    def finish_sums(ph):
        ar_all(ph).wait_recv()
        return in_order(ar.at[ph], s, SAMP)

    def last_copy(i):
        return rcopy(dots.at[0], dots.at[SAMP - i], ar_s.at[ITERS], ar_r.at[ITERS], (samp_dev(i), f))

    def last_all():
        every = dots.at[pl.ds(1, SAMP - 1)]
        return rcopy(every, every, ar_s.at[ITERS], ar_r.at[ITERS], sib)

    @scoped('sums_last')
    def sums_last(message):
        dots[0] = message
        for i in range(1, SAMP):
            last_copy(i).start()
        drain(ITERS, False)
        drain_sums(ITERS - 2)
        last_all().wait_recv()
        return in_order(dots, s, SAMP)

    @scoped('drain')
    def drain(ph, grad):
        d_copy(ph).wait_send()
        q_copy(ph).wait_send()
        rs_sent(grad).wait_send()
        ag_sent(ph).wait_send()

    def drain_setup():
        x_sent().wait_send()

        @pl.when(s < 10)
        def _():
            gf_all().wait_send()
            gs_sent().wait_send()

        for m in range(len(MSGS)):
            gy_all(m).wait_send()

    def drain_sums(ph):
        ar_all(ph).wait_send()
        fe_all(ph).wait_send()

    def send_sums(ph, message):
        fe[ph, 0] = message
        for i in FAR_FEAT:
            fe_copy(ph, i).start()

    @scoped('exchange')
    def take_sums(ph):
        fe_all(ph).wait_recv()
        return in_order(fe.at[ph], f, FEAT)

    def exchange(ph, message):
        send_sums(ph, message)
        return take_sums(ph)

    own_images(0, True)

    @pl.when(s < 10)
    @scoped('gram_sum')
    def _():
        gf_all().wait_recv()
        grecv[0] = gpart[f]
        gall[0, s] = in_order(grecv, f, FEAT)
        for i in FAR_SAMP:
            gs_copy(i).start()

    images(0, True)

    @scoped('gram_gather')
    def gram_gather(first, last):
        for m in range(first, last):
            start, count = MSGS[m]
            for o in range(start, start + count):
                @pl.when(s != o)
                def _():
                    gs_recv(o).wait_recv()
            for i in FAR_FEAT:
                gy_copy(m, i).start()

    gram_gather(0, 2)
    pieces(0, True)
    gram_gather(2, 5)

    sv = svals[...]
    low = jnp.min(jnp.min(sv, axis=1, keepdims=True), axis=0, keepdims=True)
    coef = (low + RIDGE) / (sv + RIDGE) - 1.0
    for jt in range(4):
        ccol[jt * 128 : (jt + 1) * 128, :] = column(coef[jt : jt + 1, :])
    eye = jnp.where(rows_of(128) == lax.broadcasted_iota(jnp.int32, (128, 128), 1), 1.0, 0.0).astype(f32)

    def lanes(a, b):
        return slice(a * 128, b * 128)

    def dot_hi(a, b, dims=(((1,), (0,)), ((), ()))):
        return lax.dot_general(a, b, dims, precision=HI, preferred_element_type=f32)

    def gram_block(k, l):
        blk = jnp.concatenate([gall[slot(o, f, FEAT), OFFS[k] + l - k] for o in range(FEAT)], axis=0)
        return blk if k == 0 else blk - acc[k, :, lanes(l, l + 1)]

    def add_to(k, i, a, b):
        term = dot_hi(V[k, :, lanes(i, i + 1)], V[k, :, lanes(a, b)], TN)
        first = k == 0 if b <= 4 else k == a - 4
        acc[i, :, lanes(a, b)] = term if first else acc[i, :, lanes(a, b)] + term

    def rest_of(k):
        inv = V[k, :, lanes(4 + k, 5 + k)]
        if k < 2:
            V[k, :, lanes(k + 2, 4)] = dot_hi(inv, jnp.concatenate([gram_block(k, l) for l in range(k + 2, 4)], axis=1))
        if k > 0:
            V[k, :, lanes(4, 4 + k)] = -dot_hi(inv, acc[k, :, lanes(4, 4 + k)])
        for i in range(k + 1, 4):
            if i > k + 1:
                add_to(k, i, i, 4)
            elif i < 3:
                add_to(k, i, i + 1, 4)
            if k > 0:
                add_to(k, i, 4, 4 + k)
            add_to(k, i, 4 + k, 5 + k)

    @scoped('basis_dots')
    def basis_dots(packed):
        rows = [lane_row(packed, lt // 2, lt % 2) for lt in range(LT)]

        @pl.loop(0, 8)
        def _(g):
            at = pl.ds(pl.multiple_of(g * 64, 64), 64)
            acc = BT[at, 0:128] * rows[0]
            for lt in range(1, LT):
                acc = acc + BT[at, lt * 128 : (lt + 1) * 128] * rows[lt]
            tmp[at, :] = acc

        return [jnp.sum(tmp[jt * 128 : (jt + 1) * 128, :].T, axis=0, keepdims=True) for jt in range(4)]

    def lanes_of(a, b):
        t = a * b
        t = jnp.sum(t[:, :128] + t[:, 128:256] + t[:, 256:], axis=0, keepdims=True)
        return t + pltpu.roll(t, 64, 1)

    lane = lax.broadcasted_iota(jnp.int32, (1, 128), 1)

    def both(x, z):
        return jnp.where(lane < 64, x, z)

    def halves(total):
        wide = lax.broadcasted_iota(jnp.int32, (8, 128), 1)
        lo = jnp.sum(jnp.where(wide < 64, total, 0.0), axis=1, keepdims=True)
        hi = jnp.sum(jnp.where(wide < 64, 0.0, total), axis=1, keepdims=True)
        return lo, hi

    @scoped('inner')
    def inner_part(p):
        y_rows = [jnp.zeros((8, 128), f32) for _ in range(4)]
        dot = jnp.zeros((8, 128), f32)
        for g in range(8):
            kb, at, crow = g // 2, slice((g % 2) * 64, (g % 2) * 64 + 64), slice(g * 64, (g + 1) * 64)
            m = V[kb, at, lanes(4, 5)] * p[0]
            for l in range(1, kb + 1):
                m = m + V[kb, at, lanes(4 + l, 5 + l)] * p[l]
            inner = jnp.sum(m, axis=1, keepdims=True)
            ci = ccol[crow, :] * inner
            d = ci * inner
            for b in range(8):
                dot = dot + d[b * 8 : (b + 1) * 8]
            for l in range(kb + 1):
                t = V[kb, at, lanes(4 + l, 5 + l)] * ci
                for b in range(8):
                    y_rows[l] = y_rows[l] + t[b * 8 : (b + 1) * 8]
        return (
            [jnp.sum(t, axis=0, keepdims=True) for t in y_rows],
            jnp.sum(dot, axis=0, keepdims=True)[:, :1],
        )

    @scoped('basis_apply')
    def basis_apply(y_rows):
        for jt in range(4):
            tmp[jt * 128 : (jt + 1) * 128, :] = column(y_rows[jt])

        def body(g, accs):
            out = list(accs)
            for b in range(4):
                at = pl.ds(pl.multiple_of(g * 32 + b * 8, 8), 8)
                col = tmp[at, :]
                for lt in range(LT):
                    out[lt] = out[lt] + BT[at, lt * 128 : (lt + 1) * 128] * col
            return tuple(out)

        accs = lax.fori_loop(0, 16, body, tuple(jnp.zeros((8, 128), f32) for _ in range(LT)))
        rows = [jnp.sum(t, axis=0, keepdims=True) for t in accs]
        tiles = [jnp.concatenate([rows[2 * k + h] for k in range(8)], axis=0) for h in range(2)]
        zero = jnp.zeros((1, 128), f32)
        last = jnp.concatenate([rows[16], rows[18], rows[17], rows[19]] + [zero] * 4, axis=0)
        return jnp.concatenate(tiles + [last], axis=1)

    def set_direction(ph, d):
        vec[1] = d
        dB[ph, c] = unpack(d).astype(bf16)
        d_copy(ph).start()

    NS = float(SAMP * ROWS)
    zrow = jnp.zeros((1, 128), f32)
    for kb in range(4):
        with jax.named_scope('chol_wait'):
            gy_all(kb + 1 if kb else 0).wait_recv()
        with jax.named_scope('chol'):
            FA[...] = gram_block(kb, kb)
            FN[...] = eye
            if kb > 0:
                rest_of(kb - 1)
            factor_block(FA, FN)
            V[kb, :, lanes(4 + kb, 5 + kb)] = FN[...]
            if kb == 0:
                gy_all(1).wait_recv()
            if kb < 3:
                V[kb, :, lanes(kb + 1, kb + 2)] = dot_hi(FN[...], gram_block(kb, kb + 1))
                add_to(kb, kb + 1, kb + 1, kb + 2)
        if kb == 0:
            collect(0)
            start_sums(0)
        if kb == 2:
            res = -(finish_sums(0) * (math.sqrt(F) / NS) + RIDGE * pack(w))
            vec[0] = res
            send_sums(0, jnp.concatenate(
                basis_dots(res) + [zrow, zrow, both(lanes_of(res, res), zrow), zrow], axis=0
            ))
    rest_of(3)

    drain(0, True)
    tot = take_sums(0)
    lo, hi = halves(tot)
    y_rows, py = inner_part([tot[i : i + 1] for i in range(4)])
    rr = lo[6:7]
    prow[...] = tot
    vec[2] = jnp.zeros((8, 384), f32)
    scal[0:1, :] = jnp.broadcast_to(rr, (1, 128))
    scal[1:2, :] = jnp.broadcast_to(rr + py, (1, 128))
    set_direction(1, vec[0] + basis_apply(y_rows))

    @pl.loop(0, ITERS)
    def _(it):
        ph = it + 1
        images(ph, False)
        pieces(ph, False)
        collect(ph)

        @pl.when(it == ITERS - 1)
        def _():
            d, r = vec[1], vec[0]
            dq = sums_last(jnp.broadcast_to(lanes_of(d, chip_sum(ITERS)), (8, 128)))[0:1]
            dq = dq / NS + RIDGE * lanes_of(d, d)
            send_sums(ITERS, jnp.broadcast_to(both(dq, lanes_of(r, d)), (8, 128)))
            drain_sums(ITERS - 1)
            last_all().wait_send()
            lo, hi = halves(take_sums(ITERS))
            with jax.named_scope('out'):
                out[...] = unpack(vec[2] + hi[0:1] / lo[0:1] * d)[:K]

        @pl.when(it < ITERS - 1)
        def _():
            start_sums(ph)
            drain(ph, False)

            @pl.when(it == 0)
            def _():
                drain_setup()

            @pl.when(it > 0)
            def _():
                drain_sums(ph - 2)

            d, r = vec[1], vec[0]
            q = finish_sums(ph) / NS + RIDGE * d
            bq = basis_dots(q)
            tot = exchange(ph, jnp.concatenate(bq + [
                both(lanes_of(d, q), lanes_of(r, d)),
                both(lanes_of(r, q), lanes_of(q, q)),
                both(lanes_of(r, r), zrow),
                zrow,
            ], axis=0))
            lo, hi = halves(tot)
            step = hi[4:5] / lo[4:5]
            vec[2] = vec[2] + step * d
            rn = r - step * q
            vec[0] = rn
            pn = prow[...] - step * tot
            prow[...] = pn
            y_rows, py = inner_part([pn[i : i + 1] for i in range(4)])
            rr = lo[6:7] - 2.0 * step * lo[5:6] + step * step * hi[5:6]
            new = rr + py
            beta = new / scal[1:2, 0:1]
            scal[1:2, :] = jnp.broadcast_to(new, (1, 128))
            set_direction(ph + 1, rn + basis_apply(y_rows) + beta * d)

    with jax.named_scope('last_waits'):
        fe_all(ITERS).wait_send()


def on_device(features, labels, weights, sketch_basis, sketch_values):
    vmem = pl.BlockSpec(memory_space=pltpu.VMEM)
    hbm = pl.BlockSpec(memory_space=pl.ANY)
    V = pltpu.VMEM
    dma = pltpu.SemaphoreType.DMA
    PH = ITERS + 1
    scratch = [
        V((2, HALF, COLS), bf16),
        V((CHUNKS, 16, CROWS), f32),
        V((K * COLS, RANK), f32),
        V((RANK, K * COLS), f32),
        V((PH, 2, 16, COLS), bf16),
        V((CHUNKS, YS, 8, PWIDE), f32),
        V((CHUNKS, YS, 8, PWIDE), bf16),
        V((CHUNKS, YS, 8, PWIDE), f32),
        V((ITERS, CHUNKS, YS, 8, PWIDE), bf16),
        V((CHUNKS, 16, PIECE), f32),
        V((PH, CHUNKS, YS, 8, PWIDE), bf16),
        V((2, 16, COLS), f32),
        V((PH, 16, COLS), f32),
        V((ITERS, SAMP, 8, 384), f32),
        V((SAMP, 8, 128), f32),
        V((PH, FEAT, 8, 128), f32),
        V((CHUNKS, 1, PIECE), jnp.int32),
        V((FEAT, 16, 128), f32),
        V((FEAT, 16, 128), f32),
        V((FEAT, SAMP, 16, 128), f32),
        V((4, 128, 2 * RANK), f32),
        V((4, 128, 2 * RANK), f32),
        V((128, 128), f32),
        V((128, 128), f32),
        V((RANK, 128), f32),
        V((RANK, 128), f32),
        V((3, 8, 384), f32),
        V((8, 128), f32),
        V((8, 128), f32),
        dma((CHUNKS,)), dma((1,)), dma((CHUNKS,)), dma((K,)),
        dma((1,)), dma((CHUNKS,)), dma((1,)), dma((CHUNKS,)),
        dma((1,)), dma((1,)), dma((1,)), dma((1,)),
        dma((PH,)), dma((PH,)), dma((PH,)), dma((PH,)),
        dma((1,)), dma((1,)), dma((1,)), dma((10,)),
        dma((len(MSGS),)), dma((len(MSGS),)), dma((CHUNKS,)),
    ]
    step = pl.pallas_call(
        kernel,
        out_shape=jax.ShapeDtypeStruct((K, COLS), f32),
        in_specs=[hbm, hbm, vmem, hbm, vmem],
        out_specs=vmem,
        scratch_shapes=scratch,
        compiler_params=pltpu.CompilerParams(
            collective_id=0, has_side_effects=True, vmem_limit_bytes=60 * 1024 * 1024
        ),
        name="newton_step",
    )(
        features,
        labels,
        weights,
        sketch_basis.reshape(K * COLS, RANK),
        sketch_values.reshape(4, 128),
    )
    return step


def solution(mesh):
    in_specs = (P("samp", "feat"), P("samp"), P(None, "feat"), P(None, "feat", None), P())
    return jax.shard_map(
        on_device, mesh=mesh, in_specs=in_specs, out_specs=P(None, "feat"), check_vma=False
    )
```

```python
import functools
import math

import jax
import jax.numpy as jnp
from jax import lax
from jax.experimental import pallas as pl
from jax.experimental.pallas import tpu as pltpu
from jax.sharding import PartitionSpec as P

F = 2048
ITERS = 3
RIDGE = 0.05
SAMP, YS, CORES = 16, 4, 2
FEAT = YS * CORES
ROWS = 16384
HALF = ROWS // CORES
CHUNKS = 4
CROWS = HALF // CHUNKS
PIECE = CROWS // YS
PTILES = PIECE // 128
PWIDE = PIECE + (PTILES + 3) // 4 * 128
COLS = 256
K = 10
RANK = 512
LT = K * COLS // 128
f32, bf16 = jnp.float32, jnp.bfloat16
HI = lax.Precision.HIGHEST
NT = (((1,), (1,)), ((), ()))
TN = (((0,), (0,)), ((), ()))
OFFS = (0, 4, 7, 9)
MSGS = ((0, 1), (1, 3), (4, 3), (7, 2), (9, 1))
FAR_SAMP = sorted(range(1, SAMP), key=lambda i: -(min(i // 4, 4 - i // 4) + min(i % 4, 4 - i % 4)))
FAR_FEAT = (4, 5, 3, 2, 6, 7, 1)


def scoped(name):
    def wrap(fn):
        @functools.wraps(fn)
        def run(*args):
            with jax.named_scope(name):
                return fn(*args)
        return run
    return wrap


def rcopy(src, dst, send, recv, dev):
    return pltpu.make_async_remote_copy(
        src_ref=src, dst_ref=dst, send_sem=send, recv_sem=recv,
        device_id=dev, device_id_type=pl.DeviceIdType.MESH,
    )


def rows_of(n):
    return lax.broadcasted_iota(jnp.int32, (n, 128), 0)


def pack(wide):
    low = wide[8:16]
    third = low[:, :128] + pltpu.roll(low[:, 128:], 2, 0)
    return jnp.concatenate([wide[:8], third], axis=1)


def unpack(packed):
    third = packed[:, 256:]
    row = rows_of(8)
    left = jnp.where(row < 2, third, 0.0)
    right = jnp.where(row < 2, pltpu.roll(third, 6, 0), 0.0)
    return jnp.concatenate([packed[:, :256], jnp.concatenate([left, right], axis=1)], axis=0)


def pack_piece(wide):
    low = wide[8:16]
    tiles = [wide[:8]]
    for e in range(0, PTILES, 4):
        last = low[:, e * 128 : (e + 1) * 128]
        for q in range(e + 1, min(e + 4, PTILES)):
            last = last + pltpu.roll(low[:, q * 128 : (q + 1) * 128], 2 * (q - e), 0)
        tiles.append(last)
    return jnp.concatenate(tiles, axis=1)


def shared_tile(packed, q):
    at = PIECE + q // 4 * 128
    return packed[:, at : at + 128]


def unpack_piece(packed):
    row = rows_of(8)
    low = []
    for q in range(PTILES):
        tile = shared_tile(packed, q)
        low.append(jnp.where(row < 2, pltpu.roll(tile, 8 - 2 * (q % 4), 0) if q % 4 else tile, 0.0))
    return jnp.concatenate([packed[:, :PIECE], jnp.concatenate(low, axis=1)], axis=0)


def spread_piece(packed):
    row = rows_of(8)
    low = [
        jnp.where((row >= 2 * (q % 4)) & (row < 2 * (q % 4) + 2), shared_tile(packed, q), 0.0) for q in range(PTILES)
    ]
    return jnp.concatenate([packed[:, :PIECE], jnp.concatenate(low, axis=1)], axis=0)


def fold_rows(wide):
    low = wide[8:16]
    low = low + pltpu.roll(low, 4, 0)
    low = low + pltpu.roll(low, 2, 0)
    row = lax.broadcasted_iota(jnp.int32, low.shape, 0)
    return jnp.concatenate([wide[:8], jnp.where(row < 2, low, 0.0)], axis=0)


def lane_row(packed, k, h):
    if k < 8:
        return packed[k : k + 1, h * 128 : (h + 1) * 128]
    r = 2 * h + (k - 8)
    return packed[r : r + 1, 256:384]


def column(row):
    return jnp.broadcast_to(row, (128, 128)).T


def lane_bcast(x, j):
    return jnp.broadcast_to(x[:, j : j + 1], (x.shape[0], 128))


@scoped('factor')
def factor_block(A, N):
    diag = [lane_bcast(A[0:8, :], j) for j in range(8)]
    for p in range(16):
        lo = 8 * p
        more = lo + 8 < 128
        if more:
            below = [lane_bcast(A[lo + 8 : 128, :], lo + j) for j in range(8)]
            ahead = [lane_bcast(A[lo + 8 : lo + 16, :], lo + 8 + j) for j in range(8)]
        rs, cs = [], []
        for j in range(8):
            r = lax.rsqrt(diag[j][j : j + 1, :])
            c = diag[j] * r
            for k in range(j + 1, 8):
                diag[k] = diag[k] - c * c[k : k + 1, :]
            rs.append(r)
            cs.append(c)
        arow, nrow = A[lo : lo + 8, :], N[lo : lo + 8, :]
        us, ns = [], []
        for j in range(8):
            us.append(arow[j : j + 1, :] * rs[j])
            ns.append(nrow[j : j + 1, :] * rs[j])
            if j < 7:
                arow = arow - cs[j] * us[j]
                nrow = nrow - cs[j] * ns[j]
        N[lo : lo + 8, :] = jnp.concatenate(ns, axis=0)
        if not more:
            continue
        bs = []
        for j in range(8):
            t = below[j]
            for i in range(j):
                t = t - bs[i] * cs[i][j : j + 1, :]
            bs.append(t * rs[j])
        for k in range(8):
            for j in range(8):
                ahead[k] = ahead[k] - bs[j][:8] * bs[j][k : k + 1, :]
        diag = ahead
        at, nt = A[lo + 8 : 128, :], N[lo + 8 : 128, :]
        for j in range(8):
            at = at - bs[j] * us[j]
            nt = nt - bs[j] * ns[j]
        A[lo + 8 : 128, :] = at
        N[lo + 8 : 128, :] = nt


def kernel(
    feat, labels, weights, basis, svals, out,
    X, own, bst, BT, dB, imgf, imgb, recvg, recvh, prob, E, Q, Qr, ar, dots, fe,
    lab, gpart, grecv, gall, V, acc, FA, FN, ccol, tmp, vec, prow, scal,
    sx_own, sx_s, sx_r, s_b, rs_s, rs_r, ag_s, ag_r, q_s, q_r, d_s, d_r,
    ar_s, ar_r, fe_s, fe_r, gf_s, gf_r, gs_s, gs_r, gy_s, gy_r, l_s,
):
    s = lax.axis_index("samp")
    f = lax.axis_index("feat")
    y = lax.div(f, CORES)
    c = lax.rem(f, CORES)
    sib = (s, f + 1 - 2 * c)

    def samp_dev(i):
        return lax.rem(s + i, SAMP)

    def feat_dev(i):
        return lax.rem(f + i, FEAT)

    def y_dev(i):
        return lax.rem(y + i, YS)

    def slot(o, me, n):
        return lax.rem(o - me + n, n)

    def in_order(ref, me, n):
        total = ref[slot(0, me, n)]
        for o in range(1, n):
            total = total + ref[slot(o, me, n)]
        return total

    barrier = pltpu.get_barrier_semaphore()
    for i in FAR_SAMP:
        pl.semaphore_signal(barrier, inc=1, device_id=(samp_dev(i), f), device_id_type=pl.DeviceIdType.MESH)
    for i in FAR_FEAT:
        pl.semaphore_signal(barrier, inc=1, device_id=(s, feat_dev(i)), device_id_type=pl.DeviceIdType.MESH)

    for k in range(K):
        pltpu.make_async_copy(basis.at[pl.ds(k * COLS, COLS)], bst.at[pl.ds(k * COLS, COLS)], s_b.at[k]).start()

    def own_rows(t):
        return pl.ds(pl.multiple_of(c * HALF + t * CROWS, CROWS), CROWS)

    def sib_rows(t):
        return pl.ds(pl.multiple_of((1 - c) * HALF + t * CROWS, CROWS), CROWS)

    def x_own(t):
        return pltpu.make_async_copy(feat.at[own_rows(t)], X.at[c, pl.ds(t * CROWS, CROWS)], sx_own.at[t])

    def x_send(t):
        return rcopy(feat.at[sib_rows(t)], X.at[c, pl.ds(t * CROWS, CROWS)], sx_s.at[0], sx_r.at[t], sib)

    def x_recv(t):
        dst = X.at[1 - c, pl.ds(t * CROWS, CROWS)]
        return rcopy(dst, dst, sx_s.at[0], sx_r.at[t], sib)

    def x_sent():
        return rcopy(X.at[c], X.at[c], sx_s.at[0], sx_r.at[0], sib)

    def lab_copy(t):
        start = pl.multiple_of(c * HALF + t * CROWS + y * PIECE, PIECE)
        return pltpu.make_async_copy(labels.at[pl.ds(start, PIECE)], lab.at[t, 0], l_s.at[t])


    def d_copy(ph):
        return rcopy(dB.at[ph, c], dB.at[ph, c], d_s.at[0], d_r.at[0], sib)

    def d_recv(ph):
        return rcopy(dB.at[ph, 1 - c], dB.at[ph, 1 - c], d_s.at[0], d_r.at[0], sib)

    w = jnp.concatenate([weights[...], jnp.zeros((16 - K, COLS), f32)], axis=0)
    dB[0, c] = w.astype(bf16)

    @pl.loop(0, K)
    @scoped('transpose')
    def _(k):
        pltpu.make_async_copy(
            basis.at[pl.ds(k * COLS, COLS)], bst.at[pl.ds(k * COLS, COLS)], s_b.at[k]
        ).wait()
        for h in range(2):
            for jt in range(4):
                blk = bst[pl.ds(pl.multiple_of(k * COLS + h * 128, 128), 128), jt * 128 : (jt + 1) * 128]
                BT[jt * 128 : (jt + 1) * 128, pl.ds(pl.multiple_of(k * COLS + h * 128, 128), 128)] = blk.T

    for t in range(CHUNKS):
        x_own(t).start()
        lab_copy(t).start()

    blk_id = lax.min(s, 9)
    ba = sum((blk_id >= e).astype(jnp.int32) for e in (4, 7, 9))
    bb = blk_id - lax.div(ba * (9 - ba), 2) + ba

    with jax.named_scope('gram'):
        block = lax.dot_general(
            BT[pl.ds(pl.multiple_of(ba * 128, 128), 128), :],
            BT[pl.ds(pl.multiple_of(bb * 128, 128), 128), :],
            NT, precision=HI, preferred_element_type=f32,
        )
        for g in range(FEAT):
            gpart[g] = block[g * 16 : (g + 1) * 16]

    def gf_copy(i):
        o = feat_dev(i)
        return rcopy(gpart.at[o], grecv.at[FEAT - i], gf_s.at[0], gf_r.at[0], (s, o))

    def gf_all():
        every = grecv.at[pl.ds(1, FEAT - 1)]
        return rcopy(every, every, gf_s.at[0], gf_r.at[0], sib)

    def gs_copy(i):
        return rcopy(gall.at[0, s], gall.at[0, s], gs_s.at[0], gs_r.at[s], (samp_dev(i), f))

    def gs_sent():
        every = gall.at[0, pl.ds(0, SAMP - 1)]
        return rcopy(every, every, gs_s.at[0], gs_r.at[0], sib)

    def gs_recv(o):
        return rcopy(gall.at[0, o], gall.at[0, o], gs_s.at[0], gs_r.at[o], (o, f))

    def gy_copy(m, i):
        at = pl.ds(*MSGS[m])
        return rcopy(gall.at[0, at], gall.at[FEAT - i, at], gy_s.at[m], gy_r.at[m], (s, feat_dev(i)))

    def gy_all(m):
        every = gall.at[pl.ds(1, FEAT - 1), pl.ds(*MSGS[m])]
        return rcopy(every, every, gy_s.at[m], gy_r.at[m], sib)

    with jax.named_scope('barrier'):
        pl.semaphore_wait(barrier, FEAT - 1 + SAMP - 1)

    @pl.when(s < 10)
    def _():
        for i in FAR_FEAT:
            gf_copy(i).start()

    d_copy(0).start()
    for t in range(CHUNKS):
        x_send(t).start()

    def rs_copy(ph, t, i, grad):
        o = y_dev(i)
        src = imgf.at[t, o] if grad else imgb.at[t, o]
        dst = recvg.at[t, YS - i] if grad else recvh.at[ph - 1, t, YS - i]
        return rcopy(src, dst, rs_s.at[0], rs_r.at[t], (s, CORES * o + c))

    def rs_all(ph, t, grad):
        every = recvg.at[t, pl.ds(1, YS - 1)] if grad else recvh.at[ph - 1, t, pl.ds(1, YS - 1)]
        return rcopy(every, every, rs_s.at[0], rs_r.at[t], sib)

    def rs_sent(grad):
        every = imgf.at[pl.ds(0, YS - 1)] if grad else imgb.at[pl.ds(0, YS - 1)]
        return rcopy(every, every, rs_s.at[0], rs_r.at[0], sib)

    def ag_copy(ph, t, i):
        return rcopy(E.at[ph, t, 0], E.at[ph, t, YS - i], ag_s.at[0], ag_r.at[t], (s, CORES * y_dev(i) + c))

    def ag_all(ph, t):
        every = E.at[ph, t, pl.ds(1, YS - 1)]
        return rcopy(every, every, ag_s.at[0], ag_r.at[t], sib)

    def ag_sent(ph):
        every = E.at[ph, pl.ds(0, YS - 1)]
        return rcopy(every, every, ag_s.at[0], ag_r.at[0], sib)

    @scoped('own_images')
    def own_images(ph, grad):
        for t in range(CHUNKS):
            at = slice(t * CROWS, (t + 1) * CROWS)
            if grad:
                x_own(t).wait()
            own[t] = lax.dot_general(dB[ph, c], X[c, at], NT, preferred_element_type=f32)

    @scoped('images')
    def images(ph, grad):
        if not grad:
            own_images(ph, False)
        d_recv(ph).wait_recv()
        for t in range(CHUNKS):
            at = slice(t * CROWS, (t + 1) * CROWS)
            if grad:
                x_recv(t).wait_recv()
            img = own[t] + lax.dot_general(dB[ph, 1 - c], X[1 - c, at], NT, preferred_element_type=f32)
            for o in range(YS):
                piece = pack_piece(img[:, o * PIECE : (o + 1) * PIECE])
                imgf[t, o] = piece
                if not grad:
                    imgb[t, o] = piece.astype(bf16)
            for i in (2, 1, 3):
                rs_copy(ph, t, i, grad).start()

    @scoped('pieces')
    def pieces(ph, grad):
        @pl.loop(0, CHUNKS)
        def _(t):
            total = imgf[t, y]
            rs_all(ph, t, grad).wait_recv()
            for i in range(1, YS):
                total = total + (recvg[t, i] if grad else recvh[ph - 1, t, i].astype(f32))
            total = unpack_piece(total)
            if grad:
                logits = total / math.sqrt(F)
                row = lax.broadcasted_iota(jnp.int32, (16, PIECE), 0)
                logits = jnp.where(row < K, logits, -jnp.inf)
                top = jnp.max(logits, axis=0, keepdims=True)
                ex = jnp.exp(logits - top)
                pr = ex / jnp.sum(ex, axis=0, keepdims=True)
                prob[t] = pr
                lab_copy(t).wait()
                mine = lab[t]
                coeffs = pr - jnp.where(row == mine, 1.0, 0.0)
            else:
                pr = prob[t]
                weighted = pr * total
                coeffs = weighted - pr * jnp.sum(weighted, axis=0, keepdims=True)
            E[ph, t, 0] = pack_piece(coeffs).astype(bf16)
            for i in (2, 1, 3):
                ag_copy(ph, t, i).start()

    @scoped('collect')
    def collect(ph):
        Q[...] = jnp.zeros_like(Q)

        @pl.loop(0, CHUNKS)
        def _(t):
            ag_all(ph, t).wait_recv()
            e = jnp.concatenate([spread_piece(E[ph, t, slot(o, y, YS)].astype(f32)) for o in range(YS)], axis=1).astype(bf16)
            at = pl.ds(pl.multiple_of(t * CROWS, CROWS), CROWS)
            for h in range(2):
                Q[h] = Q[h] + jnp.dot(e, X[h, at], preferred_element_type=f32)

        for h in range(2):
            Q[h] = fold_rows(Q[h])

    def q_copy(ph):
        return rcopy(Q.at[1 - c], Qr.at[ph], q_s.at[0], q_r.at[0], sib)

    def ar_copy(ph, i):
        return rcopy(ar.at[ph, 0], ar.at[ph, SAMP - i], ar_s.at[ph], ar_r.at[ph], (samp_dev(i), f))

    def ar_all(ph):
        every = ar.at[ph, pl.ds(1, SAMP - 1)]
        return rcopy(every, every, ar_s.at[ph], ar_r.at[ph], sib)

    def fe_copy(ph, i):
        return rcopy(fe.at[ph, 0], fe.at[ph, FEAT - i], fe_s.at[ph], fe_r.at[ph], (s, feat_dev(i)))

    def fe_all(ph):
        every = fe.at[ph, pl.ds(1, FEAT - 1)]
        return rcopy(every, every, fe_s.at[ph], fe_r.at[ph], sib)

    def chip_sum(ph):
        q_copy(ph).start()
        q_copy(ph).wait_recv()
        return pack(Q[c] + Qr[ph])

    @scoped('sums_start')
    def start_sums(ph):
        ar[ph, 0] = chip_sum(ph)
        for i in range(1, SAMP):
            ar_copy(ph, i).start()

    @scoped('sums_finish')
    def finish_sums(ph):
        ar_all(ph).wait_recv()
        return in_order(ar.at[ph], s, SAMP)

    def last_copy(i):
        return rcopy(dots.at[0], dots.at[SAMP - i], ar_s.at[ITERS], ar_r.at[ITERS], (samp_dev(i), f))

    def last_all():
        every = dots.at[pl.ds(1, SAMP - 1)]
        return rcopy(every, every, ar_s.at[ITERS], ar_r.at[ITERS], sib)

    @scoped('sums_last')
    def sums_last(message):
        dots[0] = message
        for i in range(1, SAMP):
            last_copy(i).start()
        drain(ITERS, False)
        drain_sums(ITERS - 2)
        last_all().wait_recv()
        return in_order(dots, s, SAMP)

    @scoped('drain')
    def drain(ph, grad):
        d_copy(ph).wait_send()
        q_copy(ph).wait_send()
        rs_sent(grad).wait_send()
        ag_sent(ph).wait_send()

    def drain_setup():
        x_sent().wait_send()

        @pl.when(s < 10)
        def _():
            gf_all().wait_send()
            gs_sent().wait_send()

        for m in range(len(MSGS)):
            gy_all(m).wait_send()

    def drain_sums(ph):
        ar_all(ph).wait_send()
        fe_all(ph).wait_send()

    def send_sums(ph, message):
        fe[ph, 0] = message
        for i in FAR_FEAT:
            fe_copy(ph, i).start()

    @scoped('exchange')
    def take_sums(ph):
        fe_all(ph).wait_recv()
        return in_order(fe.at[ph], f, FEAT)

    def exchange(ph, message):
        send_sums(ph, message)
        return take_sums(ph)

    own_images(0, True)

    @pl.when(s < 10)
    @scoped('gram_sum')
    def _():
        gf_all().wait_recv()
        grecv[0] = gpart[f]
        gall[0, s] = in_order(grecv, f, FEAT)
        for i in FAR_SAMP:
            gs_copy(i).start()

    images(0, True)

    @scoped('gram_gather')
    def gram_gather(first, last):
        for m in range(first, last):
            start, count = MSGS[m]
            for o in range(start, start + count):
                @pl.when(s != o)
                def _():
                    gs_recv(o).wait_recv()
            for i in FAR_FEAT:
                gy_copy(m, i).start()

    gram_gather(0, 2)
    pieces(0, True)
    gram_gather(2, 5)

    sv = svals[...]
    low = jnp.min(jnp.min(sv, axis=1, keepdims=True), axis=0, keepdims=True)
    coef = (low + RIDGE) / (sv + RIDGE) - 1.0
    for jt in range(4):
        ccol[jt * 128 : (jt + 1) * 128, :] = column(coef[jt : jt + 1, :])
    eye = jnp.where(rows_of(128) == lax.broadcasted_iota(jnp.int32, (128, 128), 1), 1.0, 0.0).astype(f32)

    def lanes(a, b):
        return slice(a * 128, b * 128)

    def dot_hi(a, b, dims=(((1,), (0,)), ((), ()))):
        return lax.dot_general(a, b, dims, precision=HI, preferred_element_type=f32)

    def gram_block(k, l):
        blk = jnp.concatenate([gall[slot(o, f, FEAT), OFFS[k] + l - k] for o in range(FEAT)], axis=0)
        return blk if k == 0 else blk - acc[k, :, lanes(l, l + 1)]

    def add_to(k, i, a, b):
        term = dot_hi(V[k, :, lanes(i, i + 1)], V[k, :, lanes(a, b)], TN)
        first = k == 0 if b <= 4 else k == a - 4
        acc[i, :, lanes(a, b)] = term if first else acc[i, :, lanes(a, b)] + term

    def rest_of(k):
        inv = V[k, :, lanes(4 + k, 5 + k)]
        if k < 2:
            V[k, :, lanes(k + 2, 4)] = dot_hi(inv, jnp.concatenate([gram_block(k, l) for l in range(k + 2, 4)], axis=1))
        if k > 0:
            V[k, :, lanes(4, 4 + k)] = -dot_hi(inv, acc[k, :, lanes(4, 4 + k)])
        for i in range(k + 1, 4):
            if i > k + 1:
                add_to(k, i, i, 4)
            elif i < 3:
                add_to(k, i, i + 1, 4)
            if k > 0:
                add_to(k, i, 4, 4 + k)
            add_to(k, i, 4 + k, 5 + k)

    @scoped('basis_dots')
    def basis_dots(packed):
        rows = [lane_row(packed, lt // 2, lt % 2) for lt in range(LT)]

        @pl.loop(0, 8)
        def _(g):
            at = pl.ds(pl.multiple_of(g * 64, 64), 64)
            acc = BT[at, 0:128] * rows[0]
            for lt in range(1, LT):
                acc = acc + BT[at, lt * 128 : (lt + 1) * 128] * rows[lt]
            tmp[at, :] = acc

        return [jnp.sum(tmp[jt * 128 : (jt + 1) * 128, :].T, axis=0, keepdims=True) for jt in range(4)]

    def lanes_of(a, b):
        t = a * b
        t = jnp.sum(t[:, :128] + t[:, 128:256] + t[:, 256:], axis=0, keepdims=True)
        return t + pltpu.roll(t, 64, 1)

    lane = lax.broadcasted_iota(jnp.int32, (1, 128), 1)

    def both(x, z):
        return jnp.where(lane < 64, x, z)

    def halves(total):
        wide = lax.broadcasted_iota(jnp.int32, (8, 128), 1)
        lo = jnp.sum(jnp.where(wide < 64, total, 0.0), axis=1, keepdims=True)
        hi = jnp.sum(jnp.where(wide < 64, 0.0, total), axis=1, keepdims=True)
        return lo, hi

    @scoped('inner')
    def inner_part(p):
        y_rows = [jnp.zeros((8, 128), f32) for _ in range(4)]
        dot = jnp.zeros((8, 128), f32)
        for g in range(8):
            kb, at, crow = g // 2, slice((g % 2) * 64, (g % 2) * 64 + 64), slice(g * 64, (g + 1) * 64)
            m = V[kb, at, lanes(4, 5)] * p[0]
            for l in range(1, kb + 1):
                m = m + V[kb, at, lanes(4 + l, 5 + l)] * p[l]
            inner = jnp.sum(m, axis=1, keepdims=True)
            ci = ccol[crow, :] * inner
            d = ci * inner
            for b in range(8):
                dot = dot + d[b * 8 : (b + 1) * 8]
            for l in range(kb + 1):
                t = V[kb, at, lanes(4 + l, 5 + l)] * ci
                for b in range(8):
                    y_rows[l] = y_rows[l] + t[b * 8 : (b + 1) * 8]
        return (
            [jnp.sum(t, axis=0, keepdims=True) for t in y_rows],
            jnp.sum(dot, axis=0, keepdims=True)[:, :1],
        )

    @scoped('basis_apply')
    def basis_apply(y_rows):
        for jt in range(4):
            tmp[jt * 128 : (jt + 1) * 128, :] = column(y_rows[jt])

        def body(g, accs):
            out = list(accs)
            for b in range(4):
                at = pl.ds(pl.multiple_of(g * 32 + b * 8, 8), 8)
                col = tmp[at, :]
                for lt in range(LT):
                    out[lt] = out[lt] + BT[at, lt * 128 : (lt + 1) * 128] * col
            return tuple(out)

        accs = lax.fori_loop(0, 16, body, tuple(jnp.zeros((8, 128), f32) for _ in range(LT)))
        rows = [jnp.sum(t, axis=0, keepdims=True) for t in accs]
        tiles = [jnp.concatenate([rows[2 * k + h] for k in range(8)], axis=0) for h in range(2)]
        zero = jnp.zeros((1, 128), f32)
        last = jnp.concatenate([rows[16], rows[18], rows[17], rows[19]] + [zero] * 4, axis=0)
        return jnp.concatenate(tiles + [last], axis=1)

    def set_direction(ph, d):
        vec[1] = d
        dB[ph, c] = unpack(d).astype(bf16)
        d_copy(ph).start()

    NS = float(SAMP * ROWS)
    zrow = jnp.zeros((1, 128), f32)
    for kb in range(4):
        with jax.named_scope('chol_wait'):
            gy_all(kb + 1 if kb else 0).wait_recv()
        with jax.named_scope('chol'):
            FA[...] = gram_block(kb, kb)
            FN[...] = eye
            if kb > 0:
                rest_of(kb - 1)
            factor_block(FA, FN)
            V[kb, :, lanes(4 + kb, 5 + kb)] = FN[...]
            if kb == 0:
                gy_all(1).wait_recv()
            if kb < 3:
                V[kb, :, lanes(kb + 1, kb + 2)] = dot_hi(FN[...], gram_block(kb, kb + 1))
                add_to(kb, kb + 1, kb + 1, kb + 2)
        if kb == 0:
            collect(0)
            start_sums(0)
        if kb == 2:
            res = -(finish_sums(0) * (math.sqrt(F) / NS) + RIDGE * pack(w))
            vec[0] = res
            send_sums(0, jnp.concatenate(
                basis_dots(res) + [zrow, zrow, both(lanes_of(res, res), zrow), zrow], axis=0
            ))
    rest_of(3)

    drain(0, True)
    tot = take_sums(0)
    lo, hi = halves(tot)
    y_rows, py = inner_part([tot[i : i + 1] for i in range(4)])
    rr = lo[6:7]
    prow[...] = tot
    vec[2] = jnp.zeros((8, 384), f32)
    scal[0:1, :] = jnp.broadcast_to(rr, (1, 128))
    scal[1:2, :] = jnp.broadcast_to(rr + py, (1, 128))
    set_direction(1, vec[0] + basis_apply(y_rows))

    @pl.loop(0, ITERS)
    def _(it):
        ph = it + 1
        images(ph, False)
        pieces(ph, False)
        collect(ph)

        @pl.when(it == ITERS - 1)
        def _():
            d, r = vec[1], vec[0]
            dq = sums_last(jnp.broadcast_to(lanes_of(d, chip_sum(ITERS)), (8, 128)))[0:1]
            dq = dq / NS + RIDGE * lanes_of(d, d)
            send_sums(ITERS, jnp.broadcast_to(both(dq, lanes_of(r, d)), (8, 128)))
            drain_sums(ITERS - 1)
            last_all().wait_send()
            lo, hi = halves(take_sums(ITERS))
            with jax.named_scope('out'):
                out[...] = unpack(vec[2] + hi[0:1] / lo[0:1] * d)[:K]

        @pl.when(it < ITERS - 1)
        def _():
            start_sums(ph)
            drain(ph, False)

            @pl.when(it == 0)
            def _():
                drain_setup()

            @pl.when(it > 0)
            def _():
                drain_sums(ph - 2)

            d, r = vec[1], vec[0]
            q = finish_sums(ph) / NS + RIDGE * d
            bq = basis_dots(q)
            tot = exchange(ph, jnp.concatenate(bq + [
                both(lanes_of(d, q), lanes_of(r, d)),
                both(lanes_of(r, q), lanes_of(q, q)),
                both(lanes_of(r, r), zrow),
                zrow,
            ], axis=0))
            lo, hi = halves(tot)
            step = hi[4:5] / lo[4:5]
            vec[2] = vec[2] + step * d
            rn = r - step * q
            vec[0] = rn
            pn = prow[...] - step * tot
            prow[...] = pn
            y_rows, py = inner_part([pn[i : i + 1] for i in range(4)])
            rr = lo[6:7] - 2.0 * step * lo[5:6] + step * step * hi[5:6]
            new = rr + py
            beta = new / scal[1:2, 0:1]
            scal[1:2, :] = jnp.broadcast_to(new, (1, 128))
            set_direction(ph + 1, rn + basis_apply(y_rows) + beta * d)

    with jax.named_scope('last_waits'):
        fe_all(ITERS).wait_send()


def on_device(features, labels, weights, sketch_basis, sketch_values):
    vmem = pl.BlockSpec(memory_space=pltpu.VMEM)
    hbm = pl.BlockSpec(memory_space=pl.ANY)
    V = pltpu.VMEM
    dma = pltpu.SemaphoreType.DMA
    PH = ITERS + 1
    scratch = [
        V((2, HALF, COLS), bf16),
        V((CHUNKS, 16, CROWS), f32),
        V((K * COLS, RANK), f32),
        V((RANK, K * COLS), f32),
        V((PH, 2, 16, COLS), bf16),
        V((CHUNKS, YS, 8, PWIDE), f32),
        V((CHUNKS, YS, 8, PWIDE), bf16),
        V((CHUNKS, YS, 8, PWIDE), f32),
        V((ITERS, CHUNKS, YS, 8, PWIDE), bf16),
        V((CHUNKS, 16, PIECE), f32),
        V((PH, CHUNKS, YS, 8, PWIDE), bf16),
        V((2, 16, COLS), f32),
        V((PH, 16, COLS), f32),
        V((ITERS, SAMP, 8, 384), f32),
        V((SAMP, 8, 128), f32),
        V((PH, FEAT, 8, 128), f32),
        V((CHUNKS, 1, PIECE), jnp.int32),
        V((FEAT, 16, 128), f32),
        V((FEAT, 16, 128), f32),
        V((FEAT, SAMP, 16, 128), f32),
        V((4, 128, 2 * RANK), f32),
        V((4, 128, 2 * RANK), f32),
        V((128, 128), f32),
        V((128, 128), f32),
        V((RANK, 128), f32),
        V((RANK, 128), f32),
        V((3, 8, 384), f32),
        V((8, 128), f32),
        V((8, 128), f32),
        dma((CHUNKS,)), dma((1,)), dma((CHUNKS,)), dma((K,)),
        dma((1,)), dma((CHUNKS,)), dma((1,)), dma((CHUNKS,)),
        dma((1,)), dma((1,)), dma((1,)), dma((1,)),
        dma((PH,)), dma((PH,)), dma((PH,)), dma((PH,)),
        dma((1,)), dma((1,)), dma((1,)), dma((10,)),
        dma((len(MSGS),)), dma((len(MSGS),)), dma((CHUNKS,)),
    ]
    step = pl.pallas_call(
        kernel,
        out_shape=jax.ShapeDtypeStruct((K, COLS), f32),
        in_specs=[hbm, hbm, vmem, hbm, vmem],
        out_specs=vmem,
        scratch_shapes=scratch,
        compiler_params=pltpu.CompilerParams(
            collective_id=0, has_side_effects=True, vmem_limit_bytes=60 * 1024 * 1024
        ),
        name="newton_step",
    )(
        features,
        labels,
        weights,
        sketch_basis.reshape(K * COLS, RANK),
        sketch_values.reshape(4, 128),
    )
    return step


def solution(mesh):
    in_specs = (P("samp", "feat"), P("samp"), P(None, "feat"), P(None, "feat", None), P())
    return jax.shard_map(
        on_device, mesh=mesh, in_specs=in_specs, out_specs=P(None, "feat"), check_vma=False
    )
```
